32 devices in a mesh: gx: 4 (over y, x), gy: 2 (over core), gz: 4 (over z).
Axes of the slice: x: 2, y: 2, z: 4, core: 2. Of those that a mesh axis runs over, the one named last changes fastest.
Arguments:
- rhs: float32 [8, 64, 64, 512], P(None, 'gx', 'gy', 'gz'), may hold values from -8 to 8
- stencil: float32 [14, 64, 64, 512], P(None, 'gx', 'gy', 'gz'), may hold values from 0.02 to 1
Outputs:
- solution: float32 [8, 64, 64, 512], P(None, 'gx', 'gy', 'gz')
- residual: float32 [8, 64, 64, 512], P(None, 'gx', 'gy', 'gz')
The draws below stay inside these ranges and needn't reach their ends.
All inputs are finite; a program needn't handle non-finite values.
Results may differ from the reference program's by a relative error of at most 0.00029.
Values sent between devices are 32-bit elements; how exact they have to be, the bound alone decides.
A program may use at most 128 MiB of HBM per device.

```python
import math
import jax
import jax.numpy as jnp
from jax import lax

NRHS = 8
ITERS = 2
NX = 64
NY = 64
NZ = 512


def block_levels(own_key, dims, shards, low, high):
    level = 1.0
    for dim, blocks in shards:
        steps = jax.random.uniform(jax.random.fold_in(jax.random.fold_in(own_key, 6), dim), (blocks,), jnp.float32, low / len(shards), high / len(shards))
        level = level * jnp.repeat(jnp.exp(steps), dims[dim] // blocks).reshape((-1,) + (1,) * (len(dims) - 1 - dim))
    return level


def bell_draw(rng, shape, scale, bound, split=(), dtype=jnp.bfloat16):
    level = block_levels(rng, shape, split, -0.22, 0.18) if split else 1.0
    values = jax.random.normal(rng, shape, jnp.float32) * scale * level
    return jnp.minimum(jnp.maximum(values, -bound), bound).astype(dtype)


def setup_inputs(seed: int = 0) -> dict:
    seeds = jax.random.split(jax.random.key(seed), 3)
    return {
        "rhs": bell_draw(seeds[0], (NRHS, NX, NY, NZ), 1.0, 8.0, ((1, 4), (2, 2), (3, 4)), jnp.float32),
        "stencil": jnp.clip(jnp.exp(math.log(1.0) - 3.912023 * jax.random.uniform(seeds[1], (14, NX, NY, NZ), jnp.float32) ** block_levels(seeds[1], (14, NX, NY, NZ), ((1, 4), (2, 2), (3, 4)), -0.2, 0.2)), 0.02, 1.0),
    }


FORWARD = [(a, b, c) for a in (-1, 0, 1) for b in (-1, 0, 1) for c in (-1, 0, 1) if (a, b, c) > (0, 0, 0)]

def window(array, margin, depth, offset):
    result = array
    for place in range(3):
        dim = array.ndim - 3 + place
        inner = array.shape[dim] - 2 * margin
        begin = margin - depth + offset[place]
        result = lax.slice_in_dim(result, begin, begin + inner + 2 * depth, axis=dim)
    return result

def diagonal_field(padded, margin, depth):
    total = window(padded[0], margin, depth, (0, 0, 0))
    total = total + jnp.sum(window(padded[1:], margin, depth, (0, 0, 0)), axis=0)
    for index, offset in enumerate(FORWARD):
        back = (-offset[0], -offset[1], -offset[2])
        total = total + window(padded[index + 1], margin, depth, back)
    return total

def operate(field, fmargin, padded, smargin, diag, depth):
    result = diag[None] * window(field, fmargin, depth, (0, 0, 0))
    for index, offset in enumerate(FORWARD):
        back = (-offset[0], -offset[1], -offset[2])
        ahead_w = window(padded[index + 1], smargin, depth, (0, 0, 0))
        behind_w = window(padded[index + 1], smargin, depth, back)
        result = result - ahead_w[None] * window(field, fmargin, depth, offset)
        result = result - behind_w[None] * window(field, fmargin, depth, back)
    return result

def gram(left, right):
    flat_l = left.reshape(left.shape[0], -1)
    flat_r = right.reshape(right.shape[0], -1)
    return lax.dot_general(flat_l.astype(jnp.float32), flat_r.astype(jnp.float32), (((1,), (1,)), ((), ())), precision=lax.Precision.HIGHEST, preferred_element_type=jnp.float32)

def combine(coef, field):
    return jnp.einsum('ij,ixyz->jxyz', coef, field, precision=lax.Precision.HIGHEST)

def solve_spd(matrix, right):
    factor = jnp.linalg.cholesky(matrix)
    return jax.scipy.linalg.cho_solve((factor, True), right)

def reference(rhs, stencil):
    padded = jnp.pad(stencil, ((0, 0), (1, 1), (1, 1), (1, 1)))
    diag = diagonal_field(padded, 1, 0)
    solution = jnp.zeros_like(rhs)
    residual = rhs
    direction = rhs
    norm_now = gram(residual, residual)
    for step in range(ITERS):
        field = jnp.pad(direction, ((0, 0), (1, 1), (1, 1), (1, 1)))
        image = operate(field, 1, padded, 1, diag, 0)
        alpha = solve_spd(gram(direction, image), norm_now)
        solution = solution + combine(alpha, direction)
        residual = residual - combine(alpha, image)
        if step + 1 < ITERS:
            norm_next = gram(residual, residual)
            beta = solve_spd(norm_now, norm_next)
            direction = residual + combine(beta, direction)
            norm_now = norm_next
    return (solution, residual)
```

```python
import jax
import jax.numpy as jnp
from jax import lax
from jax.experimental import pallas as pl
from jax.experimental.pallas import tpu as pltpu
from jax.sharding import PartitionSpec as P

FORWARD = [
    (a, b, c) for a in (-1, 0, 1) for b in (-1, 0, 1) for c in (-1, 0, 1) if (a, b, c) > (0, 0, 0)
]
AXES = ("gx", "gy", "gz")
LO = [k for k, o in enumerate(FORWARD) if o[2] == 1]
HI = [k for k, o in enumerate(FORWARD) if o[2] == -1]
EX = [k for k, o in enumerate(FORWARD) if o[0] == 1]
F32 = jnp.float32
NS = jax.named_scope


def runs(ks):
    out = []
    for k in ks:
        if out and out[-1][1] == k:
            out[-1][1] = k + 1
        else:
            out.append([k, k + 1])
    return out


def splat(a, k):
    return jnp.broadcast_to(a[:, k : k + 1], (8, 128))


def line(a, k):
    return jnp.broadcast_to(a[k : k + 1, :], (8, 128))


def columns(a):
    return [splat(a, k) for k in range(8)]


def mm(cols, b):
    parts = [cols[k] * line(b, k) for k in range(8)]
    while len(parts) > 1:
        parts = [parts[i] + parts[i + 1] for i in range(0, len(parts), 2)]
    return parts[0]


def solve(cols, b, row):
    cols = list(cols)
    for k in range(8):
        factor = cols[k]
        inverse = 1.0 / line(factor, k)
        pivot = line(b, k) * inverse
        b = jnp.where(row == k, pivot, b - factor * pivot)
        for j in range(k + 1, 8):
            pivot = line(cols[j], k) * inverse
            cols[j] = jnp.where(row == k, pivot, cols[j] - factor * pivot)
    return b


def transposed(a, row, lane):
    out = jnp.zeros_like(a)
    for i in range(8):
        across = jnp.sum(jnp.where(lane == row, a[:, i : i + 1], 0.0), axis=0, keepdims=True)
        out = out + jnp.where(row == i, across, 0.0)
    return out


def main_kernel(sizes, dims, rhs, sten, q1_out, q2_out, c_out, p0, q0, w, ws, s0, diag, q2, scr,
                zsend, zrecv, esend, erecv, wzsend, wzrecv, ufull, uedge, uw, red, gacc, gsum, cur,
                slot_x, slot_y, slot_z, lsem, xs, xr, ars, arr):
    nf, nx, ny = dims
    yb_n = ny // 8
    tall = ny + 16
    per = 4 * yb_n
    pos = {a: lax.axis_index(a) for a in AXES}
    lane = lax.broadcasted_iota(jnp.int32, (8, 128), 1)
    row = lax.broadcasted_iota(jnp.int32, (8, 128), 0)
    first_lane = lane == 0
    last_lane = lane == 127
    rim = first_lane | last_lane
    even = lax.rem(lane, 2) == 0
    half_lane = lane // 2
    ys = pl.ds(8, ny)
    SHIFTED = LO + HI

    barrier = pltpu.get_barrier_semaphore()
    for a in AXES:
        for d in range(1, sizes[a]):
            pl.semaphore_signal(barrier, inc=1, device_id={a: lax.rem(pos[a] + d, sizes[a])},
                                device_id_type=pl.DeviceIdType.MESH)

    loads = [
        pltpu.make_async_copy(rhs, p0.at[:, pl.ds(1, nx), ys], lsem.at[0]),
        pltpu.make_async_copy(sten.at[pl.ds(1, 13)], w.at[:, pl.ds(1, nx), ys], lsem.at[1]),
        pltpu.make_async_copy(sten.at[0], s0, lsem.at[2]),
    ]
    for copy in loads:
        copy.start()

    last = {a: sizes[a] - 1 for a in AXES}

    @pl.when(pos["gx"] == 0)
    def _():
        for buf in (p0, q0):
            buf[:, 0, ys] = jnp.zeros((nf, ny, 128), F32)
        w[:, 0, ys] = jnp.zeros((13, ny, 128), F32)

    @pl.when(pos["gx"] == last["gx"])
    def _():
        for buf in (p0, q0):
            buf[:, nx + 1, ys] = jnp.zeros((nf, ny, 128), F32)

    def clear_y(y):
        def body(x, carry):
            for buf in (p0, q0):
                buf[:, x, y : y + 8] = jnp.zeros((nf, 8, 128), F32)
            return carry

        lax.fori_loop(0, nx + 2, body, 0)

        def body_w(x, carry):
            w[:, x, y : y + 8] = jnp.zeros((13, 8, 128), F32)
            return carry

        lax.fori_loop(0, nx + 1, body_w, 0)

    @pl.when(pos["gy"] == 0)
    def _():
        clear_y(0)

    @pl.when(pos["gy"] == last["gy"])
    def _():
        clear_y(ny + 8)

    for side, place in ((0, 0), (1, last["gz"])):
        @pl.when(pos["gz"] == place)
        def _():
            for e in range(2):
                zrecv[e, side] = jnp.zeros((nf + 1, 8, 128), F32)
                erecv[e, side] = jnp.zeros((2, 8, 128), F32)
            wzrecv[side] = jnp.zeros((len(LO), 8, 128), F32)

    zsend[...] = jnp.zeros(zsend.shape, F32)
    esend[...] = jnp.zeros(esend.shape, F32)
    wzsend[...] = jnp.zeros(wzsend.shape, F32)

    pl.semaphore_wait(barrier, sum(sizes[a] - 1 for a in AXES))

    count = [0]

    def shift(axis, up, src, dst):
        n = sizes[axis]
        i = pos[axis]
        slot = count[0]
        count[0] += 1
        copy = pltpu.make_async_remote_copy(
            src_ref=src, dst_ref=dst, send_sem=xs.at[slot], recv_sem=xr.at[slot],
            device_id={axis: lax.rem(i + (1 if up else n - 1), n)},
            device_id_type=pl.DeviceIdType.MESH)
        sends = i < n - 1 if up else i > 0
        gets = i > 0 if up else i < n - 1

        @pl.when(sends)
        def _():
            copy.start()

        def finish():
            @pl.when(sends)
            def _():
                copy.wait_send()

            @pl.when(gets)
            def _():
                copy.wait_recv()

        return finish

    def finish_all(items):
        for f in items:
            f()

    def y_faces(buf, start, length):
        xs_ = pl.ds(start, length)
        return [
            shift("gy", True, buf.at[:, xs_, pl.ds(ny, 8)], buf.at[:, xs_, pl.ds(0, 8)]),
            shift("gy", False, buf.at[:, xs_, pl.ds(8, 8)], buf.at[:, xs_, pl.ds(ny + 8, 8)]),
        ]

    def w_faces(start, length, edge):
        xs_ = pl.ds(start, length)
        out = []
        for b, up, src, dst in ((1, True, ny, 0), (-1, False, 8, ny + 8)):
            for lo, hi in runs([k for k, o in enumerate(FORWARD) if o[1] == b and (o[0] or not edge)]):
                ks = pl.ds(lo, hi - lo)
                out.append(shift("gy", up, w.at[ks, xs_, pl.ds(src, 8)], w.at[ks, xs_, pl.ds(dst, 8)]))
        return out

    def x_faces(buf):
        return [
            shift("gx", True, buf.at[:, nx, ys], buf.at[:, 0, ys]),
            shift("gx", False, buf.at[:, 1, ys], buf.at[:, nx + 1, ys]),
        ]

    def z_both(send, recv):
        return [
            shift("gz", True, send, recv.at[0]),
            shift("gz", False, send, recv.at[1]),
        ]

    def gram_body(accs, ub, vb):
        return [accs[i] + ub[i : i + 1] * vb[i:] for i in range(nf)]

    def gram_start():
        return tuple(jnp.zeros((nf - i, 8, 128), F32) for i in range(nf))

    def gram_end(g, accs):
        red[...] = jnp.zeros(red.shape, F32)
        for i in range(nf):
            red[i, i:nf, :] = jnp.sum(accs[i], axis=1)
        out = jnp.zeros((8, 128), F32)
        for i in range(nf):
            t = jnp.sum(red[i], axis=1, keepdims=True)
            out = out + jnp.where(lane == 8 * g + i, t, 0.0)
            across = jnp.sum(jnp.where(lane == 8 * g + row, t, 0.0), axis=0, keepdims=True)
            out = out + jnp.where((row == i) & (lane > 8 * g + i), across, 0.0)
        if g in (0, 3):
            gacc[...] = out
        else:
            gacc[...] += out

    def own(buf):
        return lambda x, yb: buf[:, x + 1, 8 + yb * 8 : 16 + yb * 8]

    def gram_plane(accs, u, v, x):
        for yb in range(yb_n):
            accs = gram_body(accs, u(x, yb), v(x, yb))
        return tuple(accs)

    def gram(g, u, v):
        gram_end(g, lax.fori_loop(0, nx, lambda x, accs: gram_plane(accs, u, v, x), gram_start()))

    def pack_w(x, carry):
        for yb in range(yb_n):
            j = x * yb_n + yb
            here = half_lane == j
            y = 8 + yb * 8
            for n, k in enumerate(LO):
                both = w[k, x + 1, y : y + 8]
                if n < len(HI):
                    both = jnp.where(first_lane, w[HI[n], x + 1, y : y + 8], both)
                pltpu.store(wzsend.at[n], pltpu.roll(both, 2 * j + 1, 1), mask=here)
        return carry

    def shift_w(x, carry):
        for yb in range(yb_n):
            y = 8 + yb * 8
            for n, k in enumerate(SHIFTED):
                ws[n, x, yb * 8 : yb * 8 + 8] = pltpu.roll(w[k, x + 1, y : y + 8], 1 if k in LO else 127, 1)
        return carry

    def insert_w(x, carry):
        for yb in range(yb_n):
            j = x * yb_n + yb
            for n in range(len(LO)):
                edge = pltpu.roll(uw[n], 127 - 2 * j, 1)
                pltpu.store(ws.at[n, x, yb * 8 : yb * 8 + 8], edge, mask=first_lane)
                if n < len(HI):
                    pltpu.store(ws.at[len(LO) + n, x, yb * 8 : yb * 8 + 8], edge, mask=last_lane)
        return carry

    def crossing(from_low, from_high):
        return jnp.where(even, pltpu.roll(from_high, 127, 1), pltpu.roll(from_low, 1, 1))

    def sums(buf, e, x):
        for yb in range(yb_n):
            y = 8 + yb * 8
            accs = {}
            back = {}
            for a in (-1, 0, 1):
                for b in (-1, 0, 1):
                    v = buf[:, x + 1 + a, y + b : y + b + 8]
                    for c in (-1, 0, 1):
                        o = (a, b, c)
                        if o == (0, 0, 0):
                            continue
                        if o > (0, 0, 0):
                            k = FORWARD.index(o)
                            if c == 0:
                                coef = w[k, x + 1, y : y + 8]
                            else:
                                coef = ws[SHIFTED.index(k), x, yb * 8 : yb * 8 + 8]
                        else:
                            k = FORWARD.index((-a, -b, -c))
                            coef = w[k, x + 1 + a, y + b : y + b + 8]
                            if e == 0:
                                back[c] = coef if c not in back else back[c] + coef
                        term = coef[None] * v
                        accs[c] = term if c not in accs else accs[c] + term
            if e == 0:
                total = s0[x, yb * 8 : yb * 8 + 8] + back[0]
                for k in range(13):
                    total = total + w[k, x + 1, y : y + 8]
                back[0] = total
            for c in (-1, 0, 1):
                scr[c + 1, yb, 0:nf] = accs[c]
                if e == 0:
                    scr[c + 1, yb, nf] = back[c]

    def settle(buf, e, x, put, where):
        for yb in range(yb_n):
            y = 8 + yb * 8
            j = x * yb_n + yb
            if where is None:
                here = half_lane == j
            if e == 0:
                up, down = scr[2, yb, nf], scr[0, yb, nf]
                total = scr[1, yb, nf] + pltpu.roll(up, 127, 1) + pltpu.roll(down, 1, 1)
                diag[x, yb * 8 : yb * 8 + 8] = total
                both = jnp.where(first_lane, up, down)
                if where is None:
                    pltpu.store(zsend.at[e, nf], pltpu.roll(both, 2 * j + 1, 1), mask=here)
                else:
                    m = where * yb_n + yb
                    pltpu.store(esend.at[e, 1], pltpu.roll(both, 2 * m + 1, 1), mask=half_lane == m)
            else:
                total = diag[x, yb * 8 : yb * 8 + 8]
            for f in range(nf):
                up, down = scr[2, yb, f], scr[0, yb, f]
                total_f = scr[1, yb, f] + pltpu.roll(up, 127, 1) + pltpu.roll(down, 1, 1)
                put(f, x, yb, total * buf[f, x + 1, y : y + 8] - total_f)
                both = jnp.where(first_lane, up, down)
                if where is None:
                    pltpu.store(zsend.at[e, f], pltpu.roll(both, 2 * j + 1, 1), mask=here)
                else:
                    m = f * (per // 2) + where * yb_n + yb
                    pltpu.store(esend.at[e, 0], pltpu.roll(both, (2 * m + 1) % 128, 1), mask=half_lane == m)

    def gather_full(e):
        for f in range(nf + 1 - e):
            mine = zsend[e, f]
            ufull[f] = crossing(zrecv[e, 0, f] - mine, zrecv[e, 1, f] - mine)

    def gather_edge(e):
        for n in range(2 - e):
            mine = esend[e, n]
            uedge[n] = crossing(erecv[e, 0, n] - mine, erecv[e, 1, n] - mine)

    def mend(buf, e, x, get, put, where):
        for yb in range(yb_n):
            y = 8 + yb * 8
            j = x * yb_n + yb
            if e == 0:
                if where is None:
                    extra = pltpu.roll(ufull[nf], 127 - 2 * j, 1)
                else:
                    extra = pltpu.roll(uedge[1], 127 - 2 * (where * yb_n + yb), 1)
                extra = jnp.where(rim, extra, 0.0)
                diag[x, yb * 8 : yb * 8 + 8] += extra
            for f in range(nf):
                if where is None:
                    edge = pltpu.roll(ufull[f], 127 - 2 * j, 1)
                else:
                    edge = pltpu.roll(uedge[0], 127 - 2 * (f * (per // 2) + where * yb_n + yb), 1)
                value = get(f, x, yb) - jnp.where(rim, edge, 0.0)
                if e == 0:
                    value = value + extra * buf[f, x + 1, y : y + 8]
                put(f, x, yb, value)

    all_slots = (slot_y, slot_x, slot_z)
    bases = [0]
    for a in ("gy", "gx"):
        bases.append(bases[-1] + sizes[a] - 1)

    def sum_start(r, stage, value):
        a = ("gy", "gx", "gz")[stage]
        slots = all_slots[stage]
        n = sizes[a]
        i = pos[a]
        cur[r, stage] = value
        slots[r, i] = value

        def copy(d, dst):
            m = bases[stage] + d - 1
            return pltpu.make_async_remote_copy(
                src_ref=cur.at[r, stage], dst_ref=slots.at[r, dst],
                send_sem=ars.at[r, m], recv_sem=arr.at[r, m],
                device_id={a: lax.rem(i + d, n)}, device_id_type=pl.DeviceIdType.MESH)

        for d in range(1, n):
            copy(d, i).start()

        def finish():
            for d in range(1, n):
                copy(d, i).wait_send()
                copy(d, lax.rem(i + n - d, n)).wait_recv()
            total = slots[r, 0]
            for q in range(1, n):
                total = total + slots[r, q]
            return total

        return finish

    k0, k1 = EX[0], EX[-1] + 1

    def put_q1(f, x, yb, v):
        q0[f, x + 1, 8 + yb * 8 : 16 + yb * 8] = v

    def get_q1(f, x, yb):
        return q0[f, x + 1, 8 + yb * 8 : 16 + yb * 8]

    def put_q2(f, x, yb, v):
        q2[f, x, yb * 8 : yb * 8 + 8] = v

    def get_q2(f, x, yb):
        return q2[f, x, yb * 8 : yb * 8 + 8]

    half = nx // 2

    def planes(buf, e, put, lo, hi):
        def body(x, carry):
            settle(buf, e, x - 1, put, None)
            sums(buf, e, x)
            return carry

        lax.fori_loop(lo, hi, body, 0)

    def operate(buf, e, put, across, hooks=()):
        with NS(f"op{e}_st1"):
            sums(buf, e, 1)
            planes(buf, e, put, 2, half)
        with NS(f"op{e}_xwait"):
            finish_all(across)
            ends = y_faces(buf, 0, 1) + y_faces(buf, nx + 1, 1)
            if e == 0:
                ends += w_faces(0, 1, True)
        if hooks:
            hooks[0]()
        with NS(f"op{e}_st2"):
            planes(buf, e, put, half, nx - 1)
        with NS(f"op{e}_ywait"):
            finish_all(ends)
        if hooks:
            hooks[1]()
        with NS(f"op{e}_st3"):
            settle(buf, e, nx - 2, put, None)
            sums(buf, e, 0)
            first = z_both(zsend.at[e, pl.ds(0, nf + 1 - e)], zrecv.at[e, :, pl.ds(0, nf + 1 - e)])
            settle(buf, e, 0, put, 0)
            sums(buf, e, nx - 1)
            settle(buf, e, nx - 1, put, 1)
            second = z_both(esend.at[e, pl.ds(0, 2 - e)], erecv.at[e, :, pl.ds(0, 2 - e)])
        return first, second

    with NS("a_load"):
        loads[0].wait()
        sides = y_faces(p0, 1, nx)
        phase = x_faces(p0)
        loads[1].wait()
        sides += w_faces(1, nx, False)
        phase.append(shift("gx", True, w.at[pl.ds(k0, k1 - k0), nx, ys], w.at[pl.ds(k0, k1 - k0), 0, ys]))
    with NS("a_packw"):
        lax.fori_loop(0, nx, pack_w, 0)
        zw = z_both(wzsend, wzrecv)
    with NS("a_gram0"):
        gram(0, own(p0), own(p0))
    with NS("a_shiftw"):
        lax.fori_loop(0, nx, shift_w, 0)
    with NS("a_zwait"):
        finish_all(zw)
    with NS("a_insw"):
        for n in range(len(LO)):
            uw[n] = crossing(wzrecv[0, n], wzrecv[1, n])
        lax.fori_loop(0, nx, insert_w, 0)
    with NS("a_ywait"):
        loads[2].wait()
        finish_all(sides)
    first, second = operate(p0, 0, put_q1, phase)

    def mend_gram(buf, e, get, put, u, v, accs):
        mend(buf, e, 1, get, put, None)

        def body(x, accs):
            accs = gram_plane(accs, u, v, x)
            mend(buf, e, x + 1, get, put, None)
            return accs

        return gram_plane(lax.fori_loop(1, nx - 2, body, accs), u, v, nx - 2)

    with NS("b_zwait1"):
        finish_all(first)
        gather_full(0)
    with NS("b_mend"):
        accs = mend_gram(p0, 0, get_q1, put_q1, own(p0), own(q0), gram_start())
    with NS("b_zwait2"):
        finish_all(second)
    with NS("b_mend2"):
        gather_edge(0)
        mend(p0, 0, 0, get_q1, put_q1, 0)
        mend(p0, 0, nx - 1, get_q1, put_q1, 1)
        phase = x_faces(q0)
        sides = y_faces(q0, 1, nx)
        save1 = pltpu.make_async_copy(q0.at[:, pl.ds(1, nx), ys], q1_out, lsem.at[3])
        save1.start()
    with NS("b_gram1"):
        accs = gram_plane(accs, own(p0), own(q0), 0)
        accs = gram_plane(accs, own(p0), own(q0), nx - 1)
        gram_end(1, accs)
    with NS("b_gram2"):
        gram(2, own(q0), own(q0))
        pending = [sum_start(0, 0, gacc[...])]
    with NS("b_ywait"):
        finish_all(sides)
        pending.append(sum_start(0, 1, pending[0]()))

    def hook_a():
        with NS("hook_a"):
            pending.append(sum_start(0, 2, pending[1]()))

    def hook_b():
        with NS("hook_b"):
            gsum[...] = pending[2]()

    first, second = operate(q0, 1, put_q2, phase, (hook_a, hook_b))

    def get_v2(x, yb):
        return q2[:, x, yb * 8 : yb * 8 + 8]

    with NS("c_zwait1"):
        finish_all(first)
        gather_full(1)
    with NS("c_mend"):
        accs = mend_gram(q0, 1, get_q2, put_q2, own(q0), get_v2, gram_start())

    with NS("c_alg1"):
        total = gsum[...]
        small = lane < 8
        rr, pq, ss = [jnp.where(small, pltpu.roll(total, (128 - 8 * g) % 128, 1), 0.0) for g in range(3)]
        pqc, rrc, ssc = columns(pq), columns(rr), columns(ss)
        alpha = jnp.where(small, solve(pqc, rr, row), 0.0)
        alpha_t = jnp.where(small, transposed(alpha, row, lane), 0.0)
        alpha_c, alpha_tc = columns(alpha), columns(alpha_t)
        ssa = mm(ssc, alpha)
        new = rr - mm(alpha_tc, pq) - mm(pqc, alpha) + mm(alpha_tc, ssa)
        beta = jnp.where(small, solve(rrc, new, row), 0.0)
        ib = beta + jnp.where(lane == row, 1.0, 0.0)
        ib_t = jnp.where(small, transposed(ib, row, lane), 0.0)
        left = mm(columns(ib_t), mm(pqc, ib) - ssa)
        mid = mm(ssc, ib)
        left = left - mm(alpha_tc, mid)
    with NS("c_zwait2"):
        finish_all(second)
    with NS("c_mend2"):
        gather_edge(1)
        mend(q0, 1, 0, get_q2, put_q2, 0)
        mend(q0, 1, nx - 1, get_q2, put_q2, 1)
        save2 = pltpu.make_async_copy(q2, q2_out, lsem.at[4])
        save2.start()
        accs = gram_plane(accs, own(q0), get_v2, 0)
        accs = gram_plane(accs, own(q0), get_v2, nx - 1)
        gram_end(3, accs)
    with NS("c_sum"):
        done = sum_start(1, 0, gacc[...])
        done = sum_start(1, 1, done())
        done = sum_start(1, 2, done())
        total = done()
    with NS("c_alg2"):
        tt = jnp.where(small, pltpu.roll(total, 128 - 24, 1), 0.0)
        curve = left + mm(alpha_tc, mm(columns(tt), alpha))
        alpha1 = jnp.where(small, solve(columns(curve), new, row), 0.0)
        c_out[0] = alpha + mm(columns(ib), alpha1)
        c_out[1] = mm(alpha_c, alpha1)
    with NS("c_end"):
        save1.wait()
        save2.wait()


def final_kernel(yb_n, xs_n, c, r0, q1, q2, sol, res, table):
    @pl.when(pl.program_id(0) == 0)
    def _():
        for n in range(2):
            for i in range(8):
                for j in range(8):
                    table[n, i, j] = jnp.full((8, 128), c[n, i, j], F32)

    def body(x, carry):
        for yb in range(yb_n):
            y = slice(yb * 8, yb * 8 + 8)
            s = jnp.zeros((8, 8, 128), F32)
            e = r0[:, x, y]
            for i in range(8):
                t1, t2 = table[0, i], table[1, i]
                a, b, d = r0[i, x, y][None], q1[i, x, y][None], q2[i, x, y][None]
                s = s + (t1 * a - t2 * b)
                e = e + (t2 * d - t1 * b)
            sol[:, x, y] = s
            res[:, x, y] = e
        return carry

    lax.fori_loop(0, xs_n, body, 0)


def shards(sizes, rhs, stencil):
    nf, nx, ny, nz = rhs.shape
    tall = ny + 16
    field = jax.ShapeDtypeStruct(rhs.shape, F32)
    anyspace = pl.BlockSpec(memory_space=pl.ANY)
    peers = sum(sizes[a] - 1 for a in AXES)
    padded = pltpu.VMEM((nf, nx + 2, tall, nz), F32)

    def kernel(*refs):
        main_kernel(sizes, (nf, nx, ny), *refs)

    q1, q2, c = pl.pallas_call(
        kernel,
        out_shape=(field, field, jax.ShapeDtypeStruct((2, 8, 128), F32)),
        in_specs=[anyspace, anyspace],
        out_specs=(anyspace, anyspace, pl.BlockSpec(memory_space=pltpu.VMEM)),
        scratch_shapes=[
            padded, padded,
            pltpu.VMEM((13, nx + 1, tall, nz), F32),
            pltpu.VMEM((len(LO) + len(HI), nx, ny, nz), F32),
            pltpu.VMEM((nx, ny, nz), F32),
            pltpu.VMEM((nx, ny, nz), F32),
            pltpu.VMEM((nf, nx, ny, nz), F32),
            pltpu.VMEM((3, ny // 8, nf + 1, 8, nz), F32),
            pltpu.VMEM((2, nf + 1, 8, nz), F32),
            pltpu.VMEM((2, 2, nf + 1, 8, nz), F32),
            pltpu.VMEM((2, 2, 8, nz), F32),
            pltpu.VMEM((2, 2, 2, 8, nz), F32),
            pltpu.VMEM((len(LO), 8, nz), F32),
            pltpu.VMEM((2, len(LO), 8, nz), F32),
            pltpu.VMEM((nf + 1, 8, nz), F32),
            pltpu.VMEM((2, 8, nz), F32),
            pltpu.VMEM((len(LO), 8, nz), F32),
            pltpu.VMEM((8, 8, 128), F32),
            pltpu.VMEM((8, 128), F32),
            pltpu.VMEM((8, 128), F32),
            pltpu.VMEM((2, 3, 8, 128), F32),
            pltpu.VMEM((2, sizes["gx"], 8, 128), F32),
            pltpu.VMEM((2, sizes["gy"], 8, 128), F32),
            pltpu.VMEM((2, sizes["gz"], 8, 128), F32),
            pltpu.SemaphoreType.DMA((5,)),
            pltpu.SemaphoreType.DMA((40,)),
            pltpu.SemaphoreType.DMA((40,)),
            pltpu.SemaphoreType.DMA((2, peers)),
            pltpu.SemaphoreType.DMA((2, peers)),
        ],
        compiler_params=pltpu.CompilerParams(
            collective_id=0, has_side_effects=True, vmem_limit_bytes=60 * 2**20),
        name="krylov",
    )(rhs, stencil)

    step = 2
    block = pl.BlockSpec((nf, step, ny, nz), lambda i: (0, i, 0, 0))

    def last(*refs):
        final_kernel(ny // 8, step, *refs)

    return pl.pallas_call(
        last,
        grid=(nx // step,),
        out_shape=(field, field),
        in_specs=[pl.BlockSpec(memory_space=pltpu.SMEM), block, block, block],
        out_specs=(block, block),
        scratch_shapes=[pltpu.VMEM((2, 8, 8, 8, 128), F32)],
        compiler_params=pltpu.CompilerParams(dimension_semantics=("arbitrary",), vmem_limit_bytes=60 * 2**20),
        name="combine",
    )(c, rhs, q1, q2)


def solution(mesh):
    sizes = {a: mesh.shape[a] for a in AXES}
    spec = P(None, "gx", "gy", "gz")

    def run(rhs, stencil):
        return shards(sizes, rhs, stencil)

    return jax.shard_map(run, mesh=mesh, in_specs=(spec, spec), out_specs=(spec, spec), check_vma=False)
```

```python
import jax
import jax.numpy as jnp
from jax import lax
from jax.experimental import pallas as pl
from jax.experimental.pallas import tpu as pltpu
from jax.sharding import PartitionSpec as P

FORWARD = [
    (a, b, c) for a in (-1, 0, 1) for b in (-1, 0, 1) for c in (-1, 0, 1) if (a, b, c) > (0, 0, 0)
]
AXES = ("gx", "gy", "gz")
LO = [k for k, o in enumerate(FORWARD) if o[2] == 1]
HI = [k for k, o in enumerate(FORWARD) if o[2] == -1]
EX = [k for k, o in enumerate(FORWARD) if o[0] == 1]
F32 = jnp.float32
NS = jax.named_scope


def runs(ks):
    out = []
    for k in ks:
        if out and out[-1][1] == k:
            out[-1][1] = k + 1
        else:
            out.append([k, k + 1])
    return out


def splat(a, k):
    return jnp.broadcast_to(a[:, k : k + 1], (8, 128))


def line(a, k):
    return jnp.broadcast_to(a[k : k + 1, :], (8, 128))


def columns(a):
    return [splat(a, k) for k in range(8)]


def mm(cols, b):
    parts = [cols[k] * line(b, k) for k in range(8)]
    while len(parts) > 1:
        parts = [parts[i] + parts[i + 1] for i in range(0, len(parts), 2)]
    return parts[0]


def solve(cols, b, row):
    cols = list(cols)
    for k in range(8):
        factor = cols[k]
        inverse = 1.0 / line(factor, k)
        pivot = line(b, k) * inverse
        b = jnp.where(row == k, pivot, b - factor * pivot)
        for j in range(k + 1, 8):
            pivot = line(cols[j], k) * inverse
            cols[j] = jnp.where(row == k, pivot, cols[j] - factor * pivot)
    return b


def transposed(a, row, lane):
    out = jnp.zeros_like(a)
    for i in range(8):
        across = jnp.sum(jnp.where(lane == row, a[:, i : i + 1], 0.0), axis=0, keepdims=True)
        out = out + jnp.where(row == i, across, 0.0)
    return out


def main_kernel(sizes, dims, rhs, sten, x1, r1, p1, s1, t_out, p0, q0, w, ws, s0, diag, q2, scr,
                zsend, zrecv, esend, erecv, wzsend, wzrecv, ufull, uedge, uw, red, held, gacc, cur, slots,
                t_alpha, t_beta, t_ib, lsem, xs, xr, ars, arr):
    nf, nx, ny = dims
    yb_n = ny // 8
    tall = ny + 16
    per = 4 * yb_n
    pos = {a: lax.axis_index(a) for a in AXES}
    lane = lax.broadcasted_iota(jnp.int32, (8, 128), 1)
    row = lax.broadcasted_iota(jnp.int32, (8, 128), 0)
    first_lane = lane == 0
    last_lane = lane == 127
    rim = first_lane | last_lane
    even = lax.rem(lane, 2) == 0
    half_lane = lane // 2
    ys = pl.ds(8, ny)
    SHIFTED = LO + HI

    devices = sizes["gx"] * sizes["gy"] * sizes["gz"]
    me = (pos["gx"] * sizes["gy"] + pos["gy"]) * sizes["gz"] + pos["gz"]

    loads = [
        pltpu.make_async_copy(rhs, p0.at[:, pl.ds(1, nx), ys], lsem.at[0]),
        pltpu.make_async_copy(sten.at[pl.ds(1, 13)], w.at[:, pl.ds(1, nx), ys], lsem.at[1]),
        pltpu.make_async_copy(sten.at[0], s0, lsem.at[2]),
    ]
    for copy in loads:
        copy.start()

    moved = {a: [lax.rem(pos[a] + d, sizes[a]) for d in range(sizes[a])] for a in AXES}
    offsets = [(i, j, k) for i in range(sizes["gx"]) for j in range(sizes["gy"]) for k in range(sizes["gz"])][1:]
    offsets.sort(key=lambda d: -sum(min(v, sizes[a] - v) for v, a in zip(d, AXES)))

    def peer(d):
        return {a: moved[a][v] for v, a in zip(d, AXES)}

    barrier = pltpu.get_barrier_semaphore()
    for d in offsets:
        pl.semaphore_signal(barrier, inc=1, device_id=peer(d), device_id_type=pl.DeviceIdType.MESH)

    last = {a: sizes[a] - 1 for a in AXES}

    @pl.when(pos["gx"] == 0)
    def _():
        for buf in (p0, q0):
            buf[:, 0, ys] = jnp.zeros((nf, ny, 128), F32)
        w[:, 0, ys] = jnp.zeros((13, ny, 128), F32)

    @pl.when(pos["gx"] == last["gx"])
    def _():
        for buf in (p0, q0):
            buf[:, nx + 1, ys] = jnp.zeros((nf, ny, 128), F32)

    def clear_y(y):
        def body(x, carry):
            for buf in (p0, q0):
                buf[:, x, y : y + 8] = jnp.zeros((nf, 8, 128), F32)
            return carry

        lax.fori_loop(0, nx + 2, body, 0)

        def body_w(x, carry):
            w[:, x, y : y + 8] = jnp.zeros((13, 8, 128), F32)
            return carry

        lax.fori_loop(0, nx + 1, body_w, 0)

    @pl.when(pos["gy"] == 0)
    def _():
        clear_y(0)

    @pl.when(pos["gy"] == last["gy"])
    def _():
        clear_y(ny + 8)

    for side, place in ((0, 0), (1, last["gz"])):
        @pl.when(pos["gz"] == place)
        def _():
            for e in range(2):
                for part in range(2):
                    zrecv[e, part, side] = jnp.zeros((nf + 1, 8, 128), F32)
                erecv[e, side] = jnp.zeros((2, 8, 128), F32)
            wzrecv[side] = jnp.zeros((len(LO), 8, 128), F32)

    zsend[...] = jnp.zeros(zsend.shape, F32)
    esend[...] = jnp.zeros(esend.shape, F32)
    wzsend[...] = jnp.zeros(wzsend.shape, F32)

    pl.semaphore_wait(barrier, devices - 1)

    count = [0]

    def shift(axis, up, src, dst):
        n = sizes[axis]
        i = pos[axis]
        slot = count[0]
        count[0] += 1
        copy = pltpu.make_async_remote_copy(
            src_ref=src, dst_ref=dst, send_sem=xs.at[slot], recv_sem=xr.at[slot],
            device_id={axis: lax.rem(i + (1 if up else n - 1), n)},
            device_id_type=pl.DeviceIdType.MESH)
        sends = i < n - 1 if up else i > 0
        gets = i > 0 if up else i < n - 1

        @pl.when(sends)
        def _():
            copy.start()

        def finish():
            @pl.when(sends)
            def _():
                copy.wait_send()

            @pl.when(gets)
            def _():
                copy.wait_recv()

        return finish

    def finish_all(items):
        for f in items:
            f()

    def y_faces(buf, start, length):
        xs_ = pl.ds(start, length)
        return [
            shift("gy", True, buf.at[:, xs_, pl.ds(ny, 8)], buf.at[:, xs_, pl.ds(0, 8)]),
            shift("gy", False, buf.at[:, xs_, pl.ds(8, 8)], buf.at[:, xs_, pl.ds(ny + 8, 8)]),
        ]

    def w_faces(start, length, edge):
        xs_ = pl.ds(start, length)
        out = []
        for b, up, src, dst in ((1, True, ny, 0), (-1, False, 8, ny + 8)):
            for lo, hi in runs([k for k, o in enumerate(FORWARD) if o[1] == b and (o[0] or not edge)]):
                ks = pl.ds(lo, hi - lo)
                out.append(shift("gy", up, w.at[ks, xs_, pl.ds(src, 8)], w.at[ks, xs_, pl.ds(dst, 8)]))
        return out

    def x_faces(buf):
        return [
            shift("gx", True, buf.at[:, nx, ys], buf.at[:, 0, ys]),
            shift("gx", False, buf.at[:, 1, ys], buf.at[:, nx + 1, ys]),
        ]

    def z_both(send, recv):
        return [
            shift("gz", True, send, recv.at[0]),
            shift("gz", False, send, recv.at[1]),
        ]

    def gram_body(accs, ub, vb):
        return [accs[i] + ub[i : i + 1] * vb[i:] for i in range(nf)]

    def gram_start():
        return tuple(jnp.zeros((nf - i, 8, 128), F32) for i in range(nf))

    def place(g, i, j):
        return 36 * g + 8 * i - i * (i - 1) // 2 + j - i

    def gram_end(g, accs):
        red[...] = jnp.zeros(red.shape, F32)
        for i in range(nf):
            red[i, i:nf, :] = jnp.sum(accs[i], axis=1)
        out = jnp.zeros((8, 128), F32)
        for i in range(nf):
            t = jnp.sum(red[i], axis=1, keepdims=True)
            out = out + jnp.where(lane == place(g, i, row), t, 0.0)
        return out

    def own(buf):
        return lambda x, yb: buf[:, x + 1, 8 + yb * 8 : 16 + yb * 8]

    def gram_plane(accs, u, v, x):
        for yb in range(yb_n):
            accs = gram_body(accs, u(x, yb), v(x, yb))
        return tuple(accs)

    def gram(g, u, v):
        return gram_end(g, lax.fori_loop(0, nx, lambda x, accs: gram_plane(accs, u, v, x), gram_start()))

    def several(n, f):
        def body(t, carry):
            for k in range(n):
                f(t * n + k, 0)
            return carry

        lax.fori_loop(0, nx // n, body, 0)

    def pack_w(x, carry):
        for yb in range(yb_n):
            j = x * yb_n + yb
            here = half_lane == j
            y = 8 + yb * 8
            for n, k in enumerate(LO):
                both = w[k, x + 1, y : y + 8]
                if n < len(HI):
                    both = jnp.where(first_lane, w[HI[n], x + 1, y : y + 8], both)
                pltpu.store(wzsend.at[n], pltpu.roll(both, 2 * j + 1, 1), mask=here)
        return carry

    def shift_w(x, carry):
        for yb in range(yb_n):
            y = 8 + yb * 8
            for n, k in enumerate(SHIFTED):
                ws[n, x, yb * 8 : yb * 8 + 8] = pltpu.roll(w[k, x + 1, y : y + 8], 1 if k in LO else 127, 1)
        return carry

    def insert_w(x, carry):
        for yb in range(yb_n):
            j = x * yb_n + yb
            for n in range(len(LO)):
                edge = pltpu.roll(uw[n], 127 - 2 * j, 1)
                pltpu.store(ws.at[n, x, yb * 8 : yb * 8 + 8], edge, mask=first_lane)
                if n < len(HI):
                    pltpu.store(ws.at[len(LO) + n, x, yb * 8 : yb * 8 + 8], edge, mask=last_lane)
        return carry

    def crossing(from_low, from_high):
        return jnp.where(even, pltpu.roll(from_high, 127, 1), pltpu.roll(from_low, 1, 1))

    def sums(buf, e, x):
        for yb in range(yb_n):
            y = 8 + yb * 8
            accs = {}
            back = {}
            for a in (-1, 0, 1):
                for b in (-1, 0, 1):
                    v = buf[:, x + 1 + a, y + b : y + b + 8]
                    for c in (-1, 0, 1):
                        o = (a, b, c)
                        if o == (0, 0, 0):
                            continue
                        if o > (0, 0, 0):
                            k = FORWARD.index(o)
                            if c == 0:
                                coef = w[k, x + 1, y : y + 8]
                            else:
                                coef = ws[SHIFTED.index(k), x, yb * 8 : yb * 8 + 8]
                        else:
                            k = FORWARD.index((-a, -b, -c))
                            coef = w[k, x + 1 + a, y + b : y + b + 8]
                            if e == 0:
                                back[c] = coef if c not in back else back[c] + coef
                        term = coef[None] * v
                        accs[c] = term if c not in accs else accs[c] + term
            if e == 0:
                total = s0[x, yb * 8 : yb * 8 + 8] + back[0]
                for k in range(13):
                    total = total + w[k, x + 1, y : y + 8]
                back[0] = total
            for c in (-1, 0, 1):
                scr[c + 1, yb, 0:nf] = accs[c]
                if e == 0:
                    scr[c + 1, yb, nf] = back[c]

    def settle(buf, e, x, put, chunk, where=0):
        for yb in range(yb_n):
            y = 8 + yb * 8
            j = x * yb_n + yb
            edge = where * yb_n + yb
            here = half_lane == j
            if e == 0:
                up, down = scr[2, yb, nf], scr[0, yb, nf]
                total = scr[1, yb, nf] + pltpu.roll(up, 127, 1) + pltpu.roll(down, 1, 1)
                diag[x, yb * 8 : yb * 8 + 8] = total
                both = jnp.where(first_lane, up, down)
                if chunk < 2:
                    pltpu.store(zsend.at[e, chunk, nf], pltpu.roll(both, 2 * j + 1, 1), mask=here)
                else:
                    pltpu.store(esend.at[e, 1], pltpu.roll(both, 2 * edge + 1, 1), mask=half_lane == edge)
            else:
                total = diag[x, yb * 8 : yb * 8 + 8]
            for f in range(nf):
                up, down = scr[2, yb, f], scr[0, yb, f]
                total_f = scr[1, yb, f] + pltpu.roll(up, 127, 1) + pltpu.roll(down, 1, 1)
                put(f, x, yb, total * buf[f, x + 1, y : y + 8] - total_f)
                both = jnp.where(first_lane, up, down)
                if chunk < 2:
                    pltpu.store(zsend.at[e, chunk, f], pltpu.roll(both, 2 * j + 1, 1), mask=here)
                else:
                    m = f * (per // 2) + edge
                    pltpu.store(esend.at[e, 0], pltpu.roll(both, (2 * m + 1) % 128, 1), mask=half_lane == m)

    def gather(e, chunk):
        send, recv = (zsend.at[e, chunk], zrecv.at[e, chunk]) if chunk < 2 else (esend.at[e], erecv.at[e])
        for n in range((nf if chunk < 2 else 1) + 1 - e):
            mine = send[n]
            crossed[chunk][n] = crossing(recv[0, n] - mine, recv[1, n] - mine)

    crossed = [ufull.at[0], ufull.at[1], uedge]

    def mend(buf, e, x, get, put, chunk, where=0):
        for yb in range(yb_n):
            y = 8 + yb * 8
            j = x * yb_n + yb
            edge = where * yb_n + yb
            if e == 0:
                if chunk < 2:
                    extra = pltpu.roll(ufull[chunk, nf], 127 - 2 * j, 1)
                else:
                    extra = pltpu.roll(uedge[1], 127 - 2 * edge, 1)
                extra = jnp.where(rim, extra, 0.0)
                diag[x, yb * 8 : yb * 8 + 8] += extra
            for f in range(nf):
                if chunk < 2:
                    side = pltpu.roll(ufull[chunk, f], 127 - 2 * j, 1)
                else:
                    side = pltpu.roll(uedge[0], 127 - 2 * (f * (per // 2) + edge), 1)
                value = get(f, x, yb) - jnp.where(rim, side, 0.0)
                if e == 0:
                    value = value + extra * buf[f, x + 1, y : y + 8]
                put(f, x, yb, value)

    def copy_row(r, n, dst):
        return pltpu.make_async_remote_copy(
            src_ref=cur.at[r], dst_ref=slots.at[r, dst], send_sem=ars.at[r, n], recv_sem=arr.at[r, n],
            device_id=peer(offsets[n]), device_id_type=pl.DeviceIdType.MESH)

    def sum_start(r, value):
        value = jnp.sum(value, axis=0, keepdims=True)
        cur[r] = value
        slots[r, me] = value
        for n in range(devices - 1):
            copy_row(r, n, me).start()

    def sum_end(r):
        for n, d in enumerate(offsets):
            source = [moved[a][(sizes[a] - v) % sizes[a]] for v, a in zip(d, AXES)]
            copy_row(r, n, me).wait_send()
            copy_row(r, n, (source[0] * sizes["gy"] + source[1]) * sizes["gz"] + source[2]).wait_recv()
        parts = [slots[r, q] for q in range(devices)]
        while len(parts) > 1:
            parts = [a + b for a, b in zip(parts[::2], parts[1::2])] + parts[len(parts) // 2 * 2 :]
        return jnp.broadcast_to(parts[0], (8, 128))

    def extract(total, g):
        cols = []
        for k in range(8):
            where = place(g, jnp.minimum(row, k), jnp.maximum(row, k))
            cols.append(jnp.broadcast_to(jnp.sum(jnp.where(lane == where, total, 0.0), axis=1, keepdims=True), (8, 128)))
        return cols

    def matrix(cols):
        out = jnp.zeros((8, 128), F32)
        for k in range(8):
            out = jnp.where(lane == k, cols[k], out)
        return out

    def fill(tab, cols):
        for j in range(8):
            for i in range(8):
                tab[i, j] = line(cols[j], i)

    k0, k1 = EX[0], EX[-1] + 1

    def put_q1(f, x, yb, v):
        q0[f, x + 1, 8 + yb * 8 : 16 + yb * 8] = v

    def get_q1(f, x, yb):
        return q0[f, x + 1, 8 + yb * 8 : 16 + yb * 8]

    def put_q2(f, x, yb, v):
        q2[f, x, yb * 8 : yb * 8 + 8] = v

    def get_q2(f, x, yb):
        return q2[f, x, yb * 8 : yb * 8 + 8]

    turn = nx - 4

    def planes(buf, e, put, lo, hi, chunk):
        def body(x, carry):
            settle(buf, e, x - 1, put, chunk)
            sums(buf, e, x)
            return carry

        lax.fori_loop(lo, hi, body, 0)

    def operate(buf, e, put, across):
        def z_send(chunk):
            part = pl.ds(0, nf + 1 - e)
            return z_both(zsend.at[e, chunk, part], zrecv.at[e, chunk, :, part])

        with NS(f"op{e}_st1"):
            sums(buf, e, 1)
            planes(buf, e, put, 2, turn, 0)
            sent = [z_send(0)]
        with NS(f"op{e}_xwait"):
            finish_all(across)
            ends = y_faces(buf, 0, 1) + y_faces(buf, nx + 1, 1)
            if e == 0:
                ends += w_faces(0, 1, True)
        with NS(f"op{e}_st2"):
            planes(buf, e, put, turn, nx - 1, 1)
        with NS(f"op{e}_ywait"):
            finish_all(ends)
        with NS(f"op{e}_st3"):
            settle(buf, e, nx - 2, put, 1)
            sums(buf, e, 0)
            sent.append(z_send(1))
            settle(buf, e, 0, put, 2, 0)
            sums(buf, e, nx - 1)
            settle(buf, e, nx - 1, put, 2, 1)
            sent.append(z_both(esend.at[e, pl.ds(0, 2 - e)], erecv.at[e, :, pl.ds(0, 2 - e)]))
        return sent

    with NS("a_load"):
        loads[0].wait()
        sides = y_faces(p0, 1, nx)
        phase = x_faces(p0)
        loads[1].wait()
        sides += w_faces(1, nx, False)
        phase.append(shift("gx", True, w.at[pl.ds(k0, k1 - k0), nx, ys], w.at[pl.ds(k0, k1 - k0), 0, ys]))
    with NS("a_packw"):
        several(8, pack_w)
        zw = z_both(wzsend, wzrecv)
    with NS("a_gram0"):
        gacc[...] = gram(0, own(p0), own(p0))
    with NS("a_shiftw"):
        several(4, shift_w)
    with NS("a_zwait"):
        finish_all(zw)
    with NS("a_insw"):
        for n in range(len(LO)):
            uw[n] = crossing(wzrecv[0, n], wzrecv[1, n])
        several(8, insert_w)
    with NS("a_ywait"):
        loads[2].wait()
        finish_all(sides)
    sent = operate(p0, 0, put_q1, phase)

    def mend_gram(buf, e, get, put, u, v, accs, lo, hi, chunk):
        mend(buf, e, lo, get, put, chunk)

        def body(x, accs):
            accs = gram_plane(accs, u, v, x)
            mend(buf, e, x + 1, get, put, chunk)
            return accs

        return gram_plane(lax.fori_loop(lo, hi - 1, body, accs), u, v, hi - 1)

    cut = turn - 1
    with NS("b_zwait1"):
        finish_all(sent[0])
        gather(0, 0)
    with NS("b_mend1"):
        accs = mend_gram(p0, 0, get_q1, put_q1, own(p0), own(q0), gram_start(), 1, cut, 0)
        sides = y_faces(q0, 2, cut - 1)
    with NS("b_zwait2"):
        finish_all(sent[1])
        gather(0, 1)
    with NS("b_mend2"):
        accs = mend_gram(p0, 0, get_q1, put_q1, own(p0), own(q0), accs, cut, nx - 1, 1)
    with NS("b_gram2a"):
        squares = lax.fori_loop(1, cut, lambda x, accs: gram_plane(accs, own(q0), own(q0), x), gram_start())
        for i in range(nf):
            held[i, i:nf] = squares[i]
    with NS("b_zwait3"):
        finish_all(sent[2])
        gather(0, 2)
    with NS("b_mend3"):
        mend(p0, 0, 0, get_q1, put_q1, 2, 0)
        mend(p0, 0, nx - 1, get_q1, put_q1, 2, 1)
        phase = x_faces(q0)
        sides += y_faces(q0, 1, 1) + y_faces(q0, cut + 1, nx - cut)
    with NS("b_gram1"):
        accs = gram_plane(accs, own(p0), own(q0), 0)
        accs = gram_plane(accs, own(p0), own(q0), nx - 1)
        gacc[...] += gram_end(1, accs)
    with NS("b_gram2"):
        squares = tuple(held[i, i:nf] for i in range(nf))
        squares = gram_plane(squares, own(q0), own(q0), 0)
        squares = lax.fori_loop(cut, nx, lambda x, accs: gram_plane(accs, own(q0), own(q0), x), squares)
        sum_start(0, gacc[...] + gram_end(2, squares))
    with NS("b_ywait"):
        finish_all(sides)

    sent = operate(q0, 1, put_q2, phase)

    def get_v2(x, yb):
        return q2[:, x, yb * 8 : yb * 8 + 8]

    with NS("c_sum1"):
        total = sum_end(0)
    with NS("c_alg1"):
        rrc, pqc, ssc = [extract(total, g) for g in range(3)]
        rr, pq = matrix(rrc), matrix(pqc)
        alpha = solve(pqc, rr, row)
        alpha_c = columns(alpha)
        fill(t_alpha, alpha_c)
        alpha_tc = columns(transposed(alpha, row, lane))
        ssa = mm(ssc, alpha)
        new = rr - mm(alpha_tc, pq) - mm(pqc, alpha) + mm(alpha_tc, ssa)
        beta = solve(rrc, new, row)
        fill(t_beta, columns(beta))
        ib = beta + jnp.where(lane == row, 1.0, 0.0)
        ib_tc = columns(transposed(ib, row, lane))
        fill(t_ib, columns(ib))
        left = mm(ib_tc, mm(pqc, ib) - ssa) - mm(alpha_tc, mm(ssc, ib))

    def early(x, carry):
        for yb in range(yb_n):
            y = slice(yb * 8, yb * 8 + 8)
            u, v = own(p0)(x, yb), own(q0)(x, yb)
            step, rest = t_alpha[0] * u[0][None], u
            for i in range(nf):
                if i:
                    step = step + t_alpha[i] * u[i][None]
                rest = rest - t_alpha[i] * v[i][None]
            x1[:, x, y] = step
            r1[:, x, y] = rest
        return carry

    def late(x, carry):
        for yb in range(yb_n):
            y = slice(yb * 8, yb * 8 + 8)
            u, v, z = own(p0)(x, yb), own(q0)(x, yb), get_v2(x, yb)
            step, image = r1[:, x, y], jnp.zeros((nf, 8, 128), F32)
            for i in range(nf):
                step = step + t_beta[i] * u[i][None]
                image = image + (t_ib[i] * v[i][None] - t_alpha[i] * z[i][None])
            p1[:, x, y] = step
            s1[:, x, y] = image
        return carry

    with NS("c_early"):
        lax.fori_loop(0, nx, early, 0)
    with NS("c_zwait"):
        for n in range(3):
            finish_all(sent[n])
            gather(1, n)
    with NS("c_mend"):
        accs = mend_gram(q0, 1, get_q2, put_q2, own(q0), get_v2, gram_start(), 1, cut, 0)
        accs = mend_gram(q0, 1, get_q2, put_q2, own(q0), get_v2, accs, cut, nx - 1, 1)
        mend(q0, 1, 0, get_q2, put_q2, 2, 0)
        mend(q0, 1, nx - 1, get_q2, put_q2, 2, 1)
        accs = gram_plane(accs, own(q0), get_v2, 0)
        accs = gram_plane(accs, own(q0), get_v2, nx - 1)
        sum_start(1, gram_end(0, accs))
    with NS("c_late"):
        lax.fori_loop(0, nx, late, 0)
    with NS("c_sum2"):
        total = sum_end(1)
    with NS("c_alg2"):
        curve = left + mm(alpha_tc, mm(extract(total, 0), alpha))
        fill(t_out, columns(solve(columns(curve), new, row)))


def final_kernel(dims, step, t, x1, r1, p1, s1, sol, res, sol_buf, res_buf, sem):
    nf, nx, ny = dims

    def saves(n):
        part = pl.ds(n * step, step)
        return [pltpu.make_async_copy(sol_buf.at[:, part], sol.at[:, part], sem.at[0, n]),
                pltpu.make_async_copy(res_buf.at[:, part], res.at[:, part], sem.at[1, n])]

    def body(n, carry):
        for k in range(step):
            x = n * step + k
            for yb in range(ny // 8):
                y = slice(yb * 8, yb * 8 + 8)
                u, v = p1[:, x, y], s1[:, x, y]
                s, e = x1[:, x, y], r1[:, x, y]
                for i in range(nf):
                    s = s + t[i] * u[i][None]
                    e = e - t[i] * v[i][None]
                sol_buf[:, x, y] = s
                res_buf[:, x, y] = e
        for copy in saves(n):
            copy.start()
        return carry

    lax.fori_loop(0, nx // step, body, 0)

    def end(n, carry):
        for copy in saves(n):
            copy.wait()
        return carry

    lax.fori_loop(0, nx // step, end, 0)


def shards(sizes, rhs, stencil):
    nf, nx, ny, nz = rhs.shape
    tall = ny + 16
    field = jax.ShapeDtypeStruct(rhs.shape, F32)
    kept = pltpu.VMEM(rhs.shape, F32)
    table = pltpu.VMEM((8, 8, 8, nz), F32)
    anyspace = pl.BlockSpec(memory_space=pl.ANY)
    local = pl.BlockSpec(memory_space=pltpu.VMEM)
    devices = sizes["gx"] * sizes["gy"] * sizes["gz"]
    padded = pltpu.VMEM((nf, nx + 2, tall, nz), F32)

    def kernel(*refs):
        main_kernel(sizes, (nf, nx, ny), *refs)

    x1, r1, p1, s1, t = pl.pallas_call(
        kernel,
        out_shape=(kept, kept, kept, kept, table),
        in_specs=[pl.BlockSpec(memory_space=pltpu.HBM)] * 2,
        out_specs=(local,) * 5,
        scratch_shapes=[
            padded, padded,
            pltpu.VMEM((13, nx + 1, tall, nz), F32),
            pltpu.VMEM((len(LO) + len(HI), nx, ny, nz), F32),
            pltpu.VMEM((nx, ny, nz), F32),
            pltpu.VMEM((nx, ny, nz), F32),
            pltpu.VMEM((nf, nx, ny, nz), F32),
            pltpu.VMEM((3, ny // 8, nf + 1, 8, nz), F32),
            pltpu.VMEM((2, 2, nf + 1, 8, nz), F32),
            pltpu.VMEM((2, 2, 2, nf + 1, 8, nz), F32),
            pltpu.VMEM((2, 2, 8, nz), F32),
            pltpu.VMEM((2, 2, 2, 8, nz), F32),
            pltpu.VMEM((len(LO), 8, nz), F32),
            pltpu.VMEM((2, len(LO), 8, nz), F32),
            pltpu.VMEM((2, nf + 1, 8, nz), F32),
            pltpu.VMEM((2, 8, nz), F32),
            pltpu.VMEM((len(LO), 8, nz), F32),
            pltpu.VMEM((8, 8, 128), F32),
            pltpu.VMEM((8, 8, 8, 128), F32),
            pltpu.VMEM((8, 128), F32),
            pltpu.VMEM((2, 1, 128), F32),
            pltpu.VMEM((2, devices, 1, 128), F32),
            table, table, table,
            pltpu.SemaphoreType.DMA((3,)),
            pltpu.SemaphoreType.DMA((64,)),
            pltpu.SemaphoreType.DMA((64,)),
            pltpu.SemaphoreType.DMA((2, devices - 1)),
            pltpu.SemaphoreType.DMA((2, devices - 1)),
        ],
        compiler_params=pltpu.CompilerParams(
            collective_id=0, has_side_effects=True, vmem_limit_bytes=40 * 2**20),
        name="krylov",
    )(*[pltpu.with_memory_space_constraint(v, pltpu.HBM) for v in (rhs, stencil)])

    step = 2

    def last(*refs):
        final_kernel((nf, nx, ny), step, *refs)

    return pl.pallas_call(
        last,
        out_shape=(field, field),
        in_specs=[local] * 5,
        out_specs=(pl.BlockSpec(memory_space=pltpu.HBM),) * 2,
        scratch_shapes=[
            pltpu.VMEM(rhs.shape, F32), pltpu.VMEM(rhs.shape, F32),
            pltpu.SemaphoreType.DMA((2, nx // step)),
        ],
        compiler_params=pltpu.CompilerParams(vmem_limit_bytes=40 * 2**20),
        name="combine",
    )(t, x1, r1, p1, s1)


def solution(mesh):
    sizes = {a: mesh.shape[a] for a in AXES}
    spec = P(None, "gx", "gy", "gz")

    def run(rhs, stencil):
        return shards(sizes, rhs, stencil)

    return jax.shard_map(run, mesh=mesh, in_specs=(spec, spec), out_specs=(spec, spec), check_vma=False)
```

```python
import jax
import jax.numpy as jnp
from jax import lax
from jax.experimental import pallas as pl
from jax.experimental.pallas import tpu as pltpu
from jax.sharding import PartitionSpec as P

FORWARD = [
    (a, b, c) for a in (-1, 0, 1) for b in (-1, 0, 1) for c in (-1, 0, 1) if (a, b, c) > (0, 0, 0)
]
AXES = ("gx", "gy", "gz")
LO = [k for k, o in enumerate(FORWARD) if o[2] == 1]
HI = [k for k, o in enumerate(FORWARD) if o[2] == -1]
F32 = jnp.float32
NS = jax.named_scope


def runs(ks):
    out = []
    for k in ks:
        if out and out[-1][1] == k:
            out[-1][1] = k + 1
        else:
            out.append([k, k + 1])
    return out


def splat(a, k):
    return jnp.broadcast_to(a[:, k : k + 1], (8, 128))


def line(a, k):
    return jnp.broadcast_to(a[k : k + 1, :], (8, 128))


def columns(a):
    return [splat(a, k) for k in range(8)]


def mm(cols, b):
    parts = [cols[k] * line(b, k) for k in range(8)]
    while len(parts) > 1:
        parts = [parts[i] + parts[i + 1] for i in range(0, len(parts), 2)]
    return parts[0]


def solve(cols, b, row):
    cols = list(cols)
    for k in range(8):
        factor = cols[k]
        inverse = 1.0 / line(factor, k)
        pivot = line(b, k) * inverse
        b = jnp.where(row == k, pivot, b - factor * pivot)
        for j in range(k + 1, 8):
            pivot = line(cols[j], k) * inverse
            cols[j] = jnp.where(row == k, pivot, cols[j] - factor * pivot)
    return b


def transposed(a, row, lane):
    out = jnp.zeros_like(a)
    for i in range(8):
        across = jnp.sum(jnp.where(lane == row, a[:, i : i + 1], 0.0), axis=0, keepdims=True)
        out = out + jnp.where(row == i, across, 0.0)
    return out


def main_kernel(sizes, dims, rhs, sten, x1, r1, p1, s1, t_out, p0, q0, w, ws, s0, diag, q2, scr,
                xsend, xrecv, xpsend, xprecv, zsend, zrecv, wzsend, wzrecv, ucross, uw, red, held, gacc, cur, slots,
                t_alpha, t_beta, t_ib, lsem, xs, xr, ars, arr):
    nf, nx, ny = dims
    yb_n = ny // 8
    tall = ny + 16
    group = 128 // (8 * yb_n)
    deep = 4
    wide = deep * yb_n
    chunks = nx // deep
    pos = {a: lax.axis_index(a) for a in AXES}
    lane = lax.broadcasted_iota(jnp.int32, (8, 128), 1)
    row = lax.broadcasted_iota(jnp.int32, (8, 128), 0)
    first_lane = lane == 0
    last_lane = lane == 127
    rim = first_lane | last_lane
    even = lax.rem(lane, 2) == 0
    half_lane = lane // 2
    ys = pl.ds(8, ny)
    SHIFTED = LO + HI

    devices = sizes["gx"] * sizes["gy"] * sizes["gz"]
    me = (pos["gx"] * sizes["gy"] + pos["gy"]) * sizes["gz"] + pos["gz"]

    loads = [
        pltpu.make_async_copy(rhs, p0.at[:, pl.ds(1, nx), ys], lsem.at[0]),
        pltpu.make_async_copy(sten.at[pl.ds(1, 13)], w.at[:, pl.ds(1, nx), ys], lsem.at[1]),
        pltpu.make_async_copy(sten.at[0], s0, lsem.at[2]),
    ]
    loads[1].start()
    loads[2].start()

    moved = {a: [lax.rem(pos[a] + d, sizes[a]) for d in range(sizes[a])] for a in AXES}
    offsets = [(i, j, k) for i in range(sizes["gx"]) for j in range(sizes["gy"]) for k in range(sizes["gz"])][1:]
    offsets.sort(key=lambda d: -sum(min(v, sizes[a] - v) for v, a in zip(d, AXES)))

    def peer(d):
        return {a: moved[a][v] for v, a in zip(d, AXES)}

    barrier = pltpu.get_barrier_semaphore()
    for d in offsets:
        pl.semaphore_signal(barrier, inc=1, device_id=peer(d), device_id_type=pl.DeviceIdType.MESH)

    last = {a: sizes[a] - 1 for a in AXES}

    @pl.when(pos["gx"] == 0)
    def _():
        xrecv[...] = jnp.zeros(xrecv.shape, F32)
        xprecv[...] = jnp.zeros(xprecv.shape, F32)

    loads[0].start()

    @pl.when(pos["gx"] == last["gx"])
    def _():
        for buf in (p0, q0):
            buf[:, nx + 1, ys] = jnp.zeros((nf, ny, 128), F32)

    def clear_y(y):
        def body(x, carry):
            for buf in (p0, q0):
                buf[:, x, y : y + 8] = jnp.zeros((nf, 8, 128), F32)
            return carry

        lax.fori_loop(1, nx + 2, body, 0)

        def body_w(x, carry):
            w[:, x, y : y + 8] = jnp.zeros((13, 8, 128), F32)
            return carry

        lax.fori_loop(1, nx + 1, body_w, 0)

    @pl.when(pos["gy"] == 0)
    def _():
        clear_y(0)

    @pl.when(pos["gy"] == last["gy"])
    def _():
        clear_y(ny + 8)

    for side, place in ((0, 0), (1, last["gz"])):
        @pl.when(pos["gz"] == place)
        def _():
            for e in range(2):
                for n in range(chunks):
                    zrecv[e, n, side] = jnp.zeros(zrecv.shape[3:], F32)
            wzrecv[side] = jnp.zeros((len(LO), 8, 128), F32)

    zsend[...] = jnp.zeros(zsend.shape, F32)
    xpsend[...] = jnp.zeros(xpsend.shape, F32)
    wzsend[...] = jnp.zeros(wzsend.shape, F32)

    pl.semaphore_wait(barrier, devices - 1)

    count = [0]

    def shift(axis, up, src, dst):
        n = sizes[axis]
        i = pos[axis]
        slot = count[0]
        count[0] += 1
        copy = pltpu.make_async_remote_copy(
            src_ref=src, dst_ref=dst, send_sem=xs.at[slot], recv_sem=xr.at[slot],
            device_id={axis: lax.rem(i + (1 if up else n - 1), n)},
            device_id_type=pl.DeviceIdType.MESH)
        sends = i < n - 1 if up else i > 0
        gets = i > 0 if up else i < n - 1

        @pl.when(sends)
        def _():
            copy.start()

        def finish():
            @pl.when(sends)
            def _():
                copy.wait_send()

            @pl.when(gets)
            def _():
                copy.wait_recv()

        return finish

    def finish_all(items):
        for f in items:
            f()

    def y_faces(buf, start, length):
        xs_ = pl.ds(start, length)
        return [
            shift("gy", True, buf.at[:, xs_, pl.ds(ny, 8)], buf.at[:, xs_, pl.ds(0, 8)]),
            shift("gy", False, buf.at[:, xs_, pl.ds(8, 8)], buf.at[:, xs_, pl.ds(ny + 8, 8)]),
        ]

    def w_faces(start, length):
        xs_ = pl.ds(start, length)
        out = []
        for b, up, src, dst in ((1, True, ny, 0), (-1, False, 8, ny + 8)):
            for lo, hi in runs([k for k, o in enumerate(FORWARD) if o[1] == b]):
                ks = pl.ds(lo, hi - lo)
                out.append(shift("gy", up, w.at[ks, xs_, pl.ds(src, 8)], w.at[ks, xs_, pl.ds(dst, 8)]))
        return out

    def x_down(buf):
        return [shift("gx", False, buf.at[:, 1, ys], buf.at[:, nx + 1, ys])]

    def x_up(e):
        part = pl.ds(0, nf + 1 - e)
        return [shift("gx", True, xsend.at[e, part], xrecv.at[e, part]), shift("gx", True, xpsend.at[e, pl.ds(0, packs(e))], xprecv.at[e, pl.ds(0, packs(e))])]

    def z_both(send, recv):
        return [
            shift("gz", True, send, recv.at[0]),
            shift("gz", False, send, recv.at[1]),
        ]

    def gram_body(accs, ub, vb):
        return [accs[i] + ub[i : i + 1] * vb[i:] for i in range(nf)]

    def gram_start():
        return tuple(jnp.zeros((nf - i, 8, 128), F32) for i in range(nf))

    def place(g, i, j):
        return 36 * g + 8 * i - i * (i - 1) // 2 + j - i

    def gram_end(g, accs):
        red[...] = jnp.zeros(red.shape, F32)
        for i in range(nf):
            red[i, i:nf, :] = jnp.sum(accs[i], axis=1)
        out = jnp.zeros((8, 128), F32)
        for i in range(nf):
            t = jnp.sum(red[i], axis=1, keepdims=True)
            out = out + jnp.where(lane == place(g, i, row), t, 0.0)
        return out

    def own(buf):
        return lambda x, yb: buf[:, x + 1, 8 + yb * 8 : 16 + yb * 8]

    def gram_plane(accs, u, v, x):
        for yb in range(yb_n):
            accs = gram_body(accs, u(x, yb), v(x, yb))
        return tuple(accs)

    def gram(g, u, v):
        return gram_end(g, lax.fori_loop(0, nx, lambda x, accs: gram_plane(accs, u, v, x), gram_start()))

    def several(n, f):
        def body(t, carry):
            for k in range(n):
                f(t * n + k, 0)
            return carry

        lax.fori_loop(0, nx // n, body, 0)

    def pack_w(x, carry):
        for yb in range(yb_n):
            j = x * yb_n + yb
            here = half_lane == j
            y = 8 + yb * 8
            for n, k in enumerate(LO):
                both = w[k, x + 1, y : y + 8]
                if n < len(HI):
                    both = jnp.where(first_lane, w[HI[n], x + 1, y : y + 8], both)
                pltpu.store(wzsend.at[n], pltpu.roll(both, 2 * j + 1, 1), mask=here)
        return carry

    def shift_w(x, carry):
        for yb in range(yb_n):
            y = 8 + yb * 8
            for n, k in enumerate(SHIFTED):
                ws[n, x, yb * 8 : yb * 8 + 8] = pltpu.roll(w[k, x + 1, y : y + 8], 1 if k in LO else 127, 1)
        return carry

    def insert_w(x, carry):
        for yb in range(yb_n):
            j = x * yb_n + yb
            for n in range(len(LO)):
                edge = pltpu.roll(uw[n], 127 - 2 * j, 1)
                pltpu.store(ws.at[n, x, yb * 8 : yb * 8 + 8], edge, mask=first_lane)
                if n < len(HI):
                    pltpu.store(ws.at[len(LO) + n, x, yb * 8 : yb * 8 + 8], edge, mask=last_lane)
        return carry

    def crossing(from_low, from_high):
        return jnp.where(even, pltpu.roll(from_high, 127, 1), pltpu.roll(from_low, 1, 1))

    def pack_z(out, f, both, m):
        m = f % group * wide + m
        pltpu.store(out.at[f // group], pltpu.roll(both, lax.rem(2 * m + 1, 128), 1), mask=half_lane == m)

    def upward(buf, e):
        for yb in range(yb_n):
            y = 8 + yb * 8
            accs = {}
            back = {}
            for b in (-1, 0, 1):
                v = buf[:, nx, y + b : y + b + 8]
                for c in (-1, 0, 1):
                    coef = w[FORWARD.index((1, -b, -c)), nx, y + b : y + b + 8]
                    term = coef[None] * v
                    accs[c] = term if c not in accs else accs[c] + term
                    back[c] = coef if c not in back else back[c] + coef
            xsend[e, 0:nf, yb * 8 : yb * 8 + 8] = (
                accs[0] + pltpu.roll(accs[1], 127, 2) + pltpu.roll(accs[-1], 1, 2))
            both = jnp.where(first_lane[None], accs[1], accs[-1])
            for f in range(nf):
                pack_z(xpsend.at[e], f, both[f], (deep - 1) * yb_n + yb)
            if e == 0:
                xsend[e, nf, yb * 8 : yb * 8 + 8] = (
                    back[0] + pltpu.roll(back[1], 127, 1) + pltpu.roll(back[-1], 1, 1))
                both = jnp.where(first_lane, back[1], back[-1])
                pack_z(xpsend.at[e], nf, both, (deep - 1) * yb_n + yb)

    def sums(buf, e, x, lowest=False):
        for yb in range(yb_n):
            y = 8 + yb * 8
            accs = {}
            back = {}
            if lowest:
                accs[0] = xrecv[e, 0:nf, yb * 8 : yb * 8 + 8]
                if e == 0:
                    back[0] = xrecv[e, nf, yb * 8 : yb * 8 + 8]
            for a in (0, 1) if lowest else (-1, 0, 1):
                for b in (-1, 0, 1):
                    v = buf[:, x + 1 + a, y + b : y + b + 8]
                    for c in (-1, 0, 1):
                        o = (a, b, c)
                        if o == (0, 0, 0):
                            continue
                        if o > (0, 0, 0):
                            k = FORWARD.index(o)
                            if c == 0:
                                coef = w[k, x + 1, y : y + 8]
                            else:
                                coef = ws[SHIFTED.index(k), x, yb * 8 : yb * 8 + 8]
                        else:
                            k = FORWARD.index((-a, -b, -c))
                            coef = w[k, x + 1 + a, y + b : y + b + 8]
                            if e == 0:
                                back[c] = coef if c not in back else back[c] + coef
                        term = coef[None] * v
                        accs[c] = term if c not in accs else accs[c] + term
            if e == 0:
                total = s0[x, yb * 8 : yb * 8 + 8] + back[0]
                for k in range(13):
                    total = total + w[k, x + 1, y : y + 8]
                back[0] = total
            for c in (-1, 0, 1):
                scr[c + 1, yb, 0:nf] = accs[c]
                if e == 0:
                    scr[c + 1, yb, nf] = back[c]

    def settle(buf, e, x, put, chunk, where):
        for yb in range(yb_n):
            y = 8 + yb * 8
            m = where * yb_n + yb
            if e == 0:
                up, down = scr[2, yb, nf], scr[0, yb, nf]
                total = scr[1, yb, nf] + pltpu.roll(up, 127, 1) + pltpu.roll(down, 1, 1)
                diag[x, yb * 8 : yb * 8 + 8] = total
                pack_z(zsend.at[e, chunk], nf, jnp.where(first_lane, up, down), m)
            else:
                total = diag[x, yb * 8 : yb * 8 + 8]
            for f in range(nf):
                up, down = scr[2, yb, f], scr[0, yb, f]
                total_f = scr[1, yb, f] + pltpu.roll(up, 127, 1) + pltpu.roll(down, 1, 1)
                put(f, x, yb, total * buf[f, x + 1, y : y + 8] - total_f)
                pack_z(zsend.at[e, chunk], f, jnp.where(first_lane, up, down), m)

    def gather(e, chunk):
        for n in range(packs(e)):
            mine = zsend[e, chunk, n]
            ucross[chunk, n] = crossing(zrecv[e, chunk, 0, n] - mine, zrecv[e, chunk, 1, n] - mine)

    def packs(e):
        return (nf - e) // group + 1

    def mend(buf, e, x, get, put, chunk, where):
        for yb in range(yb_n):
            y = 8 + yb * 8
            m = where * yb_n + yb

            def edge(f):
                place = f % group * wide + m
                side = pltpu.roll(ucross[chunk, f // group], lax.rem(255 - 2 * place, 128), 1)
                return jnp.where(rim, side, 0.0)

            if e == 0:
                extra = edge(nf)
                diag[x, yb * 8 : yb * 8 + 8] += extra
            for f in range(nf):
                value = get(f, x, yb) - edge(f)
                if e == 0:
                    value = value + extra * buf[f, x + 1, y : y + 8]
                put(f, x, yb, value)

    def copy_row(r, n, dst):
        return pltpu.make_async_remote_copy(
            src_ref=cur.at[r], dst_ref=slots.at[r, dst], send_sem=ars.at[r, n], recv_sem=arr.at[r, n],
            device_id=peer(offsets[n]), device_id_type=pl.DeviceIdType.MESH)

    def sum_start(r, value):
        value = jnp.sum(value, axis=0, keepdims=True)
        cur[r] = value
        slots[r, me] = value
        for n in range(devices - 1):
            copy_row(r, n, me).start()

    def sum_end(r):
        for n, d in enumerate(offsets):
            source = [moved[a][(sizes[a] - v) % sizes[a]] for v, a in zip(d, AXES)]
            copy_row(r, n, me).wait_send()
            copy_row(r, n, (source[0] * sizes["gy"] + source[1]) * sizes["gz"] + source[2]).wait_recv()
        parts = [slots[r, q] for q in range(devices)]
        while len(parts) > 1:
            parts = [a + b for a, b in zip(parts[::2], parts[1::2])] + parts[len(parts) // 2 * 2 :]
        return jnp.broadcast_to(parts[0], (8, 128))

    def extract(total, g):
        cols = []
        for k in range(8):
            where = place(g, jnp.minimum(row, k), jnp.maximum(row, k))
            cols.append(jnp.broadcast_to(jnp.sum(jnp.where(lane == where, total, 0.0), axis=1, keepdims=True), (8, 128)))
        return cols

    def matrix(cols):
        out = jnp.zeros((8, 128), F32)
        for k in range(8):
            out = jnp.where(lane == k, cols[k], out)
        return out

    def fill(tab, cols):
        for j in range(8):
            for i in range(8):
                tab[i, j] = line(cols[j], i)

    def put_q1(f, x, yb, v):
        q0[f, x + 1, 8 + yb * 8 : 16 + yb * 8] = v

    def get_q1(f, x, yb):
        return q0[f, x + 1, 8 + yb * 8 : 16 + yb * 8]

    def put_q2(f, x, yb, v):
        q2[f, x, yb * 8 : yb * 8 + 8] = v

    def get_q2(f, x, yb):
        return q2[f, x, yb * 8 : yb * 8 + 8]

    def z_send(e, chunk):
        part = pl.ds(0, packs(e))
        return z_both(zsend.at[e, chunk, part], zrecv.at[e, chunk, :, part])

    def planes(buf, e, put, chunk):
        def body(t, carry):
            x = chunk * deep + 2 + t
            settle(buf, e, x - 1, put, chunk, t)
            sums(buf, e, x)
            return carry

        lax.fori_loop(0, deep, body, 0)
        return z_send(e, chunk)

    end = chunks - 1

    def interior(buf, e, put, across=None):
        sent = []
        ends = None
        sums(buf, e, 1)
        for n in range(end):
            with NS(f"op{e}_in{n}"):
                sent.append(planes(buf, e, put, n))
            if across and n == end - 2:
                ends = arrive(buf, e, across)
        with NS(f"op{e}_in{end}"):
            settle(buf, e, nx - 3, put, end, 0)
            sums(buf, e, nx - 2)
            settle(buf, e, nx - 2, put, end, 1)
        return sent, ends

    def arrive(buf, e, across):
        with NS(f"op{e}_xwait"):
            finish_all(across)
            return y_faces(buf, nx + 1, 1)

    def outer(buf, e, put, ends, across):
        with NS(f"op{e}_ywait"):
            finish_all(ends)
        with NS(f"op{e}_st3"):
            sums(buf, e, nx - 1)
            settle(buf, e, nx - 1, put, end, 2)
        with NS(f"op{e}_upwait"):
            finish_all(across)
        with NS(f"op{e}_st4"):
            sums(buf, e, 0, True)
            settle(buf, e, 0, put, end, 3)
            for n in range(packs(e)):
                zsend[e, end, n] += xprecv[e, n]
            return z_send(e, end)

    def mend_gram(buf, e, get, put, u, v, accs, chunk):
        lo = chunk * deep + 1
        mend(buf, e, lo, get, put, chunk, 0)

        def body(t, accs):
            accs = gram_plane(accs, u, v, lo + t)
            mend(buf, e, lo + t + 1, get, put, chunk, t + 1)
            return accs

        return gram_plane(lax.fori_loop(0, deep - 1, body, accs), u, v, lo + deep - 1)

    def mend_end(buf, e, get, put, between=None):
        for where, x in ((2, nx - 1), (3, 0), (0, nx - 3), (1, nx - 2)):
            mend(buf, e, x, get, put, end, where)
            if between and where == 2:
                between()

    rest = (nx - 1, 0, nx - 3, nx - 2)

    with NS("a_loadw"):
        loads[1].wait()
        rims = w_faces(nx, 1)
    with NS("a_packw"):
        several(8, pack_w)
        zw = z_both(wzsend, wzrecv)
    with NS("a_loadp"):
        loads[0].wait()
        rims += y_faces(p0, nx, 1)
        down = x_down(p0)
        sides = y_faces(p0, 1, nx - 1) + w_faces(1, nx - 1)
    with NS("a_gram0"):
        gacc[...] = gram(0, own(p0), own(p0))
    with NS("a_up"):
        finish_all(rims)
        upward(p0, 0)
        up = x_up(0)
    with NS("a_shiftw"):
        several(4, shift_w)
    with NS("a_zwait"):
        finish_all(zw)
    with NS("a_insw"):
        for n in range(len(LO)):
            uw[n] = crossing(wzrecv[0, n], wzrecv[1, n])
        several(8, insert_w)
    with NS("a_ywait"):
        loads[2].wait()
        finish_all(sides)
    sent, ends = interior(p0, 0, put_q1, down)
    sent.append(outer(p0, 0, put_q1, ends, up))

    accs = gram_start()
    sides = []
    for n in range(end):
        with NS(f"b_zwait{n}"):
            finish_all(sent[n])
            gather(0, n)
        with NS(f"b_mend{n}"):
            accs = mend_gram(p0, 0, get_q1, put_q1, own(p0), own(q0), accs, n)
            sides += y_faces(q0, n * deep + 2, deep)
    with NS(f"b_zwait{end}"):
        finish_all(sent[end])
        gather(0, end)
    rims = []
    with NS(f"b_mend{end}"):
        mend_end(p0, 0, get_q1, put_q1, lambda: rims.extend(y_faces(q0, nx, 1)))
        sides += y_faces(q0, 1, 1) + y_faces(q0, nx - 2, 2)
    with NS("b_gram1"):
        for x in rest:
            accs = gram_plane(accs, own(p0), own(q0), x)
        gacc[...] += gram_end(1, accs)
    with NS("b_gram2a"):
        down = x_down(q0)
        squares = lax.fori_loop(1, nx, lambda x, accs: gram_plane(accs, own(q0), own(q0), x), gram_start())
        for i in range(nf):
            held[i, i:nf] = squares[i]
    with NS("b_up"):
        finish_all(rims)
        upward(q0, 1)
        up = x_up(1)
    with NS("b_gram2"):
        squares = tuple(held[i, i:nf] for i in range(nf))
        squares = gram_plane(squares, own(q0), own(q0), 0)
        sum_start(0, gacc[...] + gram_end(2, squares))
    with NS("b_ywait"):
        finish_all(sides)

    sent, ends = interior(q0, 1, put_q2)

    def get_v2(x, yb):
        return q2[:, x, yb * 8 : yb * 8 + 8]

    with NS("c_sum1"):
        total = sum_end(0)
    with NS("c_alg1"):
        rrc, pqc, ssc = [extract(total, g) for g in range(3)]
        rr, pq = matrix(rrc), matrix(pqc)
        alpha = solve(pqc, rr, row)
        alpha_c = columns(alpha)
        fill(t_alpha, alpha_c)
        alpha_tc = columns(transposed(alpha, row, lane))
        ssa = mm(ssc, alpha)
        new = rr - mm(alpha_tc, pq) - mm(pqc, alpha) + mm(alpha_tc, ssa)
        beta = solve(rrc, new, row)
        fill(t_beta, columns(beta))
        ib = beta + jnp.where(lane == row, 1.0, 0.0)
        ib_tc = columns(transposed(ib, row, lane))
        fill(t_ib, columns(ib))
        left = mm(ib_tc, mm(pqc, ib) - ssa) - mm(alpha_tc, mm(ssc, ib))

    def early(x, carry):
        for yb in range(yb_n):
            y = slice(yb * 8, yb * 8 + 8)
            u, v = own(p0)(x, yb), own(q0)(x, yb)
            step, rest = t_alpha[0] * u[0][None], u
            for i in range(nf):
                if i:
                    step = step + t_alpha[i] * u[i][None]
                rest = rest - t_alpha[i] * v[i][None]
            x1[:, x, y] = step
            r1[:, x, y] = rest
        return carry

    def late(x, carry):
        for yb in range(yb_n):
            y = slice(yb * 8, yb * 8 + 8)
            u, v, z = own(p0)(x, yb), own(q0)(x, yb), get_v2(x, yb)
            step, image = r1[:, x, y], jnp.zeros((nf, 8, 128), F32)
            for i in range(nf):
                step = step + t_beta[i] * u[i][None]
                image = image + (t_ib[i] * v[i][None] - t_alpha[i] * z[i][None])
            p1[:, x, y] = step
            s1[:, x, y] = image
        return carry

    split = nx // 4
    ends = arrive(q0, 1, down)
    with NS("c_early"):
        lax.fori_loop(0, split, early, 0)
    sent.append(outer(q0, 1, put_q2, ends, up))
    accs = gram_start()
    for n in range(end):
        with NS(f"c_zwait{n}"):
            finish_all(sent[n])
            gather(1, n)
        with NS(f"c_mend{n}"):
            accs = mend_gram(q0, 1, get_q2, put_q2, own(q0), get_v2, accs, n)
    with NS(f"c_zwait{end}"):
        finish_all(sent[end])
        gather(1, end)
    with NS(f"c_mend{end}"):
        mend_end(q0, 1, get_q2, put_q2)
        for x in rest:
            accs = gram_plane(accs, own(q0), get_v2, x)
        sum_start(1, gram_end(0, accs))
    with NS("c_early2"):
        lax.fori_loop(split, nx, early, 0)
    with NS("c_late"):
        lax.fori_loop(0, nx, late, 0)
    with NS("c_sum2"):
        total = sum_end(1)
    with NS("c_alg2"):
        curve = left + mm(alpha_tc, mm(extract(total, 0), alpha))
        fill(t_out, columns(solve(columns(curve), new, row)))


def final_kernel(dims, step, t, x1, r1, p1, s1, sol, res, sol_buf, res_buf, sem):
    nf, nx, ny = dims

    def saves(n):
        part = pl.ds(n * step, step)
        return [pltpu.make_async_copy(sol_buf.at[:, part], sol.at[:, part], sem.at[0, n]),
                pltpu.make_async_copy(res_buf.at[:, part], res.at[:, part], sem.at[1, n])]

    def body(n, carry):
        for k in range(step):
            x = n * step + k
            for yb in range(ny // 8):
                y = slice(yb * 8, yb * 8 + 8)
                u, v = p1[:, x, y], s1[:, x, y]
                s, e = x1[:, x, y], r1[:, x, y]
                for i in range(nf):
                    s = s + t[i] * u[i][None]
                    e = e - t[i] * v[i][None]
                sol_buf[:, x, y] = s
                res_buf[:, x, y] = e
        for copy in saves(n):
            copy.start()
        return carry

    lax.fori_loop(0, nx // step, body, 0)

    def end(n, carry):
        for copy in saves(n):
            copy.wait()
        return carry

    lax.fori_loop(0, nx // step, end, 0)


def shards(sizes, rhs, stencil):
    nf, nx, ny, nz = rhs.shape
    tall = ny + 16
    field = jax.ShapeDtypeStruct(rhs.shape, F32)
    kept = pltpu.VMEM(rhs.shape, F32)
    table = pltpu.VMEM((8, 8, 8, nz), F32)
    anyspace = pl.BlockSpec(memory_space=pl.ANY)
    local = pl.BlockSpec(memory_space=pltpu.VMEM)
    devices = sizes["gx"] * sizes["gy"] * sizes["gz"]
    chunks, packs = nx // 4, nf // (16 // (ny // 8)) + 1
    padded = pltpu.VMEM((nf, nx + 2, tall, nz), F32)

    def kernel(*refs):
        main_kernel(sizes, (nf, nx, ny), *refs)

    x1, r1, p1, s1, t = pl.pallas_call(
        kernel,
        out_shape=(kept, kept, kept, kept, table),
        in_specs=[pl.BlockSpec(memory_space=pltpu.HBM)] * 2,
        out_specs=(local,) * 5,
        scratch_shapes=[
            padded, padded,
            pltpu.VMEM((13, nx + 1, tall, nz), F32),
            pltpu.VMEM((len(LO) + len(HI), nx, ny, nz), F32),
            pltpu.VMEM((nx, ny, nz), F32),
            pltpu.VMEM((nx, ny, nz), F32),
            pltpu.VMEM((nf, nx, ny, nz), F32),
            pltpu.VMEM((3, ny // 8, nf + 1, 8, nz), F32),
            pltpu.VMEM((2, nf + 1, ny, nz), F32),
            pltpu.VMEM((2, nf + 1, ny, nz), F32),
            pltpu.VMEM((2, packs, 8, nz), F32),
            pltpu.VMEM((2, packs, 8, nz), F32),
            pltpu.VMEM((2, chunks, packs, 8, nz), F32),
            pltpu.VMEM((2, chunks, 2, packs, 8, nz), F32),
            pltpu.VMEM((len(LO), 8, nz), F32),
            pltpu.VMEM((2, len(LO), 8, nz), F32),
            pltpu.VMEM((chunks, packs, 8, nz), F32),
            pltpu.VMEM((len(LO), 8, nz), F32),
            pltpu.VMEM((8, 8, 128), F32),
            pltpu.VMEM((8, 8, 8, 128), F32),
            pltpu.VMEM((8, 128), F32),
            pltpu.VMEM((2, 1, 128), F32),
            pltpu.VMEM((2, devices, 1, 128), F32),
            table, table, table,
            pltpu.SemaphoreType.DMA((3,)),
            pltpu.SemaphoreType.DMA((64,)),
            pltpu.SemaphoreType.DMA((64,)),
            pltpu.SemaphoreType.DMA((2, devices - 1)),
            pltpu.SemaphoreType.DMA((2, devices - 1)),
        ],
        compiler_params=pltpu.CompilerParams(
            collective_id=0, has_side_effects=True, vmem_limit_bytes=40 * 2**20),
        name="krylov",
    )(*[pltpu.with_memory_space_constraint(v, pltpu.HBM) for v in (rhs, stencil)])

    step = 2

    def last(*refs):
        final_kernel((nf, nx, ny), step, *refs)

    return pl.pallas_call(
        last,
        out_shape=(field, field),
        in_specs=[local] * 5,
        out_specs=(pl.BlockSpec(memory_space=pltpu.HBM),) * 2,
        scratch_shapes=[
            pltpu.VMEM(rhs.shape, F32), pltpu.VMEM(rhs.shape, F32),
            pltpu.SemaphoreType.DMA((2, nx // step)),
        ],
        compiler_params=pltpu.CompilerParams(vmem_limit_bytes=40 * 2**20),
        name="combine",
    )(t, x1, r1, p1, s1)


def solution(mesh):
    sizes = {a: mesh.shape[a] for a in AXES}
    spec = P(None, "gx", "gy", "gz")

    def run(rhs, stencil):
        return shards(sizes, rhs, stencil)

    return jax.shard_map(run, mesh=mesh, in_specs=(spec, spec), out_specs=(spec, spec), check_vma=False)
```

```python
import jax
import jax.numpy as jnp
from jax import lax
from jax.experimental import pallas as pl
from jax.experimental.pallas import tpu as pltpu
from jax.sharding import PartitionSpec as P

FORWARD = [
    (a, b, c) for a in (-1, 0, 1) for b in (-1, 0, 1) for c in (-1, 0, 1) if (a, b, c) > (0, 0, 0)
]
AXES = ("gx", "gy", "gz")
RECEIVES = 37
SENDS = 20
LO = [k for k, o in enumerate(FORWARD) if o[2] == 1]
HI = [k for k, o in enumerate(FORWARD) if o[2] == -1]
F32 = jnp.float32
NS = jax.named_scope


def runs(ks):
    out = []
    for k in ks:
        if out and out[-1][1] == k:
            out[-1][1] = k + 1
        else:
            out.append([k, k + 1])
    return out


def splat(a, k):
    return jnp.broadcast_to(a[:, k : k + 1], (8, 128))


def line(a, k):
    return jnp.broadcast_to(a[k : k + 1, :], (8, 128))


def columns(a):
    return [splat(a, k) for k in range(8)]


def mm(cols, b):
    parts = [cols[k] * line(b, k) for k in range(8)]
    while len(parts) > 1:
        parts = [parts[i] + parts[i + 1] for i in range(0, len(parts), 2)]
    return parts[0]


def solve(cols, b, row):
    cols = list(cols)
    for k in range(8):
        factor = cols[k]
        inverse = 1.0 / line(factor, k)
        pivot = line(b, k) * inverse
        b = jnp.where(row == k, pivot, b - factor * pivot)
        for j in range(k + 1, 8):
            pivot = line(cols[j], k) * inverse
            cols[j] = jnp.where(row == k, pivot, cols[j] - factor * pivot)
    return b


def transposed(a, row, lane):
    out = jnp.zeros_like(a)
    for i in range(8):
        across = jnp.sum(jnp.where(lane == row, a[:, i : i + 1], 0.0), axis=0, keepdims=True)
        out = out + jnp.where(row == i, across, 0.0)
    return out


def main_kernel(sizes, dims, rhs, sten, x1, r1, p1, s1, t_out, p0, q0, w, ws, s0, diag, q2, scr,
                xsend, xrecv, zsend, zrecv, wzsend, wzrecv, ucross, uw, red, held, gacc, cur, slots,
                t_alpha, t_beta, t_ib, lsem, xs, xr, ars, arr):
    nf, nx, ny = dims
    yb_n = ny // 8
    tall = ny + 16
    group = 128 // (8 * yb_n)
    deep = 4
    wide = deep * yb_n
    chunks = nx // deep

    def packs(e):
        return (nf - e) // group + 1

    pos = {a: lax.axis_index(a) for a in AXES}
    lane = lax.broadcasted_iota(jnp.int32, (8, 128), 1)
    row = lax.broadcasted_iota(jnp.int32, (8, 128), 0)
    first_lane = lane == 0
    last_lane = lane == 127
    rim = first_lane | last_lane
    even = lax.rem(lane, 2) == 0
    half_lane = lane // 2
    ys = pl.ds(8, ny)
    SHIFTED = LO + HI

    devices = sizes["gx"] * sizes["gy"] * sizes["gz"]
    me = (pos["gx"] * sizes["gy"] + pos["gy"]) * sizes["gz"] + pos["gz"]

    loads = [
        pltpu.make_async_copy(rhs, p0.at[:, pl.ds(1, nx), ys], lsem.at[0]),
        pltpu.make_async_copy(sten.at[pl.ds(1, 13)], w.at[:, pl.ds(1, nx), ys], lsem.at[1]),
        pltpu.make_async_copy(sten.at[0], s0, lsem.at[2]),
    ]
    loads[1].start()
    loads[2].start()

    moved = {a: [lax.rem(pos[a] + d, sizes[a]) for d in range(sizes[a])] for a in AXES}
    offsets = [(i, j, k) for i in range(sizes["gx"]) for j in range(sizes["gy"]) for k in range(sizes["gz"])][1:]
    offsets.sort(key=lambda d: -sum(min(v, sizes[a] - v) for v, a in zip(d, AXES)))

    def peer(d):
        return {a: moved[a][v] for v, a in zip(d, AXES)}

    barrier = pltpu.get_barrier_semaphore()
    for d in offsets:
        pl.semaphore_signal(barrier, inc=1, device_id=peer(d), device_id_type=pl.DeviceIdType.MESH)

    last = {a: sizes[a] - 1 for a in AXES}

    @pl.when(pos["gx"] == 0)
    def _():
        xrecv[...] = jnp.zeros(xrecv.shape, F32)

    loads[0].start()

    @pl.when(pos["gx"] == last["gx"])
    def _():
        for buf in (p0, q0):
            buf[:, nx + 1, ys] = jnp.zeros((nf, ny, 128), F32)

    def clear_y(y):
        def body(x, carry):
            for buf in (p0, q0):
                buf[:, x, y : y + 8] = jnp.zeros((nf, 8, 128), F32)
            return carry

        lax.fori_loop(1, nx + 2, body, 0)

        def body_w(x, carry):
            w[:, x, y : y + 8] = jnp.zeros((13, 8, 128), F32)
            return carry

        lax.fori_loop(1, nx + 1, body_w, 0)

    @pl.when(pos["gy"] == 0)
    def _():
        clear_y(0)

    @pl.when(pos["gy"] == last["gy"])
    def _():
        clear_y(ny + 8)

    for side, place in ((0, 0), (1, last["gz"])):
        @pl.when(pos["gz"] == place)
        def _():
            for e in range(2):
                for n in range(chunks):
                    zrecv[e, n, side] = jnp.zeros(zrecv.shape[3:], F32)
            wzrecv[side] = jnp.zeros((len(LO), 8, 128), F32)

    zsend[...] = jnp.zeros(zsend.shape, F32)
    for e in range(2):
        for n in range(packs(e)):
            xsend[e, n] = jnp.zeros((8, 128), F32)
    wzsend[...] = jnp.zeros(wzsend.shape, F32)

    pl.semaphore_wait(barrier, devices - 1)

    arrivals = iter(range(RECEIVES))
    free = list(range(SENDS))

    def shift(axis, up, src, dst):
        n = sizes[axis]
        i = pos[axis]
        slot = free.pop(0)
        copy = pltpu.make_async_remote_copy(
            src_ref=src, dst_ref=dst, send_sem=xs.at[slot], recv_sem=xr.at[next(arrivals)],
            device_id={axis: lax.rem(i + (1 if up else n - 1), n)},
            device_id_type=pl.DeviceIdType.MESH)
        sends = i < n - 1 if up else i > 0
        gets = i > 0 if up else i < n - 1

        @pl.when(sends)
        def _():
            copy.start()

        def finish():
            @pl.when(sends)
            def _():
                copy.wait_send()

            @pl.when(gets)
            def _():
                copy.wait_recv()

            free.append(slot)

        return finish

    def finish_all(items):
        for f in items:
            f()

    def y_faces(buf, start, length):
        xs_ = pl.ds(start, length)
        return [
            shift("gy", True, buf.at[:, xs_, pl.ds(ny, 8)], buf.at[:, xs_, pl.ds(0, 8)]),
            shift("gy", False, buf.at[:, xs_, pl.ds(8, 8)], buf.at[:, xs_, pl.ds(ny + 8, 8)]),
        ]

    def w_faces(start, length):
        xs_ = pl.ds(start, length)
        out = []
        for b, up, src, dst in ((1, True, ny, 0), (-1, False, 8, ny + 8)):
            for lo, hi in runs([k for k, o in enumerate(FORWARD) if o[1] == b]):
                ks = pl.ds(lo, hi - lo)
                out.append(shift("gy", up, w.at[ks, xs_, pl.ds(src, 8)], w.at[ks, xs_, pl.ds(dst, 8)]))
        return out

    def x_down(buf):
        return [shift("gx", False, buf.at[:, 1, ys], buf.at[:, nx + 1, ys])]

    def x_tile(f, yb):
        return packs(0) + f * yb_n + yb

    def x_up(e):
        part = pl.ds(0, x_tile(nf - e, yb_n))
        return [shift("gx", True, xsend.at[e, part], xrecv.at[e, part])]

    def z_both(send, recv):
        return [
            shift("gz", True, send, recv.at[0]),
            shift("gz", False, send, recv.at[1]),
        ]

    def gram_body(accs, ub, vb):
        return [accs[i] + ub[i : i + 1] * vb[i:] for i in range(nf)]

    def gram_start():
        return tuple(jnp.zeros((nf - i, 8, 128), F32) for i in range(nf))

    def place(g, i, j):
        return 36 * g + 8 * i - i * (i - 1) // 2 + j - i

    def gram_end(g, accs):
        red[...] = jnp.zeros(red.shape, F32)
        for i in range(nf):
            red[i, i:nf, :] = jnp.sum(accs[i], axis=1)
        out = jnp.zeros((8, 128), F32)
        for i in range(nf):
            t = jnp.sum(red[i], axis=1, keepdims=True)
            out = out + jnp.where(lane == place(g, i, row), t, 0.0)
        return out

    def own(buf):
        return lambda x, yb: buf[:, x + 1, 8 + yb * 8 : 16 + yb * 8]

    def gram_plane(accs, u, v, x):
        for yb in range(yb_n):
            accs = gram_body(accs, u(x, yb), v(x, yb))
        return tuple(accs)

    def gram(g, u, v):
        return gram_end(g, lax.fori_loop(0, nx, lambda x, accs: gram_plane(accs, u, v, x), gram_start()))

    def several(n, f):
        def body(t, carry):
            for k in range(n):
                f(t * n + k, 0)
            return carry

        lax.fori_loop(0, nx // n, body, 0)

    def pack_w(x, carry):
        for yb in range(yb_n):
            j = x * yb_n + yb
            here = half_lane == j
            y = 8 + yb * 8
            for n, k in enumerate(LO):
                both = w[k, x + 1, y : y + 8]
                if n < len(HI):
                    both = jnp.where(first_lane, w[HI[n], x + 1, y : y + 8], both)
                pltpu.store(wzsend.at[n], pltpu.roll(both, 2 * j + 1, 1), mask=here)
        return carry

    def shift_w(x, carry):
        for yb in range(yb_n):
            y = 8 + yb * 8
            for n, k in enumerate(SHIFTED):
                ws[n, x, yb * 8 : yb * 8 + 8] = pltpu.roll(w[k, x + 1, y : y + 8], 1 if k in LO else 127, 1)
        return carry

    def insert_w(x, carry):
        for yb in range(yb_n):
            j = x * yb_n + yb
            for n in range(len(LO)):
                edge = pltpu.roll(uw[n], 127 - 2 * j, 1)
                pltpu.store(ws.at[n, x, yb * 8 : yb * 8 + 8], edge, mask=first_lane)
                if n < len(HI):
                    pltpu.store(ws.at[len(LO) + n, x, yb * 8 : yb * 8 + 8], edge, mask=last_lane)
        return carry

    def crossing(from_low, from_high):
        return jnp.where(even, pltpu.roll(from_high, 127, 1), pltpu.roll(from_low, 1, 1))

    def pack_z(out, f, both, m):
        m = f % group * wide + m
        pltpu.store(out.at[f // group], pltpu.roll(both, lax.rem(2 * m + 1, 128), 1), mask=half_lane == m)

    def upward(buf, e):
        for yb in range(yb_n):
            y = 8 + yb * 8
            accs = {}
            back = {}
            for b in (-1, 0, 1):
                v = buf[:, nx, y + b : y + b + 8]
                for c in (-1, 0, 1):
                    coef = w[FORWARD.index((1, -b, -c)), nx, y + b : y + b + 8]
                    term = coef[None] * v
                    accs[c] = term if c not in accs else accs[c] + term
                    back[c] = coef if c not in back else back[c] + coef
            whole = accs[0] + pltpu.roll(accs[1], 127, 2) + pltpu.roll(accs[-1], 1, 2)
            both = jnp.where(first_lane[None], accs[1], accs[-1])
            for f in range(nf):
                xsend[e, x_tile(f, yb)] = whole[f]
                pack_z(xsend.at[e], f, both[f], (deep - 1) * yb_n + yb)
            if e == 0:
                xsend[e, x_tile(nf, yb)] = (
                    back[0] + pltpu.roll(back[1], 127, 1) + pltpu.roll(back[-1], 1, 1))
                both = jnp.where(first_lane, back[1], back[-1])
                pack_z(xsend.at[e], nf, both, (deep - 1) * yb_n + yb)

    def sums(buf, e, x, lowest=False):
        for yb in range(yb_n):
            y = 8 + yb * 8
            accs = {}
            back = {}
            if lowest:
                accs[0] = jnp.stack([xrecv[e, x_tile(f, yb)] for f in range(nf)])
                if e == 0:
                    back[0] = xrecv[e, x_tile(nf, yb)]
            for a in (0, 1) if lowest else (-1, 0, 1):
                for b in (-1, 0, 1):
                    v = buf[:, x + 1 + a, y + b : y + b + 8]
                    for c in (-1, 0, 1):
                        o = (a, b, c)
                        if o == (0, 0, 0):
                            continue
                        if o > (0, 0, 0):
                            k = FORWARD.index(o)
                            if c == 0:
                                coef = w[k, x + 1, y : y + 8]
                            else:
                                coef = ws[SHIFTED.index(k), x, yb * 8 : yb * 8 + 8]
                        else:
                            k = FORWARD.index((-a, -b, -c))
                            coef = w[k, x + 1 + a, y + b : y + b + 8]
                            if e == 0:
                                back[c] = coef if c not in back else back[c] + coef
                        term = coef[None] * v
                        accs[c] = term if c not in accs else accs[c] + term
            if e == 0:
                total = s0[x, yb * 8 : yb * 8 + 8] + back[0]
                for k in range(13):
                    total = total + w[k, x + 1, y : y + 8]
                back[0] = total
            for c in (-1, 0, 1):
                scr[c + 1, yb, 0:nf] = accs[c]
                if e == 0:
                    scr[c + 1, yb, nf] = back[c]

    def settle(buf, e, x, put, chunk, where):
        for yb in range(yb_n):
            y = 8 + yb * 8
            m = where * yb_n + yb
            if e == 0:
                up, down = scr[2, yb, nf], scr[0, yb, nf]
                total = scr[1, yb, nf] + pltpu.roll(up, 127, 1) + pltpu.roll(down, 1, 1)
                diag[x, yb * 8 : yb * 8 + 8] = total
                pack_z(zsend.at[e, chunk], nf, jnp.where(first_lane, up, down), m)
            else:
                total = diag[x, yb * 8 : yb * 8 + 8]
            for f in range(nf):
                up, down = scr[2, yb, f], scr[0, yb, f]
                total_f = scr[1, yb, f] + pltpu.roll(up, 127, 1) + pltpu.roll(down, 1, 1)
                put(f, x, yb, total * buf[f, x + 1, y : y + 8] - total_f)
                pack_z(zsend.at[e, chunk], f, jnp.where(first_lane, up, down), m)

    def gather(e, chunk):
        for n in range(packs(e)):
            mine = zsend[e, chunk, n]
            ucross[chunk, n] = crossing(zrecv[e, chunk, 0, n] - mine, zrecv[e, chunk, 1, n] - mine)

    def mend(buf, e, x, get, put, chunk, where):
        for yb in range(yb_n):
            y = 8 + yb * 8
            m = where * yb_n + yb

            def edge(f):
                place = f % group * wide + m
                side = pltpu.roll(ucross[chunk, f // group], lax.rem(255 - 2 * place, 128), 1)
                return jnp.where(rim, side, 0.0)

            if e == 0:
                extra = edge(nf)
                diag[x, yb * 8 : yb * 8 + 8] += extra
            for f in range(nf):
                value = get(f, x, yb) - edge(f)
                if e == 0:
                    value = value + extra * buf[f, x + 1, y : y + 8]
                put(f, x, yb, value)

    def copy_row(r, n, dst):
        return pltpu.make_async_remote_copy(
            src_ref=cur.at[r], dst_ref=slots.at[r, dst], send_sem=ars.at[r], recv_sem=arr.at[r],
            device_id=peer(offsets[n]), device_id_type=pl.DeviceIdType.MESH)

    def sum_start(r, value):
        value = jnp.sum(value, axis=0, keepdims=True)
        cur[r] = value
        slots[r, me] = value
        for n in range(devices - 1):
            copy_row(r, n, me).start()

    def sum_end(r):
        every = slots.at[r, pl.ds(0, devices - 1)]
        copies = pltpu.make_async_remote_copy(
            src_ref=every, dst_ref=every, send_sem=ars.at[r], recv_sem=arr.at[r],
            device_id=peer(offsets[0]), device_id_type=pl.DeviceIdType.MESH)
        copies.wait_send()
        copies.wait_recv()
        parts = [slots[r, q] for q in range(devices)]
        while len(parts) > 1:
            parts = [a + b for a, b in zip(parts[::2], parts[1::2])] + parts[len(parts) // 2 * 2 :]
        return jnp.broadcast_to(parts[0], (8, 128))

    def extract(total, g):
        cols = []
        for k in range(8):
            where = place(g, jnp.minimum(row, k), jnp.maximum(row, k))
            cols.append(jnp.broadcast_to(jnp.sum(jnp.where(lane == where, total, 0.0), axis=1, keepdims=True), (8, 128)))
        return cols

    def matrix(cols):
        out = jnp.zeros((8, 128), F32)
        for k in range(8):
            out = jnp.where(lane == k, cols[k], out)
        return out

    def fill(tab, cols):
        for j in range(8):
            for i in range(8):
                tab[i, j] = line(cols[j], i)

    def put_q1(f, x, yb, v):
        q0[f, x + 1, 8 + yb * 8 : 16 + yb * 8] = v

    def get_q1(f, x, yb):
        return q0[f, x + 1, 8 + yb * 8 : 16 + yb * 8]

    def put_q2(f, x, yb, v):
        q2[f, x, yb * 8 : yb * 8 + 8] = v

    def get_q2(f, x, yb):
        return q2[f, x, yb * 8 : yb * 8 + 8]

    def z_send(e, chunk):
        part = pl.ds(0, packs(e))
        return z_both(zsend.at[e, chunk, part], zrecv.at[e, chunk, :, part])

    def planes(buf, e, put, chunk):
        def body(t, carry):
            x = chunk * deep + 2 + t
            settle(buf, e, x - 1, put, chunk, t)
            sums(buf, e, x)
            return carry

        lax.fori_loop(0, deep, body, 0)
        return z_send(e, chunk)

    end = chunks - 1

    def interior(buf, e, put, across=None):
        sent = []
        ends = None
        sums(buf, e, 1)
        for n in range(end):
            with NS(f"op{e}_in{n}"):
                sent.append(planes(buf, e, put, n))
            if across and n == end - 2:
                ends = arrive(buf, e, across)
        with NS(f"op{e}_in{end}"):
            settle(buf, e, nx - 3, put, end, 0)
            sums(buf, e, nx - 2)
            settle(buf, e, nx - 2, put, end, 1)
        return sent, ends

    def arrive(buf, e, across):
        with NS(f"op{e}_xwait"):
            finish_all(across)
            return y_faces(buf, nx + 1, 1)

    def outer(buf, e, put, ends, across):
        with NS(f"op{e}_ywait"):
            finish_all(ends)
        with NS(f"op{e}_st3"):
            sums(buf, e, nx - 1)
            settle(buf, e, nx - 1, put, end, 2)
        with NS(f"op{e}_upwait"):
            finish_all(across)
        with NS(f"op{e}_st4"):
            sums(buf, e, 0, True)
            settle(buf, e, 0, put, end, 3)
            for n in range(packs(e)):
                zsend[e, end, n] += xrecv[e, n]
            return z_send(e, end)

    def mend_gram(buf, e, get, put, u, v, accs, chunk):
        lo = chunk * deep + 1
        mend(buf, e, lo, get, put, chunk, 0)

        def body(t, accs):
            accs = gram_plane(accs, u, v, lo + t)
            mend(buf, e, lo + t + 1, get, put, chunk, t + 1)
            return accs

        return gram_plane(lax.fori_loop(0, deep - 1, body, accs), u, v, lo + deep - 1)

    def mend_end(buf, e, get, put, between=None):
        for where, x in ((2, nx - 1), (3, 0), (0, nx - 3), (1, nx - 2)):
            mend(buf, e, x, get, put, end, where)
            if between and where == 2:
                between()

    rest = (nx - 1, 0, nx - 3, nx - 2)

    with NS("a_loadw"):
        loads[1].wait()
        rims = w_faces(1, nx)
    with NS("a_packw"):
        several(8, pack_w)
        zw = z_both(wzsend, wzrecv)
    with NS("a_loadp"):
        loads[0].wait()
        rims += y_faces(p0, nx, 1)
        down = x_down(p0)
        sides = y_faces(p0, 1, nx - 1)
    with NS("a_gram0"):
        gacc[...] = gram(0, own(p0), own(p0))
    with NS("a_shiftw"):
        several(4, shift_w)
    with NS("a_up"):
        finish_all(rims)
        upward(p0, 0)
        up = x_up(0)
    with NS("a_zwait"):
        finish_all(zw)
    with NS("a_insw"):
        for n in range(len(LO)):
            uw[n] = crossing(wzrecv[0, n], wzrecv[1, n])
        several(8, insert_w)
    with NS("a_ywait"):
        loads[2].wait()
        finish_all(sides)
    sent, ends = interior(p0, 0, put_q1, down)
    sent.append(outer(p0, 0, put_q1, ends, up))

    accs = gram_start()
    sides = []
    for n in range(end):
        with NS(f"b_zwait{n}"):
            finish_all(sent[n])
            gather(0, n)
        with NS(f"b_mend{n}"):
            accs = mend_gram(p0, 0, get_q1, put_q1, own(p0), own(q0), accs, n)
    with NS(f"b_zwait{end}"):
        finish_all(sent[end])
        gather(0, end)
    rims = []
    with NS(f"b_mend{end}"):
        mend_end(p0, 0, get_q1, put_q1, lambda: rims.extend(y_faces(q0, nx, 1)))
        sides = y_faces(q0, 1, nx - 1)
    with NS("b_gram1"):
        for x in rest:
            accs = gram_plane(accs, own(p0), own(q0), x)
        gacc[...] += gram_end(1, accs)
    with NS("b_gram2a"):
        down = x_down(q0)
        squares = lax.fori_loop(1, nx, lambda x, accs: gram_plane(accs, own(q0), own(q0), x), gram_start())
        for i in range(nf):
            held[i, i:nf] = squares[i]
    with NS("b_gram2"):
        squares = tuple(held[i, i:nf] for i in range(nf))
        squares = gram_plane(squares, own(q0), own(q0), 0)
        sum_start(0, gacc[...] + gram_end(2, squares))
    with NS("b_up"):
        finish_all(rims)
        upward(q0, 1)
        up = x_up(1)
    with NS("b_ywait"):
        finish_all(sides)

    sent, ends = interior(q0, 1, put_q2)

    def get_v2(x, yb):
        return q2[:, x, yb * 8 : yb * 8 + 8]

    with NS("c_sum1"):
        total = sum_end(0)
    with NS("c_alg1"):
        rrc, pqc, ssc = [extract(total, g) for g in range(3)]
        rr, pq = matrix(rrc), matrix(pqc)
        alpha = solve(pqc, rr, row)
        alpha_c = columns(alpha)
        fill(t_alpha, alpha_c)
        alpha_tc = columns(transposed(alpha, row, lane))
        ssa = mm(ssc, alpha)
        new = rr - mm(alpha_tc, pq) - mm(pqc, alpha) + mm(alpha_tc, ssa)
        beta = solve(rrc, new, row)
        fill(t_beta, columns(beta))
        ib = beta + jnp.where(lane == row, 1.0, 0.0)
        ib_tc = columns(transposed(ib, row, lane))
        fill(t_ib, columns(ib))
        left = mm(ib_tc, mm(pqc, ib) - ssa) - mm(alpha_tc, mm(ssc, ib))

    def early(x, carry):
        for yb in range(yb_n):
            y = slice(yb * 8, yb * 8 + 8)
            u, v = own(p0)(x, yb), own(q0)(x, yb)
            step, rest = t_alpha[0] * u[0][None], u
            for i in range(nf):
                if i:
                    step = step + t_alpha[i] * u[i][None]
                rest = rest - t_alpha[i] * v[i][None]
            x1[:, x, y] = step
            r1[:, x, y] = rest
        return carry

    def late(x, carry):
        for yb in range(yb_n):
            y = slice(yb * 8, yb * 8 + 8)
            u, v, z = own(p0)(x, yb), own(q0)(x, yb), get_v2(x, yb)
            step, image = r1[:, x, y], jnp.zeros((nf, 8, 128), F32)
            for i in range(nf):
                step = step + t_beta[i] * u[i][None]
                image = image + (t_ib[i] * v[i][None] - t_alpha[i] * z[i][None])
            p1[:, x, y] = step
            s1[:, x, y] = image
        return carry

    split = nx // 4
    ends = arrive(q0, 1, down)
    with NS("c_early"):
        lax.fori_loop(0, split, early, 0)
    sent.append(outer(q0, 1, put_q2, ends, up))
    accs = gram_start()
    for n in range(end):
        with NS(f"c_zwait{n}"):
            finish_all(sent[n])
            gather(1, n)
        with NS(f"c_mend{n}"):
            accs = mend_gram(q0, 1, get_q2, put_q2, own(q0), get_v2, accs, n)
    with NS(f"c_zwait{end}"):
        finish_all(sent[end])
        gather(1, end)
    with NS(f"c_mend{end}"):
        mend_end(q0, 1, get_q2, put_q2)
        for x in rest:
            accs = gram_plane(accs, own(q0), get_v2, x)
        sum_start(1, gram_end(0, accs))
    with NS("c_early2"):
        lax.fori_loop(split, nx, early, 0)
    with NS("c_late"):
        lax.fori_loop(0, nx, late, 0)
    with NS("c_sum2"):
        total = sum_end(1)
    with NS("c_alg2"):
        curve = left + mm(alpha_tc, mm(extract(total, 0), alpha))
        fill(t_out, columns(solve(columns(curve), new, row)))


def final_kernel(dims, step, t, x1, r1, p1, s1, sol, res, sol_buf, res_buf, sem):
    nf, nx, ny = dims

    def saves(n):
        part = pl.ds(n * step, step)
        return [pltpu.make_async_copy(sol_buf.at[:, part], sol.at[:, part], sem.at[0]),
                pltpu.make_async_copy(res_buf.at[:, part], res.at[:, part], sem.at[1])]

    def body(n, carry):
        for k in range(step):
            x = n * step + k
            for yb in range(ny // 8):
                y = slice(yb * 8, yb * 8 + 8)
                u, v = p1[:, x, y], s1[:, x, y]
                s, e = x1[:, x, y], r1[:, x, y]
                for i in range(nf):
                    s = s + t[i] * u[i][None]
                    e = e - t[i] * v[i][None]
                sol_buf[:, x, y] = s
                res_buf[:, x, y] = e
        for copy in saves(n):
            copy.start()
        return carry

    lax.fori_loop(0, nx // step, body, 0)

    pltpu.make_async_copy(sol_buf, sol, sem.at[0]).wait()
    pltpu.make_async_copy(res_buf, res, sem.at[1]).wait()


def shards(sizes, rhs, stencil):
    nf, nx, ny, nz = rhs.shape
    tall = ny + 16
    field = jax.ShapeDtypeStruct(rhs.shape, F32)
    kept = pltpu.VMEM(rhs.shape, F32)
    table = pltpu.VMEM((8, 8, 8, nz), F32)
    anyspace = pl.BlockSpec(memory_space=pl.ANY)
    local = pl.BlockSpec(memory_space=pltpu.VMEM)
    devices = sizes["gx"] * sizes["gy"] * sizes["gz"]
    chunks, packs = nx // 4, nf // (16 // (ny // 8)) + 1
    padded = pltpu.VMEM((nf, nx + 2, tall, nz), F32)

    def kernel(*refs):
        main_kernel(sizes, (nf, nx, ny), *refs)

    x1, r1, p1, s1, t = pl.pallas_call(
        kernel,
        out_shape=(kept, kept, kept, kept, table),
        in_specs=[pl.BlockSpec(memory_space=pltpu.HBM)] * 2,
        out_specs=(local,) * 5,
        scratch_shapes=[
            padded, padded,
            pltpu.VMEM((13, nx + 1, tall, nz), F32),
            pltpu.VMEM((len(LO) + len(HI), nx, ny, nz), F32),
            pltpu.VMEM((nx, ny, nz), F32),
            pltpu.VMEM((nx, ny, nz), F32),
            pltpu.VMEM((nf, nx, ny, nz), F32),
            pltpu.VMEM((3, ny // 8, nf + 1, 8, nz), F32),
            pltpu.VMEM((2, packs + (nf + 1) * ny // 8, 8, nz), F32),
            pltpu.VMEM((2, packs + (nf + 1) * ny // 8, 8, nz), F32),
            pltpu.VMEM((2, chunks, packs, 8, nz), F32),
            pltpu.VMEM((2, chunks, 2, packs, 8, nz), F32),
            pltpu.VMEM((len(LO), 8, nz), F32),
            pltpu.VMEM((2, len(LO), 8, nz), F32),
            pltpu.VMEM((chunks, packs, 8, nz), F32),
            pltpu.VMEM((len(LO), 8, nz), F32),
            pltpu.VMEM((8, 8, 128), F32),
            pltpu.VMEM((8, 8, 8, 128), F32),
            pltpu.VMEM((8, 128), F32),
            pltpu.VMEM((2, 1, 128), F32),
            pltpu.VMEM((2, devices, 1, 128), F32),
            table, table, table,
            pltpu.SemaphoreType.DMA((3,)),
            pltpu.SemaphoreType.DMA((SENDS,)),
            pltpu.SemaphoreType.DMA((RECEIVES,)),
            pltpu.SemaphoreType.DMA((2,)),
            pltpu.SemaphoreType.DMA((2,)),
        ],
        compiler_params=pltpu.CompilerParams(
            collective_id=0, has_side_effects=True, vmem_limit_bytes=40 * 2**20),
        name="krylov",
    )(*[pltpu.with_memory_space_constraint(v, pltpu.HBM) for v in (rhs, stencil)])

    step = 2

    def last(*refs):
        final_kernel((nf, nx, ny), step, *refs)

    return pl.pallas_call(
        last,
        out_shape=(field, field),
        in_specs=[local] * 5,
        out_specs=(pl.BlockSpec(memory_space=pltpu.HBM),) * 2,
        scratch_shapes=[
            pltpu.VMEM(rhs.shape, F32), pltpu.VMEM(rhs.shape, F32),
            pltpu.SemaphoreType.DMA((2,)),
        ],
        compiler_params=pltpu.CompilerParams(vmem_limit_bytes=40 * 2**20),
        name="combine",
    )(t, x1, r1, p1, s1)


def solution(mesh):
    sizes = {a: mesh.shape[a] for a in AXES}
    spec = P(None, "gx", "gy", "gz")

    def run(rhs, stencil):
        return shards(sizes, rhs, stencil)

    return jax.shard_map(run, mesh=mesh, in_specs=(spec, spec), out_specs=(spec, spec), check_vma=False)
```

```python
import jax
import jax.numpy as jnp
from jax import lax
from jax.experimental import pallas as pl
from jax.experimental.pallas import tpu as pltpu
from jax.sharding import PartitionSpec as P

FORWARD = [
    (a, b, c) for a in (-1, 0, 1) for b in (-1, 0, 1) for c in (-1, 0, 1) if (a, b, c) > (0, 0, 0)
]
AXES = ("gx", "gy", "gz")
RECEIVES = 40
SENDS = 16
LO = [k for k, o in enumerate(FORWARD) if o[2] == 1]
HI = [k for k, o in enumerate(FORWARD) if o[2] == -1]
F32 = jnp.float32
NS = jax.named_scope


def runs(ks):
    out = []
    for k in ks:
        if out and out[-1][1] == k:
            out[-1][1] = k + 1
        else:
            out.append([k, k + 1])
    return out


def splat(a, k):
    return jnp.broadcast_to(a[:, k : k + 1], (8, 128))


def line(a, k):
    return jnp.broadcast_to(a[k : k + 1, :], (8, 128))


def columns(a):
    return [splat(a, k) for k in range(8)]


def mm(cols, b):
    parts = [cols[k] * line(b, k) for k in range(8)]
    while len(parts) > 1:
        parts = [parts[i] + parts[i + 1] for i in range(0, len(parts), 2)]
    return parts[0]


def solve(cols, b, row):
    cols = list(cols)
    for k in range(8):
        factor = cols[k]
        inverse = 1.0 / line(factor, k)
        pivot = line(b, k) * inverse
        b = jnp.where(row == k, pivot, b - factor * pivot)
        for j in range(k + 1, 8):
            pivot = line(cols[j], k) * inverse
            cols[j] = jnp.where(row == k, pivot, cols[j] - factor * pivot)
    return b


def transposed(a, row, lane):
    out = jnp.zeros_like(a)
    for i in range(8):
        across = jnp.sum(jnp.where(lane == row, a[:, i : i + 1], 0.0), axis=0, keepdims=True)
        out = out + jnp.where(row == i, across, 0.0)
    return out


def main_kernel(sizes, dims, rhs, sten, x1, r1, p1, s1, t_out, p0, q0, w, ws, s0, diag, q2, scr, csend, crecv,
                xsend, xrecv, ysend, yrecv, zsend, zrecv, wzsend, wzrecv, ucross, uw, red, held, gacc, cur, slots,
                t_alpha, t_beta, t_ib, lsem, xs, xr, ars, arr, ready):
    nf, nx, ny = dims
    yb_n = ny // 8
    tall = ny + 16
    group = 128 // (8 * yb_n)
    deep = 4
    wide = deep * yb_n
    chunks = nx // deep

    def packs(e):
        return (nf - e) // group + 1

    pos = {a: lax.axis_index(a) for a in AXES}
    lane = lax.broadcasted_iota(jnp.int32, (8, 128), 1)
    row = lax.broadcasted_iota(jnp.int32, (8, 128), 0)
    first_lane = lane == 0
    last_lane = lane == 127
    rim = first_lane | last_lane
    even = lax.rem(lane, 2) == 0
    half_lane = lane // 2
    ys = pl.ds(8, ny)
    SHIFTED = LO + HI

    devices = sizes["gx"] * sizes["gy"] * sizes["gz"]
    me = (pos["gx"] * sizes["gy"] + pos["gy"]) * sizes["gz"] + pos["gz"]

    loads = [
        pltpu.make_async_copy(rhs, p0.at[:, pl.ds(1, nx), ys], lsem.at[0]),
        pltpu.make_async_copy(sten.at[pl.ds(1, 13)], w.at[:, pl.ds(1, nx), ys], lsem.at[1]),
        pltpu.make_async_copy(sten.at[0], s0, lsem.at[2]),
    ]
    loads[1].start()
    loads[2].start()

    moved = {a: [lax.rem(pos[a] + d, sizes[a]) for d in range(sizes[a])] for a in AXES}
    offsets = [(i, j, k) for i in range(sizes["gx"]) for j in range(sizes["gy"]) for k in range(sizes["gz"])][1:]
    offsets.sort(key=lambda d: -sum(min(v, sizes[a] - v) for v, a in zip(d, AXES)))

    def peer(d):
        return {a: moved[a][v] for v, a in zip(d, AXES)}

    barrier = pltpu.get_barrier_semaphore()
    lines = [d for d in offsets if sum(v > 0 for v in d) == 1]
    across = {(i % sizes["gx"], j % sizes["gy"], 0) for i in (1, -1) for j in (1, -1)}
    met = lines + sorted(across & set(offsets) - set(lines))

    def tell(sem, d):
        pl.semaphore_signal(sem, inc=1, device_id=peer(d), device_id_type=pl.DeviceIdType.MESH)

    for d in met:
        tell(barrier, d)

    last = {a: sizes[a] - 1 for a in AXES}

    @pl.when(pos["gx"] == 0)
    def _():
        xrecv[...] = jnp.zeros(xrecv.shape, F32)

    loads[0].start()

    for side, place in ((0, 0), (1, last["gy"])):
        @pl.when((pos["gx"] == last["gx"]) | (pos["gy"] == place))
        def _():
            for e in range(2):
                crecv[e, side] = jnp.zeros((nf, 128), F32)

    @pl.when(pos["gx"] == last["gx"])
    def _():
        for buf in (p0, q0):
            buf[:, nx + 1, ys] = jnp.zeros((nf, ny, 128), F32)

    def clear_y(y):
        def body(x, carry):
            p0[:, x, y : y + 8] = jnp.zeros((nf, 8, 128), F32)
            return carry

        lax.fori_loop(1, nx + 1, body, 0)

        def body_w(x, carry):
            w[:, x, y : y + 8] = jnp.zeros((13, 8, 128), F32)
            return carry

        lax.fori_loop(1, nx + 1, body_w, 0)

    @pl.when(pos["gy"] == 0)
    def _():
        clear_y(0)
        yrecv[0] = jnp.zeros((nx, nf, 128), F32)

    @pl.when(pos["gy"] == last["gy"])
    def _():
        clear_y(ny + 8)
        yrecv[1] = jnp.zeros((nx, nf, 128), F32)

    for side, place in ((0, 0), (1, last["gz"])):
        @pl.when(pos["gz"] == place)
        def _():
            for e in range(2):
                for n in range(chunks):
                    zrecv[e, n, side] = jnp.zeros(zrecv.shape[3:], F32)
            wzrecv[side] = jnp.zeros((len(LO), 8, 128), F32)

    zsend[...] = jnp.zeros(zsend.shape, F32)
    for e in range(2):
        for n in range(packs(e)):
            xsend[e, n] = jnp.zeros((8, 128), F32)
    wzsend[...] = jnp.zeros(wzsend.shape, F32)

    pl.semaphore_wait(barrier, len(met))
    for d in lines:
        if d[0]:
            tell(ready.at[0], d)

    arrivals = iter(range(RECEIVES))
    free = list(range(SENDS))

    def shift(axis, up, src, dst):
        n = sizes[axis]
        i = pos[axis]
        slot = free.pop(0)
        copy = pltpu.make_async_remote_copy(
            src_ref=src, dst_ref=dst, send_sem=xs.at[slot], recv_sem=xr.at[next(arrivals)],
            device_id={axis: lax.rem(i + (1 if up else n - 1), n)},
            device_id_type=pl.DeviceIdType.MESH)
        sends = i < n - 1 if up else i > 0
        gets = i > 0 if up else i < n - 1

        @pl.when(sends)
        def _():
            copy.start()

        def finish():
            @pl.when(sends)
            def _():
                copy.wait_send()

            @pl.when(gets)
            def _():
                copy.wait_recv()

            free.append(slot)

        return finish

    def finish_all(items):
        for f in items:
            f()

    def y_faces(buf, start, length):
        xs_ = pl.ds(start, length)
        return [
            shift("gy", True, buf.at[:, xs_, pl.ds(ny, 8)], buf.at[:, xs_, pl.ds(0, 8)]),
            shift("gy", False, buf.at[:, xs_, pl.ds(8, 8)], buf.at[:, xs_, pl.ds(ny + 8, 8)]),
        ]

    def y_rows(start, length):
        part = pl.ds(start, length)
        return [
            shift("gy", True, ysend.at[0, part], yrecv.at[0, part]),
            shift("gy", False, ysend.at[1, part], yrecv.at[1, part]),
        ]

    def y_unpack(start, length):
        def body(x, carry):
            for f in range(nf):
                q0[f, x + 1, 7:8] = yrecv[0, x, f : f + 1]
                q0[f, x + 1, ny + 8 : ny + 9] = yrecv[1, x, f : f + 1]
            return carry

        if length > 3:
            lax.fori_loop(start, start + length, body, 0)
        else:
            for x in range(start, start + length):
                body(x, 0)

    def w_faces(start, length):
        xs_ = pl.ds(start, length)
        out = []
        for b, up, src, dst in ((1, True, ny, 0), (-1, False, 8, ny + 8)):
            for lo, hi in runs([k for k, o in enumerate(FORWARD) if o[1] == b]):
                ks = pl.ds(lo, hi - lo)
                out.append(shift("gy", up, w.at[ks, xs_, pl.ds(src, 8)], w.at[ks, xs_, pl.ds(dst, 8)]))
        return out

    def corner(e, up):
        side = 0 if up else 1
        i, j = pos["gx"], pos["gy"]
        slot = free.pop(0)
        copy = pltpu.make_async_remote_copy(
            src_ref=csend.at[e, side], dst_ref=crecv.at[e, side], send_sem=xs.at[slot], recv_sem=xr.at[next(arrivals)],
            device_id={"gx": moved["gx"][-1], "gy": moved["gy"][1 if up else -1]},
            device_id_type=pl.DeviceIdType.MESH)
        sends = (i > 0) & (j < last["gy"] if up else j > 0)
        gets = (i < last["gx"]) & (j > 0 if up else j < last["gy"])

        @pl.when(sends)
        def _():
            copy.start()

        def finish():
            @pl.when(sends)
            def _():
                copy.wait_send()

            @pl.when(gets)
            def _():
                copy.wait_recv()

            free.append(slot)

        return finish

    def x_down(buf, e):
        for f in range(nf):
            csend[e, 0, f : f + 1] = buf[f, 1, ny + 7 : ny + 8]
            csend[e, 1, f : f + 1] = buf[f, 1, 8:9]
        return [shift("gx", False, buf.at[:, 1, ys], buf.at[:, nx + 1, ys]), corner(e, True), corner(e, False)]

    def corners(buf, e):
        for f in range(nf):
            buf[f, nx + 1, 7:8] = crecv[e, 0, f : f + 1]
            buf[f, nx + 1, ny + 8 : ny + 9] = crecv[e, 1, f : f + 1]

    def x_tile(f, yb):
        return packs(0) + f * yb_n + yb

    def x_up(e):
        part = pl.ds(0, x_tile(nf - e, yb_n))
        return [shift("gx", True, xsend.at[e, part], xrecv.at[e, part])]

    def z_both(send, recv):
        return [
            shift("gz", True, send, recv.at[0]),
            shift("gz", False, send, recv.at[1]),
        ]

    def gram_body(accs, ub, vb):
        return [accs[i] + ub[i : i + 1] * vb[i:] for i in range(nf)]

    def gram_start():
        return tuple(jnp.zeros((nf - i, 8, 128), F32) for i in range(nf))

    def place(g, i, j):
        return 36 * g + 8 * i - i * (i - 1) // 2 + j - i

    def gram_end(g, accs):
        red[...] = jnp.zeros(red.shape, F32)
        for i in range(nf):
            red[i, i:nf, :] = jnp.sum(accs[i], axis=1)
        out = jnp.zeros((8, 128), F32)
        for i in range(nf):
            t = jnp.sum(red[i], axis=1, keepdims=True)
            out = out + jnp.where(lane == place(g, i, row), t, 0.0)
        return out

    def own(buf):
        return lambda x, yb: buf[:, x + 1, 8 + yb * 8 : 16 + yb * 8]

    def gram_plane(accs, u, v, x):
        for yb in range(yb_n):
            accs = gram_body(accs, u(x, yb), v(x, yb))
        return tuple(accs)

    def gram(g, u, v):
        return gram_end(g, lax.fori_loop(0, nx, lambda x, accs: gram_plane(accs, u, v, x), gram_start()))

    def several(n, f):
        def body(t, carry):
            for k in range(n):
                f(t * n + k, 0)
            return carry

        lax.fori_loop(0, nx // n, body, 0)

    def pack_w(x, carry):
        for yb in range(yb_n):
            j = x * yb_n + yb
            here = half_lane == j
            y = 8 + yb * 8
            for n, k in enumerate(LO):
                both = w[k, x + 1, y : y + 8]
                if n < len(HI):
                    both = jnp.where(first_lane, w[HI[n], x + 1, y : y + 8], both)
                pltpu.store(wzsend.at[n], pltpu.roll(both, 2 * j + 1, 1), mask=here)
        return carry

    def shift_w(x, carry):
        for yb in range(yb_n):
            y = 8 + yb * 8
            for n, k in enumerate(SHIFTED):
                ws[n, x, yb * 8 : yb * 8 + 8] = pltpu.roll(w[k, x + 1, y : y + 8], 1 if k in LO else 127, 1)
        return carry

    def insert_w(x, carry):
        for yb in range(yb_n):
            j = x * yb_n + yb
            for n in range(len(LO)):
                edge = pltpu.roll(uw[n], 127 - 2 * j, 1)
                pltpu.store(ws.at[n, x, yb * 8 : yb * 8 + 8], edge, mask=first_lane)
                if n < len(HI):
                    pltpu.store(ws.at[len(LO) + n, x, yb * 8 : yb * 8 + 8], edge, mask=last_lane)
        return carry

    def crossing(from_low, from_high):
        return jnp.where(even, pltpu.roll(from_high, 127, 1), pltpu.roll(from_low, 1, 1))

    def pack_z(out, f, both, m):
        m = f % group * wide + m
        pltpu.store(out.at[f // group], pltpu.roll(both, lax.rem(2 * m + 1, 128), 1), mask=half_lane == m)

    def upward(buf, e):
        for yb in range(yb_n):
            y = 8 + yb * 8
            accs = {}
            back = {}
            for b in (-1, 0, 1):
                v = buf[:, nx, y + b : y + b + 8]
                for c in (-1, 0, 1):
                    coef = w[FORWARD.index((1, -b, -c)), nx, y + b : y + b + 8]
                    term = coef[None] * v
                    accs[c] = term if c not in accs else accs[c] + term
                    back[c] = coef if c not in back else back[c] + coef
            whole = accs[0] + pltpu.roll(accs[1], 127, 2) + pltpu.roll(accs[-1], 1, 2)
            both = jnp.where(first_lane[None], accs[1], accs[-1])
            for f in range(nf):
                xsend[e, x_tile(f, yb)] = whole[f]
                pack_z(xsend.at[e], f, both[f], (deep - 1) * yb_n + yb)
            if e == 0:
                xsend[e, x_tile(nf, yb)] = (
                    back[0] + pltpu.roll(back[1], 127, 1) + pltpu.roll(back[-1], 1, 1))
                both = jnp.where(first_lane, back[1], back[-1])
                pack_z(xsend.at[e], nf, both, (deep - 1) * yb_n + yb)

    def sums(buf, e, x, lowest=False):
        for yb in range(yb_n):
            y = 8 + yb * 8
            accs = {}
            back = {}
            if lowest:
                accs[0] = jnp.stack([xrecv[e, x_tile(f, yb)] for f in range(nf)])
                if e == 0:
                    back[0] = xrecv[e, x_tile(nf, yb)]
            for a in (0, 1) if lowest else (-1, 0, 1):
                for b in (-1, 0, 1):
                    v = buf[:, x + 1 + a, y + b : y + b + 8]
                    for c in (-1, 0, 1):
                        o = (a, b, c)
                        if o == (0, 0, 0):
                            continue
                        if o > (0, 0, 0):
                            k = FORWARD.index(o)
                            if c == 0:
                                coef = w[k, x + 1, y : y + 8]
                            else:
                                coef = ws[SHIFTED.index(k), x, yb * 8 : yb * 8 + 8]
                        else:
                            k = FORWARD.index((-a, -b, -c))
                            coef = w[k, x + 1 + a, y + b : y + b + 8]
                            if e == 0:
                                back[c] = coef if c not in back else back[c] + coef
                        term = coef[None] * v
                        accs[c] = term if c not in accs else accs[c] + term
            if e == 0:
                total = s0[x, yb * 8 : yb * 8 + 8] + back[0]
                for k in range(13):
                    total = total + w[k, x + 1, y : y + 8]
                back[0] = total
            for c in (-1, 0, 1):
                scr[c + 1, yb, 0:nf] = accs[c]
                if e == 0:
                    scr[c + 1, yb, nf] = back[c]

    def settle(buf, e, x, put, chunk, where):
        for yb in range(yb_n):
            y = 8 + yb * 8
            m = where * yb_n + yb
            if e == 0:
                up, down = scr[2, yb, nf], scr[0, yb, nf]
                total = scr[1, yb, nf] + pltpu.roll(up, 127, 1) + pltpu.roll(down, 1, 1)
                diag[x, yb * 8 : yb * 8 + 8] = total
                pack_z(zsend.at[e, chunk], nf, jnp.where(first_lane, up, down), m)
            else:
                total = diag[x, yb * 8 : yb * 8 + 8]
            for f in range(nf):
                up, down = scr[2, yb, f], scr[0, yb, f]
                total_f = scr[1, yb, f] + pltpu.roll(up, 127, 1) + pltpu.roll(down, 1, 1)
                put(f, x, yb, total * buf[f, x + 1, y : y + 8] - total_f)
                pack_z(zsend.at[e, chunk], f, jnp.where(first_lane, up, down), m)

    def gather(e, chunk):
        for n in range(packs(e)):
            mine = zsend[e, chunk, n]
            ucross[chunk, n] = crossing(zrecv[e, chunk, 0, n] - mine, zrecv[e, chunk, 1, n] - mine)

    def mend(buf, e, x, get, put, chunk, where):
        for yb in range(yb_n):
            y = 8 + yb * 8
            m = where * yb_n + yb

            def edge(f):
                place = f % group * wide + m
                side = pltpu.roll(ucross[chunk, f // group], lax.rem(255 - 2 * place, 128), 1)
                return jnp.where(rim, side, 0.0)

            if e == 0:
                extra = edge(nf)
                diag[x, yb * 8 : yb * 8 + 8] += extra
            for f in range(nf):
                value = get(f, x, yb) - edge(f)
                if e == 0:
                    value = value + extra * buf[f, x + 1, y : y + 8]
                    if yb == yb_n - 1:
                        ysend[0, x, f : f + 1] = value[7:8]
                    if yb == 0:
                        ysend[1, x, f : f + 1] = value[0:1]
                put(f, x, yb, value)

    def copy_row(r, n, dst):
        return pltpu.make_async_remote_copy(
            src_ref=cur.at[r], dst_ref=slots.at[r, dst], send_sem=ars.at[r], recv_sem=arr.at[r],
            device_id=peer(offsets[n]), device_id_type=pl.DeviceIdType.MESH)

    def sum_start(r, value):
        value = jnp.sum(value, axis=0, keepdims=True)
        cur[r] = value
        slots[r, me] = value
        for n in range(devices - 1):
            copy_row(r, n, me).start()

    def sum_end(r):
        every = slots.at[r, pl.ds(0, devices - 1)]
        copies = pltpu.make_async_remote_copy(
            src_ref=every, dst_ref=every, send_sem=ars.at[r], recv_sem=arr.at[r],
            device_id=peer(offsets[0]), device_id_type=pl.DeviceIdType.MESH)
        copies.wait_send()
        copies.wait_recv()
        parts = [slots[r, q] for q in range(devices)]
        while len(parts) > 1:
            parts = [a + b for a, b in zip(parts[::2], parts[1::2])] + parts[len(parts) // 2 * 2 :]
        return jnp.broadcast_to(parts[0], (8, 128))

    def extract(total, g):
        cols = []
        for k in range(8):
            where = place(g, jnp.minimum(row, k), jnp.maximum(row, k))
            cols.append(jnp.broadcast_to(jnp.sum(jnp.where(lane == where, total, 0.0), axis=1, keepdims=True), (8, 128)))
        return cols

    def matrix(cols):
        out = jnp.zeros((8, 128), F32)
        for k in range(8):
            out = jnp.where(lane == k, cols[k], out)
        return out

    def fill(tab, cols):
        for j in range(8):
            for i in range(8):
                tab[i, j] = line(cols[j], i)

    def put_q1(f, x, yb, v):
        q0[f, x + 1, 8 + yb * 8 : 16 + yb * 8] = v

    def get_q1(f, x, yb):
        return q0[f, x + 1, 8 + yb * 8 : 16 + yb * 8]

    def put_q2(f, x, yb, v):
        q2[f, x, yb * 8 : yb * 8 + 8] = v

    def get_q2(f, x, yb):
        return q2[f, x, yb * 8 : yb * 8 + 8]

    def z_send(e, chunk):
        part = pl.ds(0, packs(e))
        return z_both(zsend.at[e, chunk, part], zrecv.at[e, chunk, :, part])

    def planes(buf, e, put, chunk):
        def body(t, carry):
            x = chunk * deep + 2 + t
            settle(buf, e, x - 1, put, chunk, t)
            sums(buf, e, x)
            return carry

        lax.fori_loop(0, deep, body, 0)
        return z_send(e, chunk)

    end = chunks - 1

    def interior(buf, e, put):
        sent = []
        sums(buf, e, 1)
        for n in range(end):
            with NS(f"op{e}_in{n}"):
                sent.append(planes(buf, e, put, n))
        with NS(f"op{e}_in{end}"):
            settle(buf, e, nx - 3, put, end, 0)
            sums(buf, e, nx - 2)
            settle(buf, e, nx - 2, put, end, 1)
        return sent

    def outer(buf, e, put, across):
        with NS(f"op{e}_xwait"):
            finish_all(across)
        with NS(f"op{e}_st3"):
            corners(buf, e)
            sums(buf, e, nx - 1)
            settle(buf, e, nx - 1, put, end, 2)
            sums(buf, e, 0, True)
            settle(buf, e, 0, put, end, 3)
            for n in range(packs(e)):
                zsend[e, end, n] += xrecv[e, n]
            return z_send(e, end)

    def mend_gram(buf, e, get, put, u, v, accs, chunk):
        for t in range(deep):
            x = chunk * deep + 1 + t
            mend(buf, e, x, get, put, chunk, t)
            accs = gram_plane(accs, u, v, x)
        return accs

    def mend_end(buf, e, get, put, between=None):
        for where, x in ((0, nx - 3), (1, nx - 2), (2, nx - 1), (3, 0)):
            mend(buf, e, x, get, put, end, where)
            if between and where == 2:
                between()

    rest = (nx - 1, 0, nx - 3, nx - 2)

    with NS("a_loadw"):
        loads[1].wait()
        rims = w_faces(1, nx)
    with NS("a_packw"):
        several(8, pack_w)
        zw = z_both(wzsend, wzrecv)
    with NS("a_loadp"):
        loads[0].wait()
        rims += y_faces(p0, nx, 1)
        down = x_down(p0, 0)
        sides = y_faces(p0, 1, nx - 1)
    with NS("a_gram0"):
        gacc[...] = gram(0, own(p0), own(p0))
    with NS("a_shiftw"):
        several(4, shift_w)
    with NS("a_up"):
        finish_all(rims)
        upward(p0, 0)
        up = x_up(0)
    with NS("a_zwait"):
        finish_all(zw)
    with NS("a_insw"):
        for n in range(len(LO)):
            uw[n] = crossing(wzrecv[0, n], wzrecv[1, n])
        several(8, insert_w)
    pl.semaphore_wait(ready.at[0], sizes["gx"] - 1)
    for d in lines:
        if d[1]:
            tell(ready.at[1], d)
    with NS("a_ywait"):
        loads[2].wait()
        finish_all(sides)
    sent = interior(p0, 0, put_q1)
    sent.append(outer(p0, 0, put_q1, down + up))

    def squares(lo, hi, accs):
        return lax.fori_loop(lo, hi, lambda x, accs: gram_plane(accs, own(q0), own(q0), x), accs)

    def hold(n, accs):
        for i in range(nf):
            held[n, i, i:nf] = accs[i]

    def resume(n):
        return tuple(held[n, i, i:nf] for i in range(nf))

    accs = gram_start()
    for n in range(end):
        with NS(f"b_zwait{n}"):
            finish_all(sent[n])
            gather(0, n)
        with NS(f"b_mend{n}"):
            accs = mend_gram(p0, 0, get_q1, put_q1, own(p0), own(q0), accs, n)
        if n:
            with NS(f"b_square{n}"):
                hold(0, accs)
                if n == end - 1:
                    sides = y_rows(1, end * deep)
                start = 1 if n == 1 else n * deep + 1
                hold(1, squares(start, (n + 1) * deep + 1, gram_start() if n == 1 else resume(1)))
                accs = resume(0)
    with NS(f"b_zwait{end}"):
        finish_all(sent[end])
        gather(0, end)
    rims = []
    with NS(f"b_mend{end}"):
        mend_end(p0, 0, get_q1, put_q1, lambda: rims.extend(y_rows(nx - 3, 3)))
        sides += y_rows(0, 1)
    with NS("b_gram1"):
        for x in rest:
            accs = gram_plane(accs, own(p0), own(q0), x)
        gacc[...] += gram_end(1, accs)
    with NS("b_gram2"):
        down = x_down(q0, 1)
        both = resume(1)
        for x in rest:
            both = gram_plane(both, own(q0), own(q0), x)
        both = gram_end(2, both)
    pl.semaphore_wait(ready.at[1], sizes["gy"] - 1)
    with NS("b_sum"):
        sum_start(0, gacc[...] + both)
    with NS("b_up"):
        finish_all(rims)
        y_unpack(nx - 3, 3)
        upward(q0, 1)
        up = x_up(1)
    with NS("b_ywait"):
        finish_all(sides)
        y_unpack(1, end * deep)
        y_unpack(0, 1)

    sent = interior(q0, 1, put_q2)

    def get_v2(x, yb):
        return q2[:, x, yb * 8 : yb * 8 + 8]

    with NS("c_sum1"):
        total = sum_end(0)
    with NS("c_alg1"):
        rrc, pqc, ssc = [extract(total, g) for g in range(3)]
        rr, pq = matrix(rrc), matrix(pqc)
        alpha = solve(pqc, rr, row)
        alpha_c = columns(alpha)
        fill(t_alpha, alpha_c)
        alpha_tc = columns(transposed(alpha, row, lane))
        ssa = mm(ssc, alpha)
        new = rr - mm(alpha_tc, pq) - mm(pqc, alpha) + mm(alpha_tc, ssa)
        beta = solve(rrc, new, row)
        fill(t_beta, columns(beta))
        ib = beta + jnp.where(lane == row, 1.0, 0.0)
        ib_tc = columns(transposed(ib, row, lane))
        fill(t_ib, columns(ib))
        left = mm(ib_tc, mm(pqc, ib) - ssa) - mm(alpha_tc, mm(ssc, ib))

    def early(x, carry):
        for yb in range(yb_n):
            y = slice(yb * 8, yb * 8 + 8)
            u, v = own(p0)(x, yb), own(q0)(x, yb)
            step, rest = t_alpha[0] * u[0][None], u
            for i in range(nf):
                if i:
                    step = step + t_alpha[i] * u[i][None]
                rest = rest - t_alpha[i] * v[i][None]
            x1[:, x, y] = step
            r1[:, x, y] = rest
        return carry

    def late(x, carry):
        for yb in range(yb_n):
            y = slice(yb * 8, yb * 8 + 8)
            u, v, z = own(p0)(x, yb), own(q0)(x, yb), get_v2(x, yb)
            step, image = r1[:, x, y], jnp.zeros((nf, 8, 128), F32)
            for i in range(nf):
                step = step + t_beta[i] * u[i][None]
                image = image + (t_ib[i] * v[i][None] - t_alpha[i] * z[i][None])
            p1[:, x, y] = step
            s1[:, x, y] = image
        return carry

    first, second = nx // 8, nx // 2
    with NS("c_early0"):
        lax.fori_loop(0, first, early, 0)
    sent.append(outer(q0, 1, put_q2, down + up))
    accs = gram_start()
    for n in range(end):
        with NS(f"c_zwait{n}"):
            finish_all(sent[n])
            gather(1, n)
        with NS(f"c_mend{n}"):
            accs = mend_gram(q0, 1, get_q2, put_q2, own(q0), get_v2, accs, n)
    with NS("c_early1"):
        lax.fori_loop(first, second, early, 0)
    with NS(f"c_zwait{end}"):
        finish_all(sent[end])
        gather(1, end)
    with NS(f"c_mend{end}"):
        mend_end(q0, 1, get_q2, put_q2)
        for x in rest:
            accs = gram_plane(accs, own(q0), get_v2, x)
        sum_start(1, gram_end(0, accs))
    with NS("c_early2"):
        lax.fori_loop(second, nx, early, 0)
    with NS("c_late"):
        lax.fori_loop(0, nx, late, 0)
    with NS("c_sum2"):
        total = sum_end(1)
    with NS("c_alg2"):
        curve = left + mm(alpha_tc, mm(extract(total, 0), alpha))
        fill(t_out, columns(solve(columns(curve), new, row)))


def final_kernel(dims, step, t, x1, r1, p1, s1, sol, res, sol_buf, res_buf, sem):
    nf, nx, ny = dims

    def saves(n):
        part = pl.ds(n * step, step)
        return [pltpu.make_async_copy(sol_buf.at[:, part], sol.at[:, part], sem.at[0]),
                pltpu.make_async_copy(res_buf.at[:, part], res.at[:, part], sem.at[1])]

    def body(n, carry):
        for k in range(step):
            x = n * step + k
            for yb in range(ny // 8):
                y = slice(yb * 8, yb * 8 + 8)
                u, v = p1[:, x, y], s1[:, x, y]
                s, e = x1[:, x, y], r1[:, x, y]
                for i in range(nf):
                    s = s + t[i] * u[i][None]
                    e = e - t[i] * v[i][None]
                sol_buf[:, x, y] = s
                res_buf[:, x, y] = e
        for copy in saves(n):
            copy.start()
        return carry

    lax.fori_loop(0, nx // step, body, 0)

    pltpu.make_async_copy(sol_buf, sol, sem.at[0]).wait()
    pltpu.make_async_copy(res_buf, res, sem.at[1]).wait()


def shards(sizes, rhs, stencil):
    nf, nx, ny, nz = rhs.shape
    tall = ny + 16
    field = jax.ShapeDtypeStruct(rhs.shape, F32)
    kept = pltpu.VMEM(rhs.shape, F32)
    table = pltpu.VMEM((8, 8, 8, nz), F32)
    anyspace = pl.BlockSpec(memory_space=pl.ANY)
    local = pl.BlockSpec(memory_space=pltpu.VMEM)
    devices = sizes["gx"] * sizes["gy"] * sizes["gz"]
    chunks, packs = nx // 4, nf // (16 // (ny // 8)) + 1
    padded = pltpu.VMEM((nf, nx + 2, tall, nz), F32)

    def kernel(*refs):
        main_kernel(sizes, (nf, nx, ny), *refs)

    x1, r1, p1, s1, t = pl.pallas_call(
        kernel,
        out_shape=(kept, kept, kept, kept, table),
        in_specs=[pl.BlockSpec(memory_space=pltpu.HBM)] * 2,
        out_specs=(local,) * 5,
        scratch_shapes=[
            padded, padded,
            pltpu.VMEM((13, nx + 1, tall, nz), F32),
            pltpu.VMEM((len(LO) + len(HI), nx, ny, nz), F32),
            pltpu.VMEM((nx, ny, nz), F32),
            pltpu.VMEM((nx, ny, nz), F32),
            pltpu.VMEM((nf, nx, ny, nz), F32),
            pltpu.VMEM((3, ny // 8, nf + 1, 8, nz), F32),
            pltpu.VMEM((2, 2, nf, nz), F32),
            pltpu.VMEM((2, 2, nf, nz), F32),
            pltpu.VMEM((2, packs + (nf + 1) * ny // 8, 8, nz), F32),
            pltpu.VMEM((2, packs + (nf + 1) * ny // 8, 8, nz), F32),
            pltpu.VMEM((2, nx, nf, nz), F32),
            pltpu.VMEM((2, nx, nf, nz), F32),
            pltpu.VMEM((2, chunks, packs, 8, nz), F32),
            pltpu.VMEM((2, chunks, 2, packs, 8, nz), F32),
            pltpu.VMEM((len(LO), 8, nz), F32),
            pltpu.VMEM((2, len(LO), 8, nz), F32),
            pltpu.VMEM((chunks, packs, 8, nz), F32),
            pltpu.VMEM((len(LO), 8, nz), F32),
            pltpu.VMEM((8, 8, 128), F32),
            pltpu.VMEM((2, 8, 8, 8, 128), F32),
            pltpu.VMEM((8, 128), F32),
            pltpu.VMEM((2, 1, 128), F32),
            pltpu.VMEM((2, devices, 1, 128), F32),
            table, table, table,
            pltpu.SemaphoreType.DMA((3,)),
            pltpu.SemaphoreType.DMA((SENDS,)),
            pltpu.SemaphoreType.DMA((RECEIVES,)),
            pltpu.SemaphoreType.DMA((2,)),
            pltpu.SemaphoreType.DMA((2,)),
            pltpu.SemaphoreType.REGULAR((2,)),
        ],
        compiler_params=pltpu.CompilerParams(
            collective_id=0, has_side_effects=True, vmem_limit_bytes=40 * 2**20),
        name="krylov",
    )(*[pltpu.with_memory_space_constraint(v, pltpu.HBM) for v in (rhs, stencil)])

    step = 2

    def last(*refs):
        final_kernel((nf, nx, ny), step, *refs)

    return pl.pallas_call(
        last,
        out_shape=(field, field),
        in_specs=[local] * 5,
        out_specs=(pl.BlockSpec(memory_space=pltpu.HBM),) * 2,
        scratch_shapes=[
            pltpu.VMEM(rhs.shape, F32), pltpu.VMEM(rhs.shape, F32),
            pltpu.SemaphoreType.DMA((2,)),
        ],
        compiler_params=pltpu.CompilerParams(vmem_limit_bytes=40 * 2**20),
        name="combine",
    )(t, x1, r1, p1, s1)


def solution(mesh):
    sizes = {a: mesh.shape[a] for a in AXES}
    spec = P(None, "gx", "gy", "gz")

    def run(rhs, stencil):
        return shards(sizes, rhs, stencil)

    return jax.shard_map(run, mesh=mesh, in_specs=(spec, spec), out_specs=(spec, spec), check_vma=False)
```

```python
import jax
import jax.numpy as jnp
from jax import lax
from jax.experimental import pallas as pl
from jax.experimental.pallas import tpu as pltpu
from jax.sharding import PartitionSpec as P

FORWARD = [
    (a, b, c) for a in (-1, 0, 1) for b in (-1, 0, 1) for c in (-1, 0, 1) if (a, b, c) > (0, 0, 0)
]
AXES = ("gx", "gy", "gz")
RECEIVES = 40
SENDS = 16
LO = [k for k, o in enumerate(FORWARD) if o[2] == 1]
HI = [k for k, o in enumerate(FORWARD) if o[2] == -1]
F32 = jnp.float32
NS = jax.named_scope


def runs(ks):
    out = []
    for k in ks:
        if out and out[-1][1] == k:
            out[-1][1] = k + 1
        else:
            out.append([k, k + 1])
    return out


def splat(a, k):
    return jnp.broadcast_to(a[:, k : k + 1], (8, 128))


def line(a, k):
    return jnp.broadcast_to(a[k : k + 1, :], (8, 128))


def columns(a):
    return [splat(a, k) for k in range(8)]


def mm(cols, b):
    parts = [cols[k] * line(b, k) for k in range(8)]
    while len(parts) > 1:
        parts = [parts[i] + parts[i + 1] for i in range(0, len(parts), 2)]
    return parts[0]


def solve(cols, b, row):
    cols = list(cols)
    for k in range(8):
        factor = cols[k]
        inverse = 1.0 / line(factor, k)
        pivot = line(b, k) * inverse
        b = jnp.where(row == k, pivot, b - factor * pivot)
        for j in range(k + 1, 8):
            pivot = line(cols[j], k) * inverse
            cols[j] = jnp.where(row == k, pivot, cols[j] - factor * pivot)
    return b


def transposed(a, row, lane):
    out = jnp.zeros_like(a)
    for i in range(8):
        across = jnp.sum(jnp.where(lane == row, a[:, i : i + 1], 0.0), axis=0, keepdims=True)
        out = out + jnp.where(row == i, across, 0.0)
    return out


def halves(v):
    v = v.reshape(64, 128)
    high = v.astype(jnp.bfloat16)
    low = (v - high.astype(F32)).astype(jnp.bfloat16)
    return jnp.concatenate([high, low], axis=0)


def mixed(coefs, tiles):
    out = jnp.dot(coefs, jnp.concatenate([halves(v) for v in tiles], axis=1), preferred_element_type=F32)
    half = out.shape[0] // 2
    out = out[:half] + out[half:]
    return [[out[m : m + 64, n * 128 : n * 128 + 128].reshape(8, 8, 128) for n in range(len(tiles))]
            for m in range(0, half, 64)]


def spread(cols, row, lane):
    slot = lax.rem(lane // 8, 8)
    high, low = [], []
    for j in range(8):
        block = jnp.zeros((8, 128), F32)
        for i in range(8):
            block = jnp.where(slot == i, line(cols[j], i), block)
        block = jnp.where(lax.rem(lane, 8) == row, block, 0.0)
        near = block.astype(jnp.bfloat16).astype(F32)
        high.append(near)
        low.append(jnp.where(lane < 64, block - near, 0.0))
    return high, low


def stacked(parts):
    rows = [v for high, low in parts for v in high] + [v for high, low in parts for v in low]
    return jnp.concatenate(rows, axis=0).astype(jnp.bfloat16)


def main_kernel(sizes, dims, rhs, sten, x1, r1, p1, s1, t_out, p0, q0, w, ws, s0, diag, q2, scr, csend, crecv,
                xsend, xrecv, ysend, yrecv, zsend, zrecv, wzsend, wzrecv, ucross, uw, red, held, gacc, cur, slots,
                t_rhs, t_one, t_two, lsem, xs, xr, ars, arr, ready):
    nf, nx, ny = dims
    yb_n = ny // 8
    tall = ny + 16
    group = 128 // (8 * yb_n)
    deep = 4
    wide = deep * yb_n
    chunks = nx // deep

    def packs(e):
        return (nf - e) // group + 1

    pos = {a: lax.axis_index(a) for a in AXES}
    lane = lax.broadcasted_iota(jnp.int32, (8, 128), 1)
    row = lax.broadcasted_iota(jnp.int32, (8, 128), 0)
    first_lane = lane == 0
    last_lane = lane == 127
    rim = first_lane | last_lane
    even = lax.rem(lane, 2) == 0
    half_lane = lane // 2
    ys = pl.ds(8, ny)
    SHIFTED = LO + HI

    devices = sizes["gx"] * sizes["gy"] * sizes["gz"]
    me = (pos["gx"] * sizes["gy"] + pos["gy"]) * sizes["gz"] + pos["gz"]

    loads = [
        pltpu.make_async_copy(rhs, p0.at[:, pl.ds(1, nx), ys], lsem.at[0]),
        pltpu.make_async_copy(sten.at[pl.ds(1, 13)], w.at[:, pl.ds(1, nx), ys], lsem.at[1]),
        pltpu.make_async_copy(sten.at[0], s0, lsem.at[2]),
    ]
    loads[1].start()
    loads[2].start()

    moved = {a: [lax.rem(pos[a] + d, sizes[a]) for d in range(sizes[a])] for a in AXES}
    offsets = [(i, j, k) for i in range(sizes["gx"]) for j in range(sizes["gy"]) for k in range(sizes["gz"])][1:]
    offsets.sort(key=lambda d: -sum(min(v, sizes[a] - v) for v, a in zip(d, AXES)))

    def peer(d):
        return {a: moved[a][v] for v, a in zip(d, AXES)}

    barrier = pltpu.get_barrier_semaphore()
    lines = [d for d in offsets if sum(v > 0 for v in d) == 1]
    across = {(i % sizes["gx"], j % sizes["gy"], 0) for i in (1, -1) for j in (1, -1)}
    met = lines + sorted(across & set(offsets) - set(lines))

    def tell(sem, d):
        pl.semaphore_signal(sem, inc=1, device_id=peer(d), device_id_type=pl.DeviceIdType.MESH)

    for d in met:
        tell(barrier, d)

    last = {a: sizes[a] - 1 for a in AXES}

    @pl.when(pos["gx"] == 0)
    def _():
        xrecv[...] = jnp.zeros(xrecv.shape, F32)

    loads[0].start()

    for side, place in ((0, 0), (1, last["gy"])):
        @pl.when((pos["gx"] == last["gx"]) | (pos["gy"] == place))
        def _():
            for e in range(2):
                crecv[e, side] = jnp.zeros((nf, 128), F32)

    @pl.when(pos["gx"] == last["gx"])
    def _():
        for buf in (p0, q0):
            buf[:, nx + 1, ys] = jnp.zeros((nf, ny, 128), F32)

    def clear_y(y):
        def body(x, carry):
            p0[:, x, y : y + 8] = jnp.zeros((nf, 8, 128), F32)
            return carry

        lax.fori_loop(1, nx + 1, body, 0)

        def body_w(x, carry):
            w[:, x, y : y + 8] = jnp.zeros((13, 8, 128), F32)
            return carry

        lax.fori_loop(1, nx + 1, body_w, 0)

    @pl.when(pos["gy"] == 0)
    def _():
        clear_y(0)
        yrecv[0] = jnp.zeros((nx, nf, 128), F32)

    @pl.when(pos["gy"] == last["gy"])
    def _():
        clear_y(ny + 8)
        yrecv[1] = jnp.zeros((nx, nf, 128), F32)

    for side, place in ((0, 0), (1, last["gz"])):
        @pl.when(pos["gz"] == place)
        def _():
            for e in range(2):
                for n in range(chunks):
                    zrecv[e, n, side] = jnp.zeros(zrecv.shape[3:], F32)
            wzrecv[side] = jnp.zeros((len(LO), 8, 128), F32)

    zsend[...] = jnp.zeros(zsend.shape, F32)
    for e in range(2):
        for n in range(packs(e)):
            xsend[e, n] = jnp.zeros((8, 128), F32)
    wzsend[...] = jnp.zeros(wzsend.shape, F32)

    pl.semaphore_wait(barrier, len(met))
    for d in lines:
        if d[0]:
            tell(ready.at[0], d)

    arrivals = iter(range(RECEIVES))
    free = list(range(SENDS))

    def shift(axis, up, src, dst):
        n = sizes[axis]
        i = pos[axis]
        slot = free.pop(0)
        copy = pltpu.make_async_remote_copy(
            src_ref=src, dst_ref=dst, send_sem=xs.at[slot], recv_sem=xr.at[next(arrivals)],
            device_id={axis: lax.rem(i + (1 if up else n - 1), n)},
            device_id_type=pl.DeviceIdType.MESH)
        sends = i < n - 1 if up else i > 0
        gets = i > 0 if up else i < n - 1

        @pl.when(sends)
        def _():
            copy.start()

        def finish():
            @pl.when(sends)
            def _():
                copy.wait_send()

            @pl.when(gets)
            def _():
                copy.wait_recv()

            free.append(slot)

        return finish

    def finish_all(items):
        for f in items:
            f()

    def y_faces(buf, start, length):
        xs_ = pl.ds(start, length)
        return [
            shift("gy", True, buf.at[:, xs_, pl.ds(ny, 8)], buf.at[:, xs_, pl.ds(0, 8)]),
            shift("gy", False, buf.at[:, xs_, pl.ds(8, 8)], buf.at[:, xs_, pl.ds(ny + 8, 8)]),
        ]

    def y_rows(start, length):
        part = pl.ds(start, length)
        return [
            shift("gy", True, ysend.at[0, part], yrecv.at[0, part]),
            shift("gy", False, ysend.at[1, part], yrecv.at[1, part]),
        ]

    def y_unpack(start, length):
        def body(x, carry):
            for f in range(nf):
                q0[f, x + 1, 7:8] = yrecv[0, x, f : f + 1]
                q0[f, x + 1, ny + 8 : ny + 9] = yrecv[1, x, f : f + 1]
            return carry

        if length > 3:
            lax.fori_loop(start, start + length, body, 0)
        else:
            for x in range(start, start + length):
                body(x, 0)

    def w_faces(start, length):
        xs_ = pl.ds(start, length)
        out = []
        for b, up, src, dst in ((1, True, ny, 0), (-1, False, 8, ny + 8)):
            for lo, hi in runs([k for k, o in enumerate(FORWARD) if o[1] == b]):
                ks = pl.ds(lo, hi - lo)
                out.append(shift("gy", up, w.at[ks, xs_, pl.ds(src, 8)], w.at[ks, xs_, pl.ds(dst, 8)]))
        return out

    def corner(e, up):
        side = 0 if up else 1
        i, j = pos["gx"], pos["gy"]
        slot = free.pop(0)
        copy = pltpu.make_async_remote_copy(
            src_ref=csend.at[e, side], dst_ref=crecv.at[e, side], send_sem=xs.at[slot], recv_sem=xr.at[next(arrivals)],
            device_id={"gx": moved["gx"][-1], "gy": moved["gy"][1 if up else -1]},
            device_id_type=pl.DeviceIdType.MESH)
        sends = (i > 0) & (j < last["gy"] if up else j > 0)
        gets = (i < last["gx"]) & (j > 0 if up else j < last["gy"])

        @pl.when(sends)
        def _():
            copy.start()

        def finish():
            @pl.when(sends)
            def _():
                copy.wait_send()

            @pl.when(gets)
            def _():
                copy.wait_recv()

            free.append(slot)

        return finish

    def x_down(buf, e):
        for f in range(nf):
            csend[e, 0, f : f + 1] = buf[f, 1, ny + 7 : ny + 8]
            csend[e, 1, f : f + 1] = buf[f, 1, 8:9]
        return [shift("gx", False, buf.at[:, 1, ys], buf.at[:, nx + 1, ys]), corner(e, True), corner(e, False)]

    def corners(buf, e):
        for f in range(nf):
            buf[f, nx + 1, 7:8] = crecv[e, 0, f : f + 1]
            buf[f, nx + 1, ny + 8 : ny + 9] = crecv[e, 1, f : f + 1]

    def x_tile(f, yb):
        return packs(0) + f * yb_n + yb

    def x_up(e):
        part = pl.ds(0, x_tile(nf - e, yb_n))
        return [shift("gx", True, xsend.at[e, part], xrecv.at[e, part])]

    def z_both(send, recv):
        return [
            shift("gz", True, send, recv.at[0]),
            shift("gz", False, send, recv.at[1]),
        ]

    def gram_body(accs, ub, vb):
        return [accs[i] + ub[i : i + 1] * vb[i:] for i in range(nf)]

    def gram_start():
        return tuple(jnp.zeros((nf - i, 8, 128), F32) for i in range(nf))

    def place(g, i, j):
        return 36 * g + 8 * i - i * (i - 1) // 2 + j - i

    def gram_end(g, accs):
        red[...] = jnp.zeros(red.shape, F32)
        for i in range(nf):
            red[i, i:nf, :] = jnp.sum(accs[i], axis=1)
        out = jnp.zeros((8, 128), F32)
        for i in range(nf):
            t = jnp.sum(red[i], axis=1, keepdims=True)
            out = out + jnp.where(lane == place(g, i, row), t, 0.0)
        return out

    def own(buf):
        return lambda x, yb: buf[:, x + 1, 8 + yb * 8 : 16 + yb * 8]

    def gram_plane(accs, u, v, x):
        for yb in range(yb_n):
            accs = gram_body(accs, u(x, yb), v(x, yb))
        return tuple(accs)

    def gram(g, u, v):
        return gram_end(g, lax.fori_loop(0, nx, lambda x, accs: gram_plane(accs, u, v, x), gram_start()))

    def several(n, f):
        def body(t, carry):
            for k in range(n):
                f(t * n + k, 0)
            return carry

        lax.fori_loop(0, nx // n, body, 0)

    def pack_w(x, carry):
        for yb in range(yb_n):
            j = x * yb_n + yb
            here = half_lane == j
            y = 8 + yb * 8
            for n, k in enumerate(LO):
                both = w[k, x + 1, y : y + 8]
                if n < len(HI):
                    both = jnp.where(first_lane, w[HI[n], x + 1, y : y + 8], both)
                pltpu.store(wzsend.at[n], pltpu.roll(both, 2 * j + 1, 1), mask=here)
        return carry

    def shift_w(x, carry):
        for yb in range(yb_n):
            y = 8 + yb * 8
            for n, k in enumerate(SHIFTED):
                ws[n, x, yb * 8 : yb * 8 + 8] = pltpu.roll(w[k, x + 1, y : y + 8], 1 if k in LO else 127, 1)
        return carry

    def insert_w(x, carry):
        for yb in range(yb_n):
            j = x * yb_n + yb
            for n in range(len(LO)):
                edge = pltpu.roll(uw[n], 127 - 2 * j, 1)
                pltpu.store(ws.at[n, x, yb * 8 : yb * 8 + 8], edge, mask=first_lane)
                if n < len(HI):
                    pltpu.store(ws.at[len(LO) + n, x, yb * 8 : yb * 8 + 8], edge, mask=last_lane)
        return carry

    def crossing(from_low, from_high):
        return jnp.where(even, pltpu.roll(from_high, 127, 1), pltpu.roll(from_low, 1, 1))

    def pack_z(out, f, both, m):
        m = f % group * wide + m
        pltpu.store(out.at[f // group], pltpu.roll(both, lax.rem(2 * m + 1, 128), 1), mask=half_lane == m)

    def upward(buf, e):
        for yb in range(yb_n):
            y = 8 + yb * 8
            accs = {}
            back = {}
            for b in (-1, 0, 1):
                v = buf[:, nx, y + b : y + b + 8]
                for c in (-1, 0, 1):
                    coef = w[FORWARD.index((1, -b, -c)), nx, y + b : y + b + 8]
                    term = coef[None] * v
                    accs[c] = term if c not in accs else accs[c] + term
                    back[c] = coef if c not in back else back[c] + coef
            whole = accs[0] + pltpu.roll(accs[1], 127, 2) + pltpu.roll(accs[-1], 1, 2)
            both = jnp.where(first_lane[None], accs[1], accs[-1])
            for f in range(nf):
                xsend[e, x_tile(f, yb)] = whole[f]
                pack_z(xsend.at[e], f, both[f], (deep - 1) * yb_n + yb)
            if e == 0:
                xsend[e, x_tile(nf, yb)] = (
                    back[0] + pltpu.roll(back[1], 127, 1) + pltpu.roll(back[-1], 1, 1))
                both = jnp.where(first_lane, back[1], back[-1])
                pack_z(xsend.at[e], nf, both, (deep - 1) * yb_n + yb)

    def sums(buf, e, x, lowest=False):
        for yb in range(yb_n):
            y = 8 + yb * 8
            accs = {}
            back = {}
            if lowest:
                accs[0] = jnp.stack([xrecv[e, x_tile(f, yb)] for f in range(nf)])
                if e == 0:
                    back[0] = xrecv[e, x_tile(nf, yb)]
            for a in (0, 1) if lowest else (-1, 0, 1):
                for b in (-1, 0, 1):
                    v = buf[:, x + 1 + a, y + b : y + b + 8]
                    for c in (-1, 0, 1):
                        o = (a, b, c)
                        if o == (0, 0, 0):
                            continue
                        if o > (0, 0, 0):
                            k = FORWARD.index(o)
                            if c == 0:
                                coef = w[k, x + 1, y : y + 8]
                            else:
                                coef = ws[SHIFTED.index(k), x, yb * 8 : yb * 8 + 8]
                        else:
                            k = FORWARD.index((-a, -b, -c))
                            coef = w[k, x + 1 + a, y + b : y + b + 8]
                            if e == 0:
                                back[c] = coef if c not in back else back[c] + coef
                        term = coef[None] * v
                        accs[c] = term if c not in accs else accs[c] + term
            if e == 0:
                total = s0[x, yb * 8 : yb * 8 + 8] + back[0]
                for k in range(13):
                    total = total + w[k, x + 1, y : y + 8]
                back[0] = total
            for c in (-1, 0, 1):
                scr[c + 1, yb, 0:nf] = accs[c]
                if e == 0:
                    scr[c + 1, yb, nf] = back[c]

    def settle(buf, e, x, put, chunk, where):
        for yb in range(yb_n):
            y = 8 + yb * 8
            m = where * yb_n + yb
            if e == 0:
                up, down = scr[2, yb, nf], scr[0, yb, nf]
                total = scr[1, yb, nf] + pltpu.roll(up, 127, 1) + pltpu.roll(down, 1, 1)
                diag[x, yb * 8 : yb * 8 + 8] = total
                pack_z(zsend.at[e, chunk], nf, jnp.where(first_lane, up, down), m)
            else:
                total = diag[x, yb * 8 : yb * 8 + 8]
            for f in range(nf):
                up, down = scr[2, yb, f], scr[0, yb, f]
                total_f = scr[1, yb, f] + pltpu.roll(up, 127, 1) + pltpu.roll(down, 1, 1)
                put(f, x, yb, total * buf[f, x + 1, y : y + 8] - total_f)
                pack_z(zsend.at[e, chunk], f, jnp.where(first_lane, up, down), m)

    def gather(e, chunk):
        for n in range(packs(e)):
            mine = zsend[e, chunk, n]
            ucross[chunk, n] = crossing(zrecv[e, chunk, 0, n] - mine, zrecv[e, chunk, 1, n] - mine)

    def mend(buf, e, x, get, put, chunk, where):
        for yb in range(yb_n):
            y = 8 + yb * 8
            m = where * yb_n + yb

            def edge(f):
                place = f % group * wide + m
                side = pltpu.roll(ucross[chunk, f // group], lax.rem(255 - 2 * place, 128), 1)
                return jnp.where(rim, side, 0.0)

            if e == 0:
                extra = edge(nf)
                diag[x, yb * 8 : yb * 8 + 8] += extra
            for f in range(nf):
                value = get(f, x, yb) - edge(f)
                if e == 0:
                    value = value + extra * buf[f, x + 1, y : y + 8]
                    if yb == yb_n - 1:
                        ysend[0, x, f : f + 1] = value[7:8]
                    if yb == 0:
                        ysend[1, x, f : f + 1] = value[0:1]
                put(f, x, yb, value)

    def copy_row(r, n, dst):
        return pltpu.make_async_remote_copy(
            src_ref=cur.at[r], dst_ref=slots.at[r, dst], send_sem=ars.at[r], recv_sem=arr.at[r],
            device_id=peer(offsets[n]), device_id_type=pl.DeviceIdType.MESH)

    def sum_start(r, value):
        value = jnp.sum(value, axis=0, keepdims=True)
        cur[r] = value
        slots[r, me] = value
        for n in range(devices - 1):
            copy_row(r, n, me).start()

    def sum_end(r):
        every = slots.at[r, pl.ds(0, devices - 1)]
        copies = pltpu.make_async_remote_copy(
            src_ref=every, dst_ref=every, send_sem=ars.at[r], recv_sem=arr.at[r],
            device_id=peer(offsets[0]), device_id_type=pl.DeviceIdType.MESH)
        copies.wait_send()
        copies.wait_recv()
        parts = [slots[r, q] for q in range(devices)]
        while len(parts) > 1:
            parts = [a + b for a, b in zip(parts[::2], parts[1::2])] + parts[len(parts) // 2 * 2 :]
        return jnp.broadcast_to(parts[0], (8, 128))

    def extract(total, g):
        cols = []
        for k in range(8):
            where = place(g, jnp.minimum(row, k), jnp.maximum(row, k))
            cols.append(jnp.broadcast_to(jnp.sum(jnp.where(lane == where, total, 0.0), axis=1, keepdims=True), (8, 128)))
        return cols

    def matrix(cols):
        out = jnp.zeros((8, 128), F32)
        for k in range(8):
            out = jnp.where(lane == k, cols[k], out)
        return out

    def put_q1(f, x, yb, v):
        q0[f, x + 1, 8 + yb * 8 : 16 + yb * 8] = v

    def get_q1(f, x, yb):
        return q0[f, x + 1, 8 + yb * 8 : 16 + yb * 8]

    def put_q2(f, x, yb, v):
        q2[f, x, yb * 8 : yb * 8 + 8] = v

    def get_q2(f, x, yb):
        return q2[f, x, yb * 8 : yb * 8 + 8]

    def z_send(e, chunk):
        part = pl.ds(0, packs(e))
        return z_both(zsend.at[e, chunk, part], zrecv.at[e, chunk, :, part])

    def planes(buf, e, put, chunk):
        def body(t, carry):
            x = chunk * deep + 2 + t
            settle(buf, e, x - 1, put, chunk, t)
            sums(buf, e, x)
            return carry

        lax.fori_loop(0, deep, body, 0)
        return z_send(e, chunk)

    end = chunks - 1

    def interior(buf, e, put):
        sent = []
        sums(buf, e, 1)
        for n in range(end):
            with NS(f"op{e}_in{n}"):
                sent.append(planes(buf, e, put, n))
        with NS(f"op{e}_in{end}"):
            settle(buf, e, nx - 3, put, end, 0)
            sums(buf, e, nx - 2)
            settle(buf, e, nx - 2, put, end, 1)
        return sent

    def outer(buf, e, put, across):
        with NS(f"op{e}_xwait"):
            finish_all(across)
        with NS(f"op{e}_st3"):
            corners(buf, e)
            sums(buf, e, nx - 1)
            settle(buf, e, nx - 1, put, end, 2)
            sums(buf, e, 0, True)
            settle(buf, e, 0, put, end, 3)
            for n in range(packs(e)):
                zsend[e, end, n] += xrecv[e, n]
            return z_send(e, end)

    def mend_gram(buf, e, get, put, u, v, accs, chunk):
        for t in range(deep):
            x = chunk * deep + 1 + t
            mend(buf, e, x, get, put, chunk, t)
            accs = gram_plane(accs, u, v, x)
        return accs

    def mend_end(buf, e, get, put, between=None):
        for where, x in ((0, nx - 3), (1, nx - 2), (2, nx - 1), (3, 0)):
            mend(buf, e, x, get, put, end, where)
            if between and where == 2:
                between()

    rest = (nx - 1, 0, nx - 3, nx - 2)

    with NS("a_loadw"):
        loads[1].wait()
        rims = w_faces(1, nx)
    with NS("a_packw"):
        several(8, pack_w)
        zw = z_both(wzsend, wzrecv)
    with NS("a_loadp"):
        loads[0].wait()
        rims += y_faces(p0, nx, 1)
        down = x_down(p0, 0)
        sides = y_faces(p0, 1, nx - 1)
    with NS("a_gram0"):
        gacc[...] = gram(0, own(p0), own(p0))
    with NS("a_shiftw"):
        several(4, shift_w)
    with NS("a_up"):
        finish_all(rims)
        upward(p0, 0)
        up = x_up(0)
    with NS("a_zwait"):
        finish_all(zw)
    with NS("a_insw"):
        for n in range(len(LO)):
            uw[n] = crossing(wzrecv[0, n], wzrecv[1, n])
        several(8, insert_w)
    pl.semaphore_wait(ready.at[0], sizes["gx"] - 1)
    for d in lines:
        if d[1]:
            tell(ready.at[1], d)
    with NS("a_ywait"):
        loads[2].wait()
        finish_all(sides)
    sent = interior(p0, 0, put_q1)
    sent.append(outer(p0, 0, put_q1, down + up))

    def squares(lo, hi, accs):
        return lax.fori_loop(lo, hi, lambda x, accs: gram_plane(accs, own(q0), own(q0), x), accs)

    def hold(n, accs):
        for i in range(nf):
            held[n, i, i:nf] = accs[i]

    def resume(n):
        return tuple(held[n, i, i:nf] for i in range(nf))

    accs = gram_start()
    for n in range(end):
        with NS(f"b_zwait{n}"):
            finish_all(sent[n])
            gather(0, n)
        with NS(f"b_mend{n}"):
            accs = mend_gram(p0, 0, get_q1, put_q1, own(p0), own(q0), accs, n)
        if n:
            with NS(f"b_square{n}"):
                hold(0, accs)
                if n == end - 1:
                    sides = y_rows(1, end * deep)
                start = 1 if n == 1 else n * deep + 1
                hold(1, squares(start, (n + 1) * deep + 1, gram_start() if n == 1 else resume(1)))
                accs = resume(0)
    with NS(f"b_zwait{end}"):
        finish_all(sent[end])
        gather(0, end)
    rims = []
    with NS(f"b_mend{end}"):
        mend_end(p0, 0, get_q1, put_q1, lambda: rims.extend(y_rows(nx - 3, 3)))
        sides += y_rows(0, 1)
    with NS("b_gram1"):
        for x in rest:
            accs = gram_plane(accs, own(p0), own(q0), x)
        gacc[...] += gram_end(1, accs)
    with NS("b_gram2"):
        down = x_down(q0, 1)
        both = resume(1)
        for x in rest:
            both = gram_plane(both, own(q0), own(q0), x)
        both = gram_end(2, both)
    pl.semaphore_wait(ready.at[1], sizes["gy"] - 1)
    with NS("b_sum"):
        sum_start(0, gacc[...] + both)
    with NS("b_up"):
        finish_all(rims)
        y_unpack(nx - 3, 3)
        upward(q0, 1)
        up = x_up(1)
    with NS("b_ywait"):
        finish_all(sides)
        y_unpack(1, end * deep)
        y_unpack(0, 1)

    sent = interior(q0, 1, put_q2)

    def get_v2(x, yb):
        return q2[:, x, yb * 8 : yb * 8 + 8]

    with NS("c_sum1"):
        total = sum_end(0)
    with NS("c_alg1"):
        rrc, pqc, ssc = [extract(total, g) for g in range(3)]
        rr, pq = matrix(rrc), matrix(pqc)
        alpha = solve(pqc, rr, row)
        alpha_c = columns(alpha)
        alpha_tc = columns(transposed(alpha, row, lane))
        ssa = mm(ssc, alpha)
        new = rr - mm(alpha_tc, pq) - mm(pqc, alpha) + mm(alpha_tc, ssa)
        beta = solve(rrc, new, row)
        ib = beta + jnp.where(lane == row, 1.0, 0.0)
        ib_tc = columns(transposed(ib, row, lane))
        wide_a, wide_b, wide_i = [spread(c, row, lane) for c in (alpha_c, columns(beta), columns(ib))]
        t_rhs[...] = stacked([wide_a, wide_b])
        t_one[...] = stacked([wide_a, wide_i])
        t_two[...] = stacked([wide_a])
        left = mm(ib_tc, mm(pqc, ib) - ssa) - mm(alpha_tc, mm(ssc, ib))

    def late(x):
        u, v, z = [[g(x, yb) for yb in range(yb_n)] for g in (own(p0), own(q0), get_v2)]
        step, turn = mixed(t_rhs[...], u)
        drop, grow = mixed(t_one[...], v)
        (fall,) = mixed(t_two[...], z)
        for yb in range(yb_n):
            y = slice(yb * 8, yb * 8 + 8)
            left_over = u[yb] - drop[yb]
            x1[:, x, y] = step[yb]
            r1[:, x, y] = left_over
            p1[:, x, y] = left_over + turn[yb]
            s1[:, x, y] = grow[yb] - fall[yb]

    sent.append(outer(q0, 1, put_q2, down + up))
    accs = gram_start()
    for n in range(end):
        with NS(f"c_zwait{n}"):
            finish_all(sent[n])
            gather(1, n)
        with NS(f"c_mend{n}"):
            accs = mend_gram(q0, 1, get_q2, put_q2, own(q0), get_v2, accs, n)
    with NS(f"c_zwait{end}"):
        finish_all(sent[end])
        gather(1, end)
    with NS(f"c_mend{end}"):
        mend_end(q0, 1, get_q2, put_q2)
        for x in rest:
            accs = gram_plane(accs, own(q0), get_v2, x)
        sum_start(1, gram_end(0, accs))
    with NS("c_late"):
        several(4, lambda x, carry: late(x))
    with NS("c_sum2"):
        total = sum_end(1)
    with NS("c_alg2"):
        curve = left + mm(alpha_tc, mm(extract(total, 0), alpha))
        t_out[...] = stacked([spread(columns(solve(columns(curve), new, row)), row, lane)])


def final_kernel(dims, step, t, x1, r1, p1, s1, sol, res, sol_buf, res_buf, sem):
    nf, nx, ny = dims

    def saves(n):
        part = pl.ds(n * step, step)
        return [pltpu.make_async_copy(sol_buf.at[:, part], sol.at[:, part], sem.at[0]),
                pltpu.make_async_copy(res_buf.at[:, part], res.at[:, part], sem.at[1])]

    blocks = [slice(yb * 8, yb * 8 + 8) for yb in range(ny // 8)]

    def applied(d, x):
        return mixed(t[...], [d[:, x, y] for y in blocks])[0]

    def body(n, carry):
        for k in range(step):
            x = n * step + k
            for y, v in zip(blocks, applied(p1, x)):
                sol_buf[:, x, y] = x1[:, x, y] + v
            for y, v in zip(blocks, applied(s1, x)):
                res_buf[:, x, y] = r1[:, x, y] - v
        for copy in saves(n):
            copy.start()
        return carry

    lax.fori_loop(0, nx // step, body, 0)

    pltpu.make_async_copy(sol_buf, sol, sem.at[0]).wait()
    pltpu.make_async_copy(res_buf, res, sem.at[1]).wait()


def shards(sizes, rhs, stencil):
    nf, nx, ny, nz = rhs.shape
    tall = ny + 16
    field = jax.ShapeDtypeStruct(rhs.shape, F32)
    kept = pltpu.VMEM(rhs.shape, F32)
    anyspace = pl.BlockSpec(memory_space=pl.ANY)
    local = pl.BlockSpec(memory_space=pltpu.VMEM)
    devices = sizes["gx"] * sizes["gy"] * sizes["gz"]
    chunks, packs = nx // 4, nf // (16 // (ny // 8)) + 1
    padded = pltpu.VMEM((nf, nx + 2, tall, nz), F32)

    def kernel(*refs):
        main_kernel(sizes, (nf, nx, ny), *refs)

    x1, r1, p1, s1, t = pl.pallas_call(
        kernel,
        out_shape=(kept, kept, kept, kept, pltpu.VMEM((128, 128), jnp.bfloat16)),
        in_specs=[pl.BlockSpec(memory_space=pltpu.HBM)] * 2,
        out_specs=(local,) * 5,
        scratch_shapes=[
            padded, padded,
            pltpu.VMEM((13, nx + 1, tall, nz), F32),
            pltpu.VMEM((len(LO) + len(HI), nx, ny, nz), F32),
            pltpu.VMEM((nx, ny, nz), F32),
            pltpu.VMEM((nx, ny, nz), F32),
            pltpu.VMEM((nf, nx, ny, nz), F32),
            pltpu.VMEM((3, ny // 8, nf + 1, 8, nz), F32),
            pltpu.VMEM((2, 2, nf, nz), F32),
            pltpu.VMEM((2, 2, nf, nz), F32),
            pltpu.VMEM((2, packs + (nf + 1) * ny // 8, 8, nz), F32),
            pltpu.VMEM((2, packs + (nf + 1) * ny // 8, 8, nz), F32),
            pltpu.VMEM((2, nx, nf, nz), F32),
            pltpu.VMEM((2, nx, nf, nz), F32),
            pltpu.VMEM((2, chunks, packs, 8, nz), F32),
            pltpu.VMEM((2, chunks, 2, packs, 8, nz), F32),
            pltpu.VMEM((len(LO), 8, nz), F32),
            pltpu.VMEM((2, len(LO), 8, nz), F32),
            pltpu.VMEM((chunks, packs, 8, nz), F32),
            pltpu.VMEM((len(LO), 8, nz), F32),
            pltpu.VMEM((8, 8, 128), F32),
            pltpu.VMEM((2, 8, 8, 8, 128), F32),
            pltpu.VMEM((8, 128), F32),
            pltpu.VMEM((2, 1, 128), F32),
            pltpu.VMEM((2, devices, 1, 128), F32),
            pltpu.VMEM((256, 128), jnp.bfloat16),
            pltpu.VMEM((256, 128), jnp.bfloat16),
            pltpu.VMEM((128, 128), jnp.bfloat16),
            pltpu.SemaphoreType.DMA((3,)),
            pltpu.SemaphoreType.DMA((SENDS,)),
            pltpu.SemaphoreType.DMA((RECEIVES,)),
            pltpu.SemaphoreType.DMA((2,)),
            pltpu.SemaphoreType.DMA((2,)),
            pltpu.SemaphoreType.REGULAR((2,)),
        ],
        compiler_params=pltpu.CompilerParams(
            collective_id=0, has_side_effects=True, vmem_limit_bytes=40 * 2**20),
        name="krylov",
    )(*[pltpu.with_memory_space_constraint(v, pltpu.HBM) for v in (rhs, stencil)])

    step = 4

    def last(*refs):
        final_kernel((nf, nx, ny), step, *refs)

    return pl.pallas_call(
        last,
        out_shape=(field, field),
        in_specs=[local] * 5,
        out_specs=(pl.BlockSpec(memory_space=pltpu.HBM),) * 2,
        scratch_shapes=[
            pltpu.VMEM(rhs.shape, F32), pltpu.VMEM(rhs.shape, F32),
            pltpu.SemaphoreType.DMA((2,)),
        ],
        compiler_params=pltpu.CompilerParams(vmem_limit_bytes=40 * 2**20),
        name="combine",
    )(t, x1, r1, p1, s1)


def solution(mesh):
    sizes = {a: mesh.shape[a] for a in AXES}
    spec = P(None, "gx", "gy", "gz")

    def run(rhs, stencil):
        return shards(sizes, rhs, stencil)

    return jax.shard_map(run, mesh=mesh, in_specs=(spec, spec), out_specs=(spec, spec), check_vma=False)
```

```python
import jax
import jax.numpy as jnp
from jax import lax
from jax.experimental import pallas as pl
from jax.experimental.pallas import tpu as pltpu
from jax.sharding import PartitionSpec as P

FORWARD = [
    (a, b, c) for a in (-1, 0, 1) for b in (-1, 0, 1) for c in (-1, 0, 1) if (a, b, c) > (0, 0, 0)
]
AXES = ("gx", "gy", "gz")
RECEIVES = 40
SENDS = 16
LO = [k for k, o in enumerate(FORWARD) if o[2] == 1]
HI = [k for k, o in enumerate(FORWARD) if o[2] == -1]
F32 = jnp.float32
NS = jax.named_scope


def runs(ks):
    out = []
    for k in ks:
        if out and out[-1][1] == k:
            out[-1][1] = k + 1
        else:
            out.append([k, k + 1])
    return out


def splat(a, k):
    return jnp.broadcast_to(a[:, k : k + 1], (8, 128))


def line(a, k):
    return jnp.broadcast_to(a[k : k + 1, :], (8, 128))


def columns(a):
    return [splat(a, k) for k in range(8)]


def mm(cols, b):
    parts = [cols[k] * line(b, k) for k in range(8)]
    while len(parts) > 1:
        parts = [parts[i] + parts[i + 1] for i in range(0, len(parts), 2)]
    return parts[0]


def solve(cols, b, row):
    cols = list(cols)
    for k in range(8):
        factor = cols[k]
        inverse = 1.0 / line(factor, k)
        pivot = line(b, k) * inverse
        b = jnp.where(row == k, pivot, b - factor * pivot)
        for j in range(k + 1, 8):
            pivot = line(cols[j], k) * inverse
            cols[j] = jnp.where(row == k, pivot, cols[j] - factor * pivot)
    return b


def transposed(a, row, lane):
    out = jnp.zeros_like(a)
    for i in range(8):
        across = jnp.sum(jnp.where(lane == row, a[:, i : i + 1], 0.0), axis=0, keepdims=True)
        out = out + jnp.where(row == i, across, 0.0)
    return out


def main_kernel(sizes, dims, rhs, sten, x1, r1, p1, s1, t_out, m_out, p0, q0, w, ws, s0, diag, q2, scr, csend, crecv,
                xsend, xrecv, ysend, yrecv, zsend, zrecv, wzsend, wzrecv, ucross, uw, red, held, gacc, cur, slots,
                t_alpha, t_beta, t_ib, lsem, xs, xr, ars, arr, ready):
    nf, nx, ny = dims
    yb_n = ny // 8
    tall = ny + 16
    group = 128 // (8 * yb_n)
    deep = 4
    wide = deep * yb_n
    chunks = nx // deep

    def packs(e):
        return (nf - e) // group + 1

    pos = {a: lax.axis_index(a) for a in AXES}
    lane = lax.broadcasted_iota(jnp.int32, (8, 128), 1)
    row = lax.broadcasted_iota(jnp.int32, (8, 128), 0)
    first_lane = lane == 0
    last_lane = lane == 127
    rim = first_lane | last_lane
    even = lax.rem(lane, 2) == 0
    half_lane = lane // 2
    ys = pl.ds(8, ny)
    SHIFTED = LO + HI

    devices = sizes["gx"] * sizes["gy"] * sizes["gz"]
    me = (pos["gx"] * sizes["gy"] + pos["gy"]) * sizes["gz"] + pos["gz"]

    loads = [
        pltpu.make_async_copy(rhs, p0.at[:, pl.ds(1, nx), ys], lsem.at[0]),
        pltpu.make_async_copy(sten.at[pl.ds(1, 13)], w.at[:, pl.ds(1, nx), ys], lsem.at[1]),
        pltpu.make_async_copy(sten.at[0], s0, lsem.at[2]),
    ]
    loads[1].start()
    loads[2].start()

    moved = {a: [lax.rem(pos[a] + d, sizes[a]) for d in range(sizes[a])] for a in AXES}
    offsets = [(i, j, k) for i in range(sizes["gx"]) for j in range(sizes["gy"]) for k in range(sizes["gz"])][1:]
    offsets.sort(key=lambda d: -sum(min(v, sizes[a] - v) for v, a in zip(d, AXES)))

    def peer(d):
        return {a: moved[a][v] for v, a in zip(d, AXES)}

    barrier = pltpu.get_barrier_semaphore()
    lines = [d for d in offsets if sum(v > 0 for v in d) == 1]
    across = {(i % sizes["gx"], j % sizes["gy"], 0) for i in (1, -1) for j in (1, -1)}
    met = lines + sorted(across & set(offsets) - set(lines))

    def tell(sem, d):
        pl.semaphore_signal(sem, inc=1, device_id=peer(d), device_id_type=pl.DeviceIdType.MESH)

    for d in met:
        tell(barrier, d)

    last = {a: sizes[a] - 1 for a in AXES}

    @pl.when(pos["gx"] == 0)
    def _():
        xrecv[...] = jnp.zeros(xrecv.shape, F32)

    loads[0].start()

    for side, place in ((0, 0), (1, last["gy"])):
        @pl.when((pos["gx"] == last["gx"]) | (pos["gy"] == place))
        def _():
            for e in range(2):
                crecv[e, side] = jnp.zeros((nf, 128), F32)

    @pl.when(pos["gx"] == last["gx"])
    def _():
        for buf in (p0, q0):
            buf[:, nx + 1, ys] = jnp.zeros((nf, ny, 128), F32)

    def clear_y(y):
        def body(x, carry):
            p0[:, x, y : y + 8] = jnp.zeros((nf, 8, 128), F32)
            return carry

        lax.fori_loop(1, nx + 1, body, 0)

        def body_w(x, carry):
            w[:, x, y : y + 8] = jnp.zeros((13, 8, 128), F32)
            return carry

        lax.fori_loop(1, nx + 1, body_w, 0)

    @pl.when(pos["gy"] == 0)
    def _():
        clear_y(0)
        yrecv[0] = jnp.zeros((nx, nf, 128), F32)

    @pl.when(pos["gy"] == last["gy"])
    def _():
        clear_y(ny + 8)
        yrecv[1] = jnp.zeros((nx, nf, 128), F32)

    for side, place in ((0, 0), (1, last["gz"])):
        @pl.when(pos["gz"] == place)
        def _():
            for e in range(2):
                for n in range(chunks):
                    zrecv[e, n, side] = jnp.zeros(zrecv.shape[3:], F32)
            wzrecv[side] = jnp.zeros((len(LO), 8, 128), F32)

    zsend[...] = jnp.zeros(zsend.shape, F32)
    for e in range(2):
        for n in range(packs(e)):
            xsend[e, n] = jnp.zeros((8, 128), F32)
    wzsend[...] = jnp.zeros(wzsend.shape, F32)

    pl.semaphore_wait(barrier, len(met))
    for d in lines:
        if d[0]:
            tell(ready.at[0], d)

    arrivals = iter(range(RECEIVES))
    free = list(range(SENDS))

    def shift(axis, up, src, dst):
        n = sizes[axis]
        i = pos[axis]
        slot = free.pop(0)
        copy = pltpu.make_async_remote_copy(
            src_ref=src, dst_ref=dst, send_sem=xs.at[slot], recv_sem=xr.at[next(arrivals)],
            device_id={axis: lax.rem(i + (1 if up else n - 1), n)},
            device_id_type=pl.DeviceIdType.MESH)
        sends = i < n - 1 if up else i > 0
        gets = i > 0 if up else i < n - 1

        @pl.when(sends)
        def _():
            copy.start()

        def finish():
            @pl.when(sends)
            def _():
                copy.wait_send()

            @pl.when(gets)
            def _():
                copy.wait_recv()

            free.append(slot)

        return finish

    def finish_all(items):
        for f in items:
            f()

    def y_faces(buf, start, length):
        xs_ = pl.ds(start, length)
        return [
            shift("gy", True, buf.at[:, xs_, pl.ds(ny, 8)], buf.at[:, xs_, pl.ds(0, 8)]),
            shift("gy", False, buf.at[:, xs_, pl.ds(8, 8)], buf.at[:, xs_, pl.ds(ny + 8, 8)]),
        ]

    def y_rows(start, length):
        part = pl.ds(start, length)
        return [
            shift("gy", True, ysend.at[0, part], yrecv.at[0, part]),
            shift("gy", False, ysend.at[1, part], yrecv.at[1, part]),
        ]

    def y_unpack(start, length):
        def body(x, carry):
            for f in range(nf):
                q0[f, x + 1, 7:8] = yrecv[0, x, f : f + 1]
                q0[f, x + 1, ny + 8 : ny + 9] = yrecv[1, x, f : f + 1]
            return carry

        if length > 3:
            lax.fori_loop(start, start + length, body, 0)
        else:
            for x in range(start, start + length):
                body(x, 0)

    def w_faces(start, length):
        xs_ = pl.ds(start, length)
        out = []
        for b, up, src, dst in ((1, True, ny, 0), (-1, False, 8, ny + 8)):
            for lo, hi in runs([k for k, o in enumerate(FORWARD) if o[1] == b]):
                ks = pl.ds(lo, hi - lo)
                out.append(shift("gy", up, w.at[ks, xs_, pl.ds(src, 8)], w.at[ks, xs_, pl.ds(dst, 8)]))
        return out

    def corner(e, up):
        side = 0 if up else 1
        i, j = pos["gx"], pos["gy"]
        slot = free.pop(0)
        copy = pltpu.make_async_remote_copy(
            src_ref=csend.at[e, side], dst_ref=crecv.at[e, side], send_sem=xs.at[slot], recv_sem=xr.at[next(arrivals)],
            device_id={"gx": moved["gx"][-1], "gy": moved["gy"][1 if up else -1]},
            device_id_type=pl.DeviceIdType.MESH)
        sends = (i > 0) & (j < last["gy"] if up else j > 0)
        gets = (i < last["gx"]) & (j > 0 if up else j < last["gy"])

        @pl.when(sends)
        def _():
            copy.start()

        def finish():
            @pl.when(sends)
            def _():
                copy.wait_send()

            @pl.when(gets)
            def _():
                copy.wait_recv()

            free.append(slot)

        return finish

    def x_down(buf, e):
        for f in range(nf):
            csend[e, 0, f : f + 1] = buf[f, 1, ny + 7 : ny + 8]
            csend[e, 1, f : f + 1] = buf[f, 1, 8:9]
        return [shift("gx", False, buf.at[:, 1, ys], buf.at[:, nx + 1, ys]), corner(e, True), corner(e, False)]

    def corners(buf, e):
        for f in range(nf):
            buf[f, nx + 1, 7:8] = crecv[e, 0, f : f + 1]
            buf[f, nx + 1, ny + 8 : ny + 9] = crecv[e, 1, f : f + 1]

    def x_tile(f, yb):
        return packs(0) + f * yb_n + yb

    def x_up(e):
        part = pl.ds(0, x_tile(nf - e, yb_n))
        return [shift("gx", True, xsend.at[e, part], xrecv.at[e, part])]

    def z_both(send, recv):
        return [
            shift("gz", True, send, recv.at[0]),
            shift("gz", False, send, recv.at[1]),
        ]

    def gram_body(accs, ub, vb):
        return [accs[i] + ub[i : i + 1] * vb[i:] for i in range(nf)]

    def gram_start():
        return tuple(jnp.zeros((nf - i, 8, 128), F32) for i in range(nf))

    def place(g, i, j):
        return 36 * g + 8 * i - i * (i - 1) // 2 + j - i

    def gram_end(g, accs):
        red[...] = jnp.zeros(red.shape, F32)
        for i in range(nf):
            red[i, i:nf, :] = jnp.sum(accs[i], axis=1)
        out = jnp.zeros((8, 128), F32)
        for i in range(nf):
            t = jnp.sum(red[i], axis=1, keepdims=True)
            out = out + jnp.where(lane == place(g, i, row), t, 0.0)
        return out

    def own(buf):
        return lambda x, yb: buf[:, x + 1, 8 + yb * 8 : 16 + yb * 8]

    def gram_plane(accs, u, v, x):
        for yb in range(yb_n):
            accs = gram_body(accs, u(x, yb), v(x, yb))
        return tuple(accs)

    def gram(g, u, v):
        return gram_end(g, lax.fori_loop(0, nx, lambda x, accs: gram_plane(accs, u, v, x), gram_start()))

    def several(n, f):
        def body(t, carry):
            for k in range(n):
                f(t * n + k, 0)
            return carry

        lax.fori_loop(0, nx // n, body, 0)

    def pack_w(x, carry):
        for yb in range(yb_n):
            j = x * yb_n + yb
            here = half_lane == j
            y = 8 + yb * 8
            for n, k in enumerate(LO):
                both = w[k, x + 1, y : y + 8]
                if n < len(HI):
                    both = jnp.where(first_lane, w[HI[n], x + 1, y : y + 8], both)
                pltpu.store(wzsend.at[n], pltpu.roll(both, 2 * j + 1, 1), mask=here)
        return carry

    def shift_w(x, carry):
        for yb in range(yb_n):
            y = 8 + yb * 8
            for n, k in enumerate(SHIFTED):
                ws[n, x, yb * 8 : yb * 8 + 8] = pltpu.roll(w[k, x + 1, y : y + 8], 1 if k in LO else 127, 1)
        return carry

    def insert_w(x, carry):
        for yb in range(yb_n):
            j = x * yb_n + yb
            for n in range(len(LO)):
                edge = pltpu.roll(uw[n], 127 - 2 * j, 1)
                pltpu.store(ws.at[n, x, yb * 8 : yb * 8 + 8], edge, mask=first_lane)
                if n < len(HI):
                    pltpu.store(ws.at[len(LO) + n, x, yb * 8 : yb * 8 + 8], edge, mask=last_lane)
        return carry

    def crossing(from_low, from_high):
        return jnp.where(even, pltpu.roll(from_high, 127, 1), pltpu.roll(from_low, 1, 1))

    def pack_z(out, f, both, m):
        m = f % group * wide + m
        pltpu.store(out.at[f // group], pltpu.roll(both, lax.rem(2 * m + 1, 128), 1), mask=half_lane == m)

    def upward(buf, e):
        for yb in range(yb_n):
            y = 8 + yb * 8
            accs = {}
            back = {}
            for b in (-1, 0, 1):
                v = buf[:, nx, y + b : y + b + 8]
                for c in (-1, 0, 1):
                    coef = w[FORWARD.index((1, -b, -c)), nx, y + b : y + b + 8]
                    term = coef[None] * v
                    accs[c] = term if c not in accs else accs[c] + term
                    back[c] = coef if c not in back else back[c] + coef
            whole = accs[0] + pltpu.roll(accs[1], 127, 2) + pltpu.roll(accs[-1], 1, 2)
            both = jnp.where(first_lane[None], accs[1], accs[-1])
            for f in range(nf):
                xsend[e, x_tile(f, yb)] = whole[f]
                pack_z(xsend.at[e], f, both[f], (deep - 1) * yb_n + yb)
            if e == 0:
                xsend[e, x_tile(nf, yb)] = (
                    back[0] + pltpu.roll(back[1], 127, 1) + pltpu.roll(back[-1], 1, 1))
                both = jnp.where(first_lane, back[1], back[-1])
                pack_z(xsend.at[e], nf, both, (deep - 1) * yb_n + yb)

    def sums(buf, e, x, lowest=False):
        for yb in range(yb_n):
            y = 8 + yb * 8
            accs = {}
            back = {}
            if lowest:
                accs[0] = jnp.stack([xrecv[e, x_tile(f, yb)] for f in range(nf)])
                if e == 0:
                    back[0] = xrecv[e, x_tile(nf, yb)]
            for a in (0, 1) if lowest else (-1, 0, 1):
                for b in (-1, 0, 1):
                    v = buf[:, x + 1 + a, y + b : y + b + 8]
                    for c in (-1, 0, 1):
                        o = (a, b, c)
                        if o == (0, 0, 0):
                            continue
                        if o > (0, 0, 0):
                            k = FORWARD.index(o)
                            if c == 0:
                                coef = w[k, x + 1, y : y + 8]
                            else:
                                coef = ws[SHIFTED.index(k), x, yb * 8 : yb * 8 + 8]
                        else:
                            k = FORWARD.index((-a, -b, -c))
                            coef = w[k, x + 1 + a, y + b : y + b + 8]
                            if e == 0:
                                back[c] = coef if c not in back else back[c] + coef
                        term = coef[None] * v
                        accs[c] = term if c not in accs else accs[c] + term
            if e == 0:
                total = s0[x, yb * 8 : yb * 8 + 8] + back[0]
                for k in range(13):
                    total = total + w[k, x + 1, y : y + 8]
                back[0] = total
            for c in (-1, 0, 1):
                scr[c + 1, yb, 0:nf] = accs[c]
                if e == 0:
                    scr[c + 1, yb, nf] = back[c]

    def settle(buf, e, x, put, chunk, where):
        for yb in range(yb_n):
            y = 8 + yb * 8
            m = where * yb_n + yb
            if e == 0:
                up, down = scr[2, yb, nf], scr[0, yb, nf]
                total = scr[1, yb, nf] + pltpu.roll(up, 127, 1) + pltpu.roll(down, 1, 1)
                diag[x, yb * 8 : yb * 8 + 8] = total
                pack_z(zsend.at[e, chunk], nf, jnp.where(first_lane, up, down), m)
            else:
                total = diag[x, yb * 8 : yb * 8 + 8]
            for f in range(nf):
                up, down = scr[2, yb, f], scr[0, yb, f]
                total_f = scr[1, yb, f] + pltpu.roll(up, 127, 1) + pltpu.roll(down, 1, 1)
                put(f, x, yb, total * buf[f, x + 1, y : y + 8] - total_f)
                pack_z(zsend.at[e, chunk], f, jnp.where(first_lane, up, down), m)

    def gather(e, chunk):
        for n in range(packs(e)):
            mine = zsend[e, chunk, n]
            ucross[chunk, n] = crossing(zrecv[e, chunk, 0, n] - mine, zrecv[e, chunk, 1, n] - mine)

    def mend(buf, e, x, get, put, chunk, where):
        for yb in range(yb_n):
            y = 8 + yb * 8
            m = where * yb_n + yb

            def edge(f):
                place = f % group * wide + m
                side = pltpu.roll(ucross[chunk, f // group], lax.rem(255 - 2 * place, 128), 1)
                return jnp.where(rim, side, 0.0)

            if e == 0:
                extra = edge(nf)
                diag[x, yb * 8 : yb * 8 + 8] += extra
            for f in range(nf):
                value = get(f, x, yb) - edge(f)
                if e == 0:
                    value = value + extra * buf[f, x + 1, y : y + 8]
                    if yb == yb_n - 1:
                        ysend[0, x, f : f + 1] = value[7:8]
                    if yb == 0:
                        ysend[1, x, f : f + 1] = value[0:1]
                put(f, x, yb, value)

    def copy_row(r, n, dst):
        return pltpu.make_async_remote_copy(
            src_ref=cur.at[r], dst_ref=slots.at[r, dst], send_sem=ars.at[r], recv_sem=arr.at[r],
            device_id=peer(offsets[n]), device_id_type=pl.DeviceIdType.MESH)

    def sum_start(r, value):
        value = jnp.sum(value, axis=0, keepdims=True)
        cur[r] = value
        slots[r, me] = value
        for n in range(devices - 1):
            copy_row(r, n, me).start()

    def sum_end(r):
        every = slots.at[r, pl.ds(0, devices - 1)]
        copies = pltpu.make_async_remote_copy(
            src_ref=every, dst_ref=every, send_sem=ars.at[r], recv_sem=arr.at[r],
            device_id=peer(offsets[0]), device_id_type=pl.DeviceIdType.MESH)
        copies.wait_send()
        copies.wait_recv()
        parts = [slots[r, q] for q in range(devices)]
        while len(parts) > 1:
            parts = [a + b for a, b in zip(parts[::2], parts[1::2])] + parts[len(parts) // 2 * 2 :]
        return jnp.broadcast_to(parts[0], (8, 128))

    def extract(total, g):
        cols = []
        for k in range(8):
            where = place(g, jnp.minimum(row, k), jnp.maximum(row, k))
            cols.append(jnp.broadcast_to(jnp.sum(jnp.where(lane == where, total, 0.0), axis=1, keepdims=True), (8, 128)))
        return cols

    def matrix(cols):
        out = jnp.zeros((8, 128), F32)
        for k in range(8):
            out = jnp.where(lane == k, cols[k], out)
        return out

    def fill(tab, cols):
        for j in range(8):
            for i in range(8):
                tab[i, j] = line(cols[j], i)

    def put_q1(f, x, yb, v):
        q0[f, x + 1, 8 + yb * 8 : 16 + yb * 8] = v

    def get_q1(f, x, yb):
        return q0[f, x + 1, 8 + yb * 8 : 16 + yb * 8]

    def put_q2(f, x, yb, v):
        q2[f, x, yb * 8 : yb * 8 + 8] = v

    def get_q2(f, x, yb):
        return q2[f, x, yb * 8 : yb * 8 + 8]

    def z_send(e, chunk):
        part = pl.ds(0, packs(e))
        return z_both(zsend.at[e, chunk, part], zrecv.at[e, chunk, :, part])

    def planes(buf, e, put, chunk):
        def body(t, carry):
            x = chunk * deep + 2 + t
            settle(buf, e, x - 1, put, chunk, t)
            sums(buf, e, x)
            return carry

        lax.fori_loop(0, deep, body, 0)
        return z_send(e, chunk)

    end = chunks - 1

    def interior(buf, e, put):
        sent = []
        sums(buf, e, 1)
        for n in range(end):
            with NS(f"op{e}_in{n}"):
                sent.append(planes(buf, e, put, n))
        with NS(f"op{e}_in{end}"):
            settle(buf, e, nx - 3, put, end, 0)
            sums(buf, e, nx - 2)
            settle(buf, e, nx - 2, put, end, 1)
        return sent

    def outer(buf, e, put, across):
        with NS(f"op{e}_xwait"):
            finish_all(across)
        with NS(f"op{e}_st3"):
            corners(buf, e)
            sums(buf, e, nx - 1)
            settle(buf, e, nx - 1, put, end, 2)
            sums(buf, e, 0, True)
            settle(buf, e, 0, put, end, 3)
            for n in range(packs(e)):
                zsend[e, end, n] += xrecv[e, n]
            return z_send(e, end)

    def mend_gram(buf, e, get, put, u, v, accs, chunk):
        for t in range(deep):
            x = chunk * deep + 1 + t
            mend(buf, e, x, get, put, chunk, t)
            accs = gram_plane(accs, u, v, x)
        return accs

    def mend_end(buf, e, get, put, between=None):
        for where, x in ((0, nx - 3), (1, nx - 2), (2, nx - 1), (3, 0)):
            mend(buf, e, x, get, put, end, where)
            if between and where == 2:
                between()

    rest = (nx - 1, 0, nx - 3, nx - 2)

    with NS("a_loadw"):
        loads[1].wait()
        rims = w_faces(1, nx)
    with NS("a_packw"):
        several(8, pack_w)
        zw = z_both(wzsend, wzrecv)
    with NS("a_loadp"):
        loads[0].wait()
        rims += y_faces(p0, nx, 1)
        down = x_down(p0, 0)
        sides = y_faces(p0, 1, nx - 1)
    with NS("a_gram0"):
        gacc[...] = gram(0, own(p0), own(p0))
    with NS("a_shiftw"):
        several(4, shift_w)
    with NS("a_up"):
        finish_all(rims)
        upward(p0, 0)
        up = x_up(0)
    with NS("a_zwait"):
        finish_all(zw)
    with NS("a_insw"):
        for n in range(len(LO)):
            uw[n] = crossing(wzrecv[0, n], wzrecv[1, n])
        several(8, insert_w)
    pl.semaphore_wait(ready.at[0], sizes["gx"] - 1)
    for d in lines:
        if d[1]:
            tell(ready.at[1], d)
    with NS("a_ywait"):
        loads[2].wait()
        finish_all(sides)
    sent = interior(p0, 0, put_q1)
    sent.append(outer(p0, 0, put_q1, down + up))

    def squares(lo, hi, accs):
        return lax.fori_loop(lo, hi, lambda x, accs: gram_plane(accs, own(q0), own(q0), x), accs)

    def hold(n, accs):
        for i in range(nf):
            held[n, i, i:nf] = accs[i]

    def resume(n):
        return tuple(held[n, i, i:nf] for i in range(nf))

    accs = gram_start()
    for n in range(end):
        with NS(f"b_zwait{n}"):
            finish_all(sent[n])
            gather(0, n)
        with NS(f"b_mend{n}"):
            accs = mend_gram(p0, 0, get_q1, put_q1, own(p0), own(q0), accs, n)
        if n:
            with NS(f"b_square{n}"):
                hold(0, accs)
                if n == end - 1:
                    sides = y_rows(1, end * deep)
                start = 1 if n == 1 else n * deep + 1
                hold(1, squares(start, (n + 1) * deep + 1, gram_start() if n == 1 else resume(1)))
                accs = resume(0)
    with NS(f"b_zwait{end}"):
        finish_all(sent[end])
        gather(0, end)
    rims = []
    with NS(f"b_mend{end}"):
        mend_end(p0, 0, get_q1, put_q1, lambda: rims.extend(y_rows(nx - 3, 3)))
        sides += y_rows(0, 1)
    with NS("b_gram1"):
        for x in rest:
            accs = gram_plane(accs, own(p0), own(q0), x)
        gacc[...] += gram_end(1, accs)
    with NS("b_gram2"):
        down = x_down(q0, 1)
        both = resume(1)
        for x in rest:
            both = gram_plane(both, own(q0), own(q0), x)
        both = gram_end(2, both)
    pl.semaphore_wait(ready.at[1], sizes["gy"] - 1)
    with NS("b_sum"):
        sum_start(0, gacc[...] + both)
    with NS("b_up"):
        finish_all(rims)
        y_unpack(nx - 3, 3)
        upward(q0, 1)
        up = x_up(1)
    with NS("b_ywait"):
        finish_all(sides)
        y_unpack(1, end * deep)
        y_unpack(0, 1)

    sent = interior(q0, 1, put_q2)

    def get_v2(x, yb):
        return q2[:, x, yb * 8 : yb * 8 + 8]

    with NS("c_sum1"):
        total = sum_end(0)
    with NS("c_alg1"):
        rrc, pqc, ssc = [extract(total, g) for g in range(3)]
        rr, pq = matrix(rrc), matrix(pqc)
        alpha = solve(pqc, rr, row)
        alpha_c = columns(alpha)
        fill(t_alpha, alpha_c)
        alpha_tc = columns(transposed(alpha, row, lane))
        ssa = mm(ssc, alpha)
        new = rr - mm(alpha_tc, pq) - mm(pqc, alpha) + mm(alpha_tc, ssa)
        beta = solve(rrc, new, row)
        fill(t_beta, columns(beta))
        ib = beta + jnp.where(lane == row, 1.0, 0.0)
        ib_tc = columns(transposed(ib, row, lane))
        fill(t_ib, columns(ib))
        left = mm(ib_tc, mm(pqc, ib) - ssa) - mm(alpha_tc, mm(ssc, ib))

    def early(x, carry):
        for yb in range(yb_n):
            y = slice(yb * 8, yb * 8 + 8)
            u, v = own(p0)(x, yb), own(q0)(x, yb)
            step, rest = t_alpha[0] * u[0][None], u
            for i in range(nf):
                if i:
                    step = step + t_alpha[i] * u[i][None]
                rest = rest - t_alpha[i] * v[i][None]
            x1[:, x, y] = step
            r1[:, x, y] = rest
        return carry

    def late(x, carry):
        for yb in range(yb_n):
            y = slice(yb * 8, yb * 8 + 8)
            u, v, z = own(p0)(x, yb), own(q0)(x, yb), get_v2(x, yb)
            step, image = r1[:, x, y], jnp.zeros((nf, 8, 128), F32)
            for i in range(nf):
                step = step + t_beta[i] * u[i][None]
                image = image + (t_ib[i] * v[i][None] - t_alpha[i] * z[i][None])
            p1[:, x, y] = step
            s1[:, x, y] = image
        return carry

    first, second = nx // 8, nx // 2
    with NS("c_early0"):
        lax.fori_loop(0, first, early, 0)
    sent.append(outer(q0, 1, put_q2, down + up))
    accs = gram_start()
    for n in range(end):
        with NS(f"c_zwait{n}"):
            finish_all(sent[n])
            gather(1, n)
        with NS(f"c_mend{n}"):
            accs = mend_gram(q0, 1, get_q2, put_q2, own(q0), get_v2, accs, n)
    with NS("c_early1"):
        lax.fori_loop(first, second, early, 0)
    with NS(f"c_zwait{end}"):
        finish_all(sent[end])
        gather(1, end)
    with NS(f"c_mend{end}"):
        mend_end(q0, 1, get_q2, put_q2)
        for x in rest:
            accs = gram_plane(accs, own(q0), get_v2, x)
        sum_start(1, gram_end(0, accs))
    with NS("c_early2"):
        lax.fori_loop(second, nx, early, 0)
    with NS("c_late"):
        lax.fori_loop(0, nx, late, 0)
    with NS("c_sum2"):
        total = sum_end(1)
    with NS("c_alg2"):
        curve = left + mm(alpha_tc, mm(extract(total, 0), alpha))
        cols = columns(solve(columns(curve), new, row))
        fill(t_out, cols)
        slot = lax.rem(lane // 8, 8)
        high, low = [], []
        for j in range(8):
            block = jnp.zeros((8, 128), F32)
            for i in range(8):
                block = jnp.where(slot == i, line(cols[j], i), block)
            block = jnp.where(lax.rem(lane, 8) == row, block, 0.0)
            near = block.astype(jnp.bfloat16).astype(F32)
            high.append(near)
            low.append(jnp.where(lane < 64, block - near, 0.0))
        m_out[...] = jnp.concatenate(high + low, axis=0).astype(jnp.bfloat16)


def final_kernel(dims, step, t, m, x1, r1, p1, s1, sol, res, sol_buf, res_buf, sem):
    nf, nx, ny = dims

    def saves(n):
        part = pl.ds(n * step, step)
        return [pltpu.make_async_copy(sol_buf.at[:, part], sol.at[:, part], sem.at[0]),
                pltpu.make_async_copy(res_buf.at[:, part], res.at[:, part], sem.at[1])]

    def halves(v):
        v = v.reshape(64, 128)
        high = v.astype(jnp.bfloat16)
        low = (v - high.astype(F32)).astype(jnp.bfloat16)
        return jnp.concatenate([high, low], axis=0)

    blocks = [slice(yb * 8, yb * 8 + 8) for yb in range(ny // 8)]

    def body(n, carry):
        for k in range(step):
            x = n * step + k
            both = jnp.concatenate([halves(p1[:, x, y]) for y in blocks], axis=1)
            moves = jnp.dot(m[...], both, preferred_element_type=F32)
            moves = moves[:64] + moves[64:]
            for b, y in enumerate(blocks):
                v, e = s1[:, x, y], r1[:, x, y]
                for i in range(nf):
                    e = e - t[i] * v[i][None]
                sol_buf[:, x, y] = x1[:, x, y] + moves[:, b * 128 : b * 128 + 128].reshape(8, 8, 128)
                res_buf[:, x, y] = e
        for copy in saves(n):
            copy.start()
        return carry

    lax.fori_loop(0, nx // step, body, 0)

    pltpu.make_async_copy(sol_buf, sol, sem.at[0]).wait()
    pltpu.make_async_copy(res_buf, res, sem.at[1]).wait()


def shards(sizes, rhs, stencil):
    nf, nx, ny, nz = rhs.shape
    tall = ny + 16
    field = jax.ShapeDtypeStruct(rhs.shape, F32)
    kept = pltpu.VMEM(rhs.shape, F32)
    table = pltpu.VMEM((8, 8, 8, nz), F32)
    anyspace = pl.BlockSpec(memory_space=pl.ANY)
    local = pl.BlockSpec(memory_space=pltpu.VMEM)
    devices = sizes["gx"] * sizes["gy"] * sizes["gz"]
    chunks, packs = nx // 4, nf // (16 // (ny // 8)) + 1
    padded = pltpu.VMEM((nf, nx + 2, tall, nz), F32)

    def kernel(*refs):
        main_kernel(sizes, (nf, nx, ny), *refs)

    x1, r1, p1, s1, t, m = pl.pallas_call(
        kernel,
        out_shape=(kept, kept, kept, kept, table, pltpu.VMEM((128, 128), jnp.bfloat16)),
        in_specs=[pl.BlockSpec(memory_space=pltpu.HBM)] * 2,
        out_specs=(local,) * 6,
        scratch_shapes=[
            padded, padded,
            pltpu.VMEM((13, nx + 1, tall, nz), F32),
            pltpu.VMEM((len(LO) + len(HI), nx, ny, nz), F32),
            pltpu.VMEM((nx, ny, nz), F32),
            pltpu.VMEM((nx, ny, nz), F32),
            pltpu.VMEM((nf, nx, ny, nz), F32),
            pltpu.VMEM((3, ny // 8, nf + 1, 8, nz), F32),
            pltpu.VMEM((2, 2, nf, nz), F32),
            pltpu.VMEM((2, 2, nf, nz), F32),
            pltpu.VMEM((2, packs + (nf + 1) * ny // 8, 8, nz), F32),
            pltpu.VMEM((2, packs + (nf + 1) * ny // 8, 8, nz), F32),
            pltpu.VMEM((2, nx, nf, nz), F32),
            pltpu.VMEM((2, nx, nf, nz), F32),
            pltpu.VMEM((2, chunks, packs, 8, nz), F32),
            pltpu.VMEM((2, chunks, 2, packs, 8, nz), F32),
            pltpu.VMEM((len(LO), 8, nz), F32),
            pltpu.VMEM((2, len(LO), 8, nz), F32),
            pltpu.VMEM((chunks, packs, 8, nz), F32),
            pltpu.VMEM((len(LO), 8, nz), F32),
            pltpu.VMEM((8, 8, 128), F32),
            pltpu.VMEM((2, 8, 8, 8, 128), F32),
            pltpu.VMEM((8, 128), F32),
            pltpu.VMEM((2, 1, 128), F32),
            pltpu.VMEM((2, devices, 1, 128), F32),
            table, table, table,
            pltpu.SemaphoreType.DMA((3,)),
            pltpu.SemaphoreType.DMA((SENDS,)),
            pltpu.SemaphoreType.DMA((RECEIVES,)),
            pltpu.SemaphoreType.DMA((2,)),
            pltpu.SemaphoreType.DMA((2,)),
            pltpu.SemaphoreType.REGULAR((2,)),
        ],
        compiler_params=pltpu.CompilerParams(
            collective_id=0, has_side_effects=True, vmem_limit_bytes=40 * 2**20),
        name="krylov",
    )(*[pltpu.with_memory_space_constraint(v, pltpu.HBM) for v in (rhs, stencil)])

    step = 4

    def last(*refs):
        final_kernel((nf, nx, ny), step, *refs)

    return pl.pallas_call(
        last,
        out_shape=(field, field),
        in_specs=[local] * 6,
        out_specs=(pl.BlockSpec(memory_space=pltpu.HBM),) * 2,
        scratch_shapes=[
            pltpu.VMEM(rhs.shape, F32), pltpu.VMEM(rhs.shape, F32),
            pltpu.SemaphoreType.DMA((2,)),
        ],
        compiler_params=pltpu.CompilerParams(vmem_limit_bytes=40 * 2**20),
        name="combine",
    )(t, m, x1, r1, p1, s1)


def solution(mesh):
    sizes = {a: mesh.shape[a] for a in AXES}
    spec = P(None, "gx", "gy", "gz")

    def run(rhs, stencil):
        return shards(sizes, rhs, stencil)

    return jax.shard_map(run, mesh=mesh, in_specs=(spec, spec), out_specs=(spec, spec), check_vma=False)
```
